32 devices in a mesh: seqs: 4 (over y, z), states: 8 (over x, core).
Axes of the slice: x: 4, y: 2, z: 2, core: 2. Of those that a mesh axis runs over, the one named last changes fastest.
The devices are a block of a 4x4x8 slice.
Arguments:
- trans_mat: bfloat16 [16384, 16384], P(None, 'states')
- emit_mat: bfloat16 [16384, 10000], P('states')
- init_prob: float32 [16384], P('states')
- tokens: int32 [512, 8], P('seqs'), parts along dimension 0
- lengths: int32 [512], P('seqs'), parts along dimension 0
Outputs:
- output 1: float32 [512], P('seqs'), parts along dimension 0
- output 2: float32 [512, 16384], P('seqs', 'states'), parts along dimension 0
- output 3: float32 [65536, 2048], P(('seqs', 'states')), parts along dimension 0
There are 4 independent parts. The reference program is written for one: setup_inputs(seed, part) draws one part's arguments, and reference() takes and returns one part's arrays. A program takes and returns all parts, laid end to end along the dimension named above; an argument that names none is the same for every part.
All inputs are finite; a program needn't handle non-finite values.
Results may differ from the reference program's by a relative error of at most 0.001.
Values are sent between devices in bfloat16 or wider.
A program may use at most 768 MiB of HBM per device.

```python
import jax
import jax.numpy as jnp
from jax import lax

K = 16384
V = 10000
B = 128
T = 8
GROUPS = 8
BLOCK_SIZE = K // GROUPS


def setup_inputs(seed: int = 0, part: int = 0) -> dict:
    key = jax.random.key(seed)
    key_trans, key_emit, key_init, key_part = jax.random.split(key, 4)
    part_key = jax.random.fold_in(key_part, part)
    key_tok, key_len = jax.random.split(part_key, 2)
    tile_rows = 512

    def trans_tile(tile_idx):
        logits = 2.0 * jax.random.normal(jax.random.fold_in(key_trans, tile_idx), (tile_rows, K), jnp.float32)
        return jax.nn.softmax(logits, axis=1).astype(jnp.bfloat16)

    def emit_tile(tile_idx):
        logits = 1.5 * jax.random.normal(jax.random.fold_in(key_emit, tile_idx), (tile_rows, V), jnp.float32)
        return jax.nn.softmax(logits, axis=1).astype(jnp.bfloat16)

    tile_ids = jnp.arange(K // tile_rows)
    trans_mat = lax.map(trans_tile, tile_ids).reshape(K, K)
    emit_mat = lax.map(emit_tile, tile_ids).reshape(K, V)
    init_prob = jax.nn.softmax(2.0 * jax.random.normal(key_init, (K,), jnp.float32))
    tokens = jax.random.randint(key_tok, (B, T), 0, V, jnp.int32)
    drawn_len = jax.random.randint(key_len, (B,), 1, T + 1, jnp.int32)
    lengths = jnp.where(jnp.arange(B) == 0, T, drawn_len).astype(jnp.int32)
    return {'trans_mat': trans_mat, 'emit_mat': emit_mat, 'init_prob': init_prob, 'tokens': tokens, 'lengths': lengths}


def reference(trans_mat, emit_mat, init_prob, tokens, lengths):
    def emit_at(step_idx):
        return jnp.take(emit_mat, tokens[:, step_idx], axis=1).T.astype(jnp.float32)

    first_mass = init_prob[None, :] * emit_at(0)
    first_norm = jnp.sum(first_mass, axis=1)
    alpha_first = first_mass / first_norm[:, None]

    def forward_step(alpha_cur, step_idx):
        pred_mass = jnp.dot(alpha_cur.astype(jnp.bfloat16), trans_mat, preferred_element_type=jnp.float32)
        new_mass = pred_mass * emit_at(step_idx)
        norm_sum = jnp.sum(new_mass, axis=1)
        live_mask = step_idx < lengths
        step_scale = jnp.where(live_mask, norm_sum, 1.0)
        alpha_next = jnp.where(live_mask[:, None], new_mass / norm_sum[:, None], alpha_cur)
        return alpha_next, (alpha_cur.astype(jnp.bfloat16), step_scale)

    later_steps = jnp.arange(1, T)
    alpha_last, (alpha_prev, scales) = lax.scan(forward_step, alpha_first, later_steps)
    loglik = jnp.log(first_norm) + jnp.sum(jnp.log(scales), axis=0)

    def backward_step(carry, inputs):
        beta_cur, pair_sum = carry
        step_idx, prev_bf, step_scale = inputs
        live_mask = step_idx < lengths
        weight = jnp.where(live_mask[:, None], emit_at(step_idx) * beta_cur / step_scale[:, None], 0.0).astype(jnp.bfloat16)
        pair_sum = pair_sum + jnp.einsum('bgi,bgj->gij', prev_bf.reshape(B, GROUPS, BLOCK_SIZE).astype(jnp.float32), weight.reshape(B, GROUPS, BLOCK_SIZE).astype(jnp.float32))
        beta_prev = lax.dot_general(weight, trans_mat, (((1,), (1,)), ((), ())), preferred_element_type=jnp.float32)
        beta_prev = beta_prev + jnp.where(live_mask, 0.0, 1.0)[:, None]
        return (beta_prev, pair_sum), None

    start = (jnp.ones((B, K), jnp.float32), jnp.zeros((GROUPS, BLOCK_SIZE, BLOCK_SIZE), jnp.float32))
    (_, pair_sum), _ = lax.scan(backward_step, start, (later_steps, alpha_prev, scales), reverse=True)
    diag_blocks = jnp.moveaxis(jnp.diagonal(trans_mat.reshape(GROUPS, BLOCK_SIZE, GROUPS, BLOCK_SIZE), axis1=0, axis2=2), 2, 0)
    counts = (diag_blocks.astype(jnp.float32) * pair_sum).reshape(K, BLOCK_SIZE)
    return loglik, alpha_last, counts
```

```python
import functools

import jax
import jax.numpy as jnp
from jax import lax
from jax.experimental import pallas as pl
from jax.experimental.pallas import tpu as pltpu
from jax.sharding import PartitionSpec as P

AXIS = "states"
LANES = 128
F32 = jnp.float32
BF16 = jnp.bfloat16


def _loop(n, body):
    def step(i, carry):
        body(i)
        return carry

    lax.fori_loop(0, n, step, 0)


def _recursion(caps, a_hbm, em_hbm, pi_ref, lcol_ref, lrow_ref, al_hbm, w_hbm, post_hbm, ll_ref,
               ring, al, acc, cur, emv, rcs, sbuf, csend, cbuf, wv, ost, sst, own, dbuf, trans, fin,
               ring_sem, em_sem, al_recv, own_send, part_send, on_send, c_send, c_recv, save_sem, post_sem,
               d_send, d_recv, s_send, t_recv, f_recv):
    nd = cbuf.shape[0]
    nx = nd // 2
    step_count, seqs, bs = em_hbm.shape
    hb = bs // 2
    slab = min(512, hb)
    tiles = bs // LANES
    g = lax.axis_index(AXIS)
    x, c = g // 2, g % 2

    def dev(dx, flip):
        return ((x + dx) % nx) * 2 + (c + flip) % 2

    partner, right, left = dev(0, 1), dev(1, 0), dev(nx - 1, 0)

    def remote(src, dst, send, recv, to):
        return pltpu.make_async_remote_copy(
            src_ref=src, dst_ref=dst, send_sem=send, recv_sem=recv,
            device_id={AXIS: to}, device_id_type=pl.DeviceIdType.MESH)

    def for_caps(t, fn):
        sizes = sorted(set(caps))
        if len(sizes) == 1:
            fn(sizes[0])
            return
        for tt in range(1, step_count):
            pl.when(t == tt)(functools.partial(fn, caps[tt - 1]))

    def fwd_row(group, i):
        if group == 0:
            src, half = dev(0, i // 2), i % 2
        elif group == 3:
            src, half = dev(2, i // 2), i % 2
        else:
            src, half = dev(nx - 1 - 2 * (i % 2), i // 2), (group - 1 + i % 2) % 2
        return src * bs + half * hb

    def bwd_row(group, i):
        q, flip = i // 2, 1 - i % 2
        if group == 0:
            src, half = dev(2, flip), q
        elif group == 3:
            src, half = dev(0, flip), q
        else:
            src, half = dev(1 + 2 * q, flip), (1 - q if group == 1 else q)
        return src * bs + half * hb

    def tile_copy(row, slot):
        return pltpu.make_async_copy(a_hbm.at[pl.ds(pl.multiple_of(row, hb), hb)], ring.at[slot], ring_sem.at[slot])

    def em_copy(t):
        return pltpu.make_async_copy(em_hbm.at[t], emv.at[t % 2], em_sem.at[t % 2])

    for grp in range(2):
        _loop(4, lambda i, grp=grp: tile_copy(fwd_row(grp, i), grp * 4 + i).start())
    em_copy(0).start()
    em_copy(1).start()

    barrier = pltpu.get_barrier_semaphore()
    for k in range(1, nd):
        pl.semaphore_signal(barrier, inc=1, device_id={AXIS: (g + k) % nd}, device_id_type=pl.DeviceIdType.MESH)
    pl.semaphore_wait(barrier, nd - 1)

    def rows_of(i):
        return pl.ds(pl.multiple_of(i * 16, 16), 16)

    def lane(k):
        return pl.ds(k * LANES, LANES)

    def inner(k):
        return (k * LANES) // hb, pl.ds((k * LANES) % hb, LANES)

    def weigh(t, first):
        def body(i):
            r = rows_of(i)
            total = jnp.zeros((16, LANES), F32)
            for k in range(tiles):
                e = emv[t % 2, r, lane(k)].astype(F32)
                mass = (pi_ref[:, lane(k)] * e) if first else acc[r, lane(k)] * e
                acc[r, lane(k)] = mass
                total = total + mass
            sbuf[r, :] = total

        _loop(seqs // 16, body)

    def normalise(t):
        row = jnp.sum(jnp.transpose(sbuf[...]), axis=0, keepdims=True)
        wide = jnp.broadcast_to(row, csend.shape)
        csend[...] = wide
        cbuf[g] = wide
        copies = [remote(csend, cbuf.at[g], c_send.at[k - 1], c_recv.at[g], (g + k) % nd) for k in range(1, nd)]
        for cp in copies:
            cp.start()
        for k in range(1, nd):
            frm = (g + k) % nd
            remote(csend, cbuf.at[frm], c_send.at[k - 1], c_recv.at[frm], frm).wait_recv()
        norm = cbuf[0, 0:1, :]
        for d in range(1, nd):
            norm = norm + cbuf[d, 0:1, :]
        rcs[t] = 1.0 / jnp.transpose(jnp.broadcast_to(norm, (LANES, LANES)))
        ll_ref[...] = ll_ref[...] + jnp.where(t < lrow_ref[...], jnp.log(jnp.broadcast_to(norm, ll_ref.shape)), 0.0)

        def body(i):
            r = rows_of(i)
            rc = rcs[t, r, :]
            live = t < lcol_ref[r, :]
            for k in range(tiles):
                h, col = inner(k)
                val = jnp.where(live, acc[r, lane(k)] * rc, cur[r, lane(k)])
                cur[r, lane(k)] = val
                al[0, h, r, col] = val.astype(BF16)

        _loop(seqs // 16, body)
        for cp in copies:
            cp.wait_send()

    ll_ref[...] = jnp.zeros_like(ll_ref)
    em_copy(0).wait()
    weigh(0, True)
    normalise(0)

    def own_copies(rows):
        m = pl.ds(0, rows)
        out = [remote(al.at[0, h, m], al.at[1, h, m], own_send.at[0, h], al_recv.at[1, h], partner) for h in (0, 1)]
        for h in (0, 1):
            out.append(remote(al.at[0, h, m], al.at[2, h, m], own_send.at[1, h], al_recv.at[2, h], right))
            out.append(remote(al.at[0, 1 - h, m], al.at[3, 1 - h, m], own_send.at[2, 1 - h], al_recv.at[3, 1 - h], left))
        return out

    def to_partner(slot, to_slot, half, rows):
        m = pl.ds(0, rows)
        return remote(al.at[slot, half, m], al.at[to_slot, half, m], part_send.at[slot, half], al_recv.at[to_slot, half], partner)

    def onward(s, rows):
        m = pl.ds(0, rows)
        return remote(al.at[2 + s, s, m], al.at[6, s, m], on_send.at[s], al_recv.at[6, s], dev(1 + (nx - 2) * s, 0))

    def arrived(slot, half, rows):
        m = pl.ds(0, rows)
        remote(al.at[slot, half, m], al.at[slot, half, m], part_send.at[slot, half], al_recv.at[slot, half], partner).wait_recv()

    def save_copies(t):
        return [pltpu.make_async_copy(al.at[0, h], al_hbm.at[t, :, pl.ds(h * hb, hb)], save_sem.at[h]) for h in (0, 1)]

    def multiply(slot, half, buf):
        lhs = al[slot, half]
        for n in range(bs // slab):
            cols = pl.ds(n * slab, slab)
            acc[:, cols] = acc[:, cols] + jnp.dot(lhs, ring[buf, :, cols], preferred_element_type=F32)

    def next_pass(t, group, i):
        slot = group * 4 + i

        @pl.when(t < step_count - 1)
        def _():
            tile_copy(fwd_row(group, i), slot).start()

        @pl.when(t == step_count - 1)
        def _():
            tile_copy(bwd_row(group, i), slot).start()

    def forward(idx):
        t = idx + 1
        for_caps(t, lambda rows: [cp.start() for cp in own_copies(rows)] and None)
        for cp in save_copies(t - 1):
            cp.start()

        @pl.when(t + 1 < step_count)
        def _():
            em_copy(t + 1).start()

        acc[...] = jnp.zeros_like(acc)

        def group0(i):
            slot, half = i // 2, i % 2
            pl.when(i >= 2)(lambda: for_caps(t, lambda rows: arrived(1, half, rows)))
            tile_copy(0, i).wait()
            multiply(slot, half, i)
            tile_copy(fwd_row(2, i), i).start()

        def group12(i, k):
            slot, half = 2 + i, (k + i % 2) % 2
            for_caps(t, lambda rows: arrived(slot, half, rows))

            @pl.when(i < 2)
            def _():
                def send(rows):
                    to_partner(slot, slot + 2, half, rows).start()
                    if k == 0:
                        onward(i, rows).start()

                for_caps(t, send)

            buf = 4 * (1 - k) + i
            tile_copy(0, buf).wait()
            multiply(slot, half, buf)
            if k == 0:
                tile_copy(fwd_row(3, i), buf).start()
            else:
                next_pass(t, 0, i)

        def group3(i):
            slot, half = 6 + i // 2, i % 2

            def ready(rows):
                arrived(slot, half, rows)
                pl.when(i < 2)(lambda: to_partner(6, 7, half, rows).start())

            for_caps(t, ready)
            tile_copy(0, 4 + i).wait()
            multiply(slot, half, 4 + i)
            next_pass(t, 1, i)

        _loop(4, group0)
        _loop(4, lambda i: group12(i, 0))
        _loop(4, lambda i: group12(i, 1))
        _loop(4, group3)

        def drained(rows):
            for cp in own_copies(rows):
                cp.wait_send()
            for half in (0, 1):
                to_partner(2, 4, half, rows).wait_send()
                to_partner(3, 5, half, rows).wait_send()
                to_partner(6, 7, half, rows).wait_send()
                onward(half, rows).wait_send()

        for_caps(t, drained)
        for cp in save_copies(t - 1):
            cp.wait()
        em_copy(t).wait()
        weigh(t, False)
        normalise(t)

    _loop(step_count - 1, forward)

    post_copy = pltpu.make_async_copy(cur, post_hbm, post_sem)
    post_copy.start()

    def weights(t):
        def body(i):
            r = rows_of(i)
            rc = rcs[t, r, :]
            live = t < lcol_ref[r, :]
            for k in range(tiles):
                h, col = inner(k)
                val = emv[t % 2, r, lane(k)].astype(F32) * own[h, r, col] * rc
                wv[r, lane(k)] = jnp.where(live, val, 0.0).astype(BF16)

        _loop(seqs // 16, body)

    def w_copy(t):
        return pltpu.make_async_copy(wv, w_hbm.at[t - 1], save_sem.at[0])

    def partial_sums(out, buf):
        for n in range(hb // slab):
            rows = pl.ds(n * slab, slab)
            out[:, rows] = lax.dot_general(wv[...], ring[buf, rows, :], (((1,), (1,)), ((), ())), preferred_element_type=F32)

    def add_into(out, *terms):
        def body(i):
            r = rows_of(i)
            val = out[r, :]
            for term in terms:
                val = val + term[r, :]
            out[r, :] = val

        _loop(seqs // 16, body)

    def to_core(p, q, rows):
        m = pl.ds(0, rows)
        return remote(ost.at[q, m], dbuf.at[p, m], d_send.at[q], d_recv.at[p], partner)

    def ring_copy(t, stage, q, rows):
        m, par, to = pl.ds(0, rows), t % 2, dev(1 + (nx - 2) * q, 0)
        if stage == 0:
            return remote(sst.at[q, m], trans.at[par, q, m], s_send.at[q], t_recv.at[par, q], to)
        half = 1 - q if stage == 1 else q
        p = stage * 2 + q
        return remote(sst.at[p, m], fin.at[par, q, half, m], s_send.at[p], f_recv.at[par, q, half], to)

    def backward(idx):
        t = step_count - 1 - idx
        par = t % 2
        weights(t)
        w_copy(t).start()

        @pl.when(t > 2)
        def _():
            em_copy(t - 2).start()

        def stage(n):
            def pair(q):
                p = n * 2 + q
                buf = 4 * (n % 2) + 2 * q
                if n > 0:
                    for_caps(t, lambda rows: to_core(p, q, rows).wait_send())
                tile_copy(0, buf).wait()
                partial_sums(ost.at[q], buf)
                for_caps(t, lambda rows: to_core(p, q, rows).start())

                def refill(i):
                    row = bwd_row((n + 2) % 4, 2 * q + i)
                    if n < 2:
                        tile_copy(row, buf + i).start()
                    else:
                        pl.when(t > 2)(lambda: tile_copy(row, buf + i).start())

                refill(0)
                tile_copy(0, buf + 1).wait()
                out = own.at[q] if n == 3 else sst.at[p]
                partial_sums(out, buf + 1)
                refill(1)
                for_caps(t, lambda rows: to_core(p, q, rows).wait_recv())
                if n == 2:
                    for_caps(t, lambda rows: ring_copy(t, 0, q, rows).wait_recv())
                    add_into(out, dbuf.at[p], trans.at[par, q])
                else:
                    add_into(out, dbuf.at[p])
                if n < 3:
                    for_caps(t, lambda rows: ring_copy(t, n, q, rows).start())

            _loop(2, pair)

        for n in range(4):
            stage(n)

        def landed(rows):
            for n in (1, 2):
                for q in (0, 1):
                    ring_copy(t, n, q, rows).wait_recv()

        for_caps(t, landed)

        def body(i):
            r = rows_of(i)
            live = t < lcol_ref[r, :]
            for k in range(tiles):
                h, col = inner(k)
                val = own[h, r, col] + fin[par, 0, h, r, col] + fin[par, 1, h, r, col]
                own[h, r, col] = jnp.where(live, val, 1.0)

        _loop(seqs // 16, body)

        def drained(rows):
            for q in (0, 1):
                to_core(6 + q, q, rows).wait_send()
                for n in range(3):
                    ring_copy(t, n, q, rows).wait_send()

        for_caps(t, drained)
        w_copy(t).wait()

        @pl.when(t > 2)
        def _():
            em_copy(t - 2).wait()

    own[...] = jnp.ones_like(own)
    _loop(step_count - 2, backward)
    weights(1)
    w_copy(1).start()
    w_copy(1).wait()
    post_copy.wait()


def _run_recursion(nd, caps, trans_loc, em, init_loc, lengths):
    step_count, seqs, bs = em.shape
    hb = bs // 2
    dma = pltpu.SemaphoreType.DMA
    lcol = jnp.broadcast_to(lengths[:, None], (seqs, LANES))
    lrow = jnp.broadcast_to(lengths[None, :], (8, seqs))
    vm, hbm = pl.BlockSpec(memory_space=pltpu.VMEM), pl.BlockSpec(memory_space=pl.ANY)
    scratch = [
        pltpu.VMEM((8, hb, bs), BF16),
        pltpu.VMEM((8, 2, seqs, hb), BF16),
        pltpu.VMEM((seqs, bs), F32),
        pltpu.VMEM((seqs, bs), F32),
        pltpu.VMEM((2, seqs, bs), BF16),
        pltpu.VMEM((step_count, seqs, LANES), F32),
        pltpu.VMEM((seqs, LANES), F32),
        pltpu.VMEM((8, seqs), F32),
        pltpu.VMEM((nd, 8, seqs), F32),
        pltpu.VMEM((seqs, bs), BF16),
        pltpu.VMEM((2, seqs, hb), F32),
        pltpu.VMEM((6, seqs, hb), F32),
        pltpu.VMEM((2, seqs, hb), F32),
        pltpu.VMEM((8, seqs, hb), F32),
        pltpu.VMEM((2, 2, seqs, hb), F32),
        pltpu.VMEM((2, 2, 2, seqs, hb), F32),
        dma((8,)), dma((2,)), dma((8, 2)), dma((3, 2)), dma((8, 2)), dma((2,)), dma((nd,)), dma((nd,)), dma((2,)), dma,
        dma((2,)), dma((8,)), dma((6,)), dma((2, 2)), dma((2, 2, 2)),
    ]
    return pl.pallas_call(
        functools.partial(_recursion, caps),
        name="recursion",
        out_shape=[
            jax.ShapeDtypeStruct((step_count - 1, seqs, bs), BF16),
            jax.ShapeDtypeStruct((step_count - 1, seqs, bs), BF16),
            jax.ShapeDtypeStruct((seqs, bs), F32),
            jax.ShapeDtypeStruct((8, seqs), F32),
        ],
        in_specs=[hbm, hbm, vm, vm, vm],
        out_specs=[hbm, hbm, hbm, vm],
        scratch_shapes=scratch,
        compiler_params=pltpu.CompilerParams(collective_id=0, has_side_effects=True, vmem_limit_bytes=66_000_000),
    )(trans_loc, em, init_loc[None, :], lcol, lrow)


def solution(mesh):
    nd = mesh.shape[AXIS]

    def local_run(trans_loc, emit_loc, init_loc, tokens_loc, lengths_loc):
        seqs, step_count = tokens_loc.shape
        bs = trans_loc.shape[1]
        em = jnp.take(emit_loc.T, tokens_loc.T.reshape(-1), axis=0, mode="clip").reshape(step_count, seqs, bs)
        caps = (seqs,) * (step_count - 1)
        alphas, ws, post, ll = _run_recursion(nd, caps, trans_loc, em, init_loc, lengths_loc)
        pair_sum = lax.dot_general(alphas.reshape(-1, bs), ws.reshape(-1, bs), (((0,), (0,)), ((), ())), preferred_element_type=F32)
        diag = lax.dynamic_slice_in_dim(trans_loc, lax.axis_index(AXIS) * bs, bs, axis=0)
        return ll[0], post, diag.astype(F32) * pair_sum

    return jax.shard_map(
        local_run,
        mesh=mesh,
        in_specs=(P(None, AXIS), P(AXIS, None), P(AXIS), P("seqs", None), P("seqs")),
        out_specs=(P("seqs"), P("seqs", AXIS), P(("seqs", AXIS), None)),
        check_vma=False,
    )
```

```python
import functools
import math

import jax
import jax.numpy as jnp
from jax import lax
from jax.experimental import pallas as pl
from jax.experimental.pallas import tpu as pltpu
from jax.sharding import PartitionSpec as P

AXIS = "states"
LANES = 128
F32 = jnp.float32
BF16 = jnp.bfloat16


def _loop(n, body):
    def step(i, carry):
        body(i)
        return carry

    lax.fori_loop(0, n, step, 0)


def _recursion(caps, a_hbm, em_hbm, pi_ref, lcol_ref, lrow_ref, al_hbm, w_hbm, post_hbm, ll_ref,
               held, ring, al, acc, cur, emv, rcs, sbuf, csend, cbuf, wv, ost, sst, own, dbuf, trans, fin,
               held_sem, ring_sem, em_sem, al_recv, own_send, part_send, on_send, c_send, c_recv, save_sem, post_sem,
               d_send, d_recv, s_send, t_recv, f_recv):
    nd = cbuf.shape[0]
    nx = nd // 2
    step_count, seqs, bs = em_hbm.shape
    hb = bs // 2
    slab = min(512, hb)
    tiles = bs // LANES
    kept = max(caps[1:])
    g = lax.axis_index(AXIS)
    x, c = g // 2, g % 2

    def dev(dx, flip):
        return ((x + dx) % nx) * 2 + (c + flip) % 2

    partner, right, left = dev(0, 1), dev(1, 0), dev(nx - 1, 0)

    def remote(src, dst, send, recv, to):
        return pltpu.make_async_remote_copy(
            src_ref=src, dst_ref=dst, send_sem=send, recv_sem=recv,
            device_id={AXIS: to}, device_id_type=pl.DeviceIdType.MESH)

    def for_caps(t, fn, first=1):
        if len(set(caps)) == 1:
            fn(caps[0])
            return
        for tt in range(first, step_count):
            pl.when(t == tt)(functools.partial(fn, caps[tt - 1]))

    def fwd_row(group, i):
        if group == 0:
            src, half = dev(0, i // 2), i % 2
        elif group == 3:
            src, half = dev(2, i // 2), i % 2
        else:
            src, half = dev(nx - 1 - 2 * (i % 2), i // 2), (group - 1 + i % 2) % 2
        return src * bs + half * hb

    def bwd_row(group, i):
        q, flip = i // 2, 1 - i % 2
        if group == 0:
            src, half = dev(2, flip), q
        elif group == 3:
            src, half = dev(0, flip), q
        else:
            src, half = dev(1 + 2 * q, flip), (1 - q if group == 1 else q)
        return src * bs + half * hb

    def tile_copy(row, slot):
        return pltpu.make_async_copy(a_hbm.at[pl.ds(pl.multiple_of(row, hb), hb)], ring.at[slot], ring_sem.at[slot])

    def held_copy(i):
        return pltpu.make_async_copy(a_hbm.at[pl.ds(pl.multiple_of(fwd_row(0, i), hb), hb)], held.at[i], held_sem.at[i])

    def em_copy(t):
        return pltpu.make_async_copy(em_hbm.at[t], emv.at[t % 2], em_sem.at[t % 2])

    em_copy(0).start()
    em_copy(1).start()
    _loop(4, lambda i: held_copy(i).start())
    _loop(4, lambda i: tile_copy(fwd_row(1, i), i).start())

    barrier = pltpu.get_barrier_semaphore()
    for k in range(1, nd):
        pl.semaphore_signal(barrier, inc=1, device_id={AXIS: (g + k) % nd}, device_id_type=pl.DeviceIdType.MESH)
    pl.semaphore_wait(barrier, nd - 1)

    def rows_of(i):
        return pl.ds(pl.multiple_of(i * 16, 16), 16)

    def lane(k):
        return pl.ds(k * LANES, LANES)

    def inner(k):
        return (k * LANES) // hb, pl.ds((k * LANES) % hb, LANES)

    def weigh(t, first):
        def body(i):
            r = rows_of(i)
            total = jnp.zeros((16, LANES), F32)
            for k in range(tiles):
                e = emv[t % 2, r, lane(k)].astype(F32)
                mass = (pi_ref[:, lane(k)] * e) if first else acc[r, lane(k)] * e
                acc[r, lane(k)] = mass
                total = total + mass
            sbuf[r, :] = total

        _loop(seqs // 16, body)

    def normalise(t):
        row = jnp.sum(jnp.transpose(sbuf[...]), axis=0, keepdims=True)
        wide = jnp.broadcast_to(row, csend.shape)
        csend[...] = wide
        cbuf[g] = wide
        copies = [remote(csend, cbuf.at[g], c_send.at[k - 1], c_recv.at[g], (g + k) % nd) for k in range(1, nd)]
        for cp in copies:
            cp.start()
        for k in range(1, nd):
            frm = (g + k) % nd
            remote(csend, cbuf.at[frm], c_send.at[k - 1], c_recv.at[frm], frm).wait_recv()
        norm = cbuf[0, 0:1, :]
        for d in range(1, nd):
            norm = norm + cbuf[d, 0:1, :]
        rcs[t] = 1.0 / jnp.transpose(jnp.broadcast_to(norm, (LANES, LANES)))
        ll_ref[...] = ll_ref[...] + jnp.where(t < lrow_ref[...], jnp.log(jnp.broadcast_to(norm, ll_ref.shape)), 0.0)

        def body(i):
            r = rows_of(i)
            rc = rcs[t, r, :]
            live = t < lcol_ref[r, :]
            for k in range(tiles):
                h, col = inner(k)
                val = jnp.where(live, acc[r, lane(k)] * rc, cur[r, lane(k)])
                cur[r, lane(k)] = val
                al[0, h, r, col] = val.astype(BF16)

        _loop(seqs // 16, body)
        for cp in copies:
            cp.wait_send()

    ll_ref[...] = jnp.zeros_like(ll_ref)
    em_copy(0).wait()
    weigh(0, True)
    normalise(0)

    def own_copies(rows):
        m = pl.ds(0, rows)
        out = [remote(al.at[0, h, m], al.at[1, h, m], own_send.at[0, h], al_recv.at[1, h], partner) for h in (0, 1)]
        for h in (0, 1):
            out.append(remote(al.at[0, h, m], al.at[2, h, m], own_send.at[1, h], al_recv.at[2, h], right))
            out.append(remote(al.at[0, 1 - h, m], al.at[3, 1 - h, m], own_send.at[2, 1 - h], al_recv.at[3, 1 - h], left))
        return out

    def to_partner(slot, to_slot, half, rows):
        m = pl.ds(0, rows)
        return remote(al.at[slot, half, m], al.at[to_slot, half, m], part_send.at[slot, half], al_recv.at[to_slot, half], partner)

    def onward(s, rows):
        m = pl.ds(0, rows)
        return remote(al.at[2 + s, s, m], al.at[6, s, m], on_send.at[s], al_recv.at[6, s], dev(1 + (nx - 2) * s, 0))

    def arrived(slot, half, rows):
        m = pl.ds(0, rows)
        remote(al.at[slot, half, m], al.at[slot, half, m], part_send.at[slot, half], al_recv.at[slot, half], partner).wait_recv()

    def save_copies(t):
        return [pltpu.make_async_copy(al.at[0, h], al_hbm.at[t, :, pl.ds(h * hb, hb)], save_sem.at[h]) for h in (0, 1)]

    def multiply(slot, half, tile):
        lhs = al[slot, half]
        for n in range(bs // slab):
            cols = pl.ds(n * slab, slab)
            acc[:, cols] = acc[:, cols] + jnp.dot(lhs, tile[:, cols], preferred_element_type=F32)

    def next_pass(t, i):
        @pl.when(t < step_count - 1)
        def _():
            tile_copy(fwd_row(1, i), i).start()

        @pl.when(t == step_count - 1)
        def _():
            tile_copy(bwd_row(0, i), i).start()

    def forward(idx):
        t = idx + 1
        for_caps(t, lambda rows: [cp.start() for cp in own_copies(rows)] and None)
        for cp in save_copies(t - 1):
            cp.start()

        @pl.when(t + 1 < step_count)
        def _():
            em_copy(t + 1).start()

        acc[...] = jnp.zeros_like(acc)

        def group0(i):
            slot, half = i // 2, i % 2
            pl.when(i >= 2)(lambda: for_caps(t, lambda rows: arrived(1, half, rows)))
            pl.when(t == 1)(lambda: held_copy(i).wait())
            multiply(slot, half, held.at[i])

        def group12(i, k):
            slot, half = 2 + i, (k + i % 2) % 2
            for_caps(t, lambda rows: arrived(slot, half, rows))

            @pl.when(i < 2)
            def _():
                def send(rows):
                    to_partner(slot, slot + 2, half, rows).start()
                    if k == 0:
                        onward(i, rows).start()

                for_caps(t, send)

            tile_copy(0, i).wait()
            multiply(slot, half, ring.at[i])
            tile_copy(fwd_row(2 + k, i), i).start()

        def group3(i):
            slot, half = 6 + i // 2, i % 2

            def ready(rows):
                arrived(slot, half, rows)
                pl.when(i < 2)(lambda: to_partner(6, 7, half, rows).start())

            for_caps(t, ready)
            tile_copy(0, i).wait()
            multiply(slot, half, ring.at[i])
            next_pass(t, i)

        _loop(4, group0)
        _loop(4, lambda i: group12(i, 0))
        _loop(4, lambda i: group12(i, 1))
        _loop(4, group3)

        def drained(rows):
            for cp in own_copies(rows):
                cp.wait_send()
            for half in (0, 1):
                to_partner(2, 4, half, rows).wait_send()
                to_partner(3, 5, half, rows).wait_send()
                to_partner(6, 7, half, rows).wait_send()
                onward(half, rows).wait_send()

        for_caps(t, drained)
        for cp in save_copies(t - 1):
            cp.wait()
        em_copy(t).wait()
        weigh(t, False)
        normalise(t)

    _loop(step_count - 1, forward)

    post_copy = pltpu.make_async_copy(cur, post_hbm, post_sem)
    post_copy.start()

    def weights(t):
        def body(i):
            r = rows_of(i)
            rc = rcs[t, r, :]
            live = t < lcol_ref[r, :]
            for k in range(tiles):
                h, col = inner(k)
                val = emv[t % 2, r, lane(k)].astype(F32) * own[h, r, col] * rc
                wv[r, lane(k)] = jnp.where(live, val, 0.0).astype(BF16)

        _loop(seqs // 16, body)

    def w_copy(t):
        return pltpu.make_async_copy(wv, w_hbm.at[t - 1], save_sem.at[0])

    def partial_sums(out, tile):
        for n in range(hb // slab):
            rows = pl.ds(n * slab, slab)
            out[0:kept, rows] = lax.dot_general(
                wv[0:kept, :], tile[rows, :], (((1,), (1,)), ((), ())), preferred_element_type=F32)

    def add_into(out, *terms):
        def body(i):
            r = pl.ds(pl.multiple_of(i * 8, 8), 8)
            val = out[r, :]
            for term in terms:
                val = val + term[r, :]
            out[r, :] = val

        _loop(kept // 8, body)

    def to_core(p, q, rows):
        m = pl.ds(0, rows)
        return remote(ost.at[q, m], dbuf.at[p, m], d_send.at[q], d_recv.at[p], partner)

    def ring_copy(t, stage, q, rows):
        m, par, to = pl.ds(0, rows), t % 2, dev(1 + (nx - 2) * q, 0)
        if stage == 0:
            return remote(sst.at[q, m], trans.at[par, q, m], s_send.at[q], t_recv.at[par, q], to)
        half = 1 - q if stage == 1 else q
        p = stage * 2 + q
        return remote(sst.at[p, m], fin.at[par, q, half, m], s_send.at[p], f_recv.at[par, q, half], to)

    def backward(idx):
        t = step_count - 1 - idx
        par = t % 2
        weights(t)
        w_copy(t).start()

        @pl.when(t > 2)
        def _():
            em_copy(t - 2).start()

        def stage(n):
            def pair(q):
                p = n * 2 + q
                buf = 2 * q
                if n > 0:
                    for_caps(t, lambda rows: to_core(p, q, rows).wait_send(), 2)
                if n < 3:
                    tile_copy(0, buf).wait()
                    partial_sums(ost.at[q], ring.at[buf])
                else:
                    partial_sums(ost.at[q], held.at[2 + q])
                for_caps(t, lambda rows: to_core(p, q, rows).start(), 2)

                def refill(i):
                    row = bwd_row((n + 1) % 3, buf + i)
                    if n < 2:
                        tile_copy(row, buf + i).start()
                    elif n == 2:
                        pl.when(t > 2)(lambda: tile_copy(row, buf + i).start())

                refill(0)
                out = own.at[q] if n == 3 else sst.at[p]
                if n < 3:
                    tile_copy(0, buf + 1).wait()
                    partial_sums(out, ring.at[buf + 1])
                else:
                    partial_sums(out, held.at[q])
                refill(1)
                for_caps(t, lambda rows: to_core(p, q, rows).wait_recv(), 2)
                if n == 2:
                    for_caps(t, lambda rows: ring_copy(t, 0, q, rows).wait_recv(), 2)
                    add_into(out, dbuf.at[p], trans.at[par, q])
                else:
                    add_into(out, dbuf.at[p])
                if n < 3:
                    for_caps(t, lambda rows: ring_copy(t, n, q, rows).start(), 2)

            _loop(2, pair)

        for n in range(4):
            stage(n)

        def landed(rows):
            for n in (1, 2):
                for q in (0, 1):
                    ring_copy(t, n, q, rows).wait_recv()

        for_caps(t, landed, 2)

        def body(i):
            r = pl.ds(pl.multiple_of(i * 8, 8), 8)
            live = t < lcol_ref[r, :]
            for k in range(tiles):
                h, col = inner(k)
                val = own[h, r, col] + fin[par, 0, h, r, col] + fin[par, 1, h, r, col]
                own[h, r, col] = jnp.where(live, val, 1.0)

        _loop(kept // 8, body)

        def drained(rows):
            for q in (0, 1):
                to_core(6 + q, q, rows).wait_send()
                for n in range(3):
                    ring_copy(t, n, q, rows).wait_send()

        for_caps(t, drained, 2)
        w_copy(t).wait()

        @pl.when(t > 2)
        def _():
            em_copy(t - 2).wait()

    own[...] = jnp.ones_like(own)
    _loop(step_count - 2, backward)
    weights(1)
    w_copy(1).start()
    w_copy(1).wait()
    post_copy.wait()


def _run_recursion(nd, caps, ident, trans_loc, em, init_loc, lengths):
    step_count, seqs, bs = em.shape
    hb = bs // 2
    kept = max(caps[1:])
    dma = pltpu.SemaphoreType.DMA
    lcol = jnp.broadcast_to(lengths[:, None], (seqs, LANES))
    lrow = jnp.broadcast_to(lengths[None, :], (8, seqs))
    vm, hbm = pl.BlockSpec(memory_space=pltpu.VMEM), pl.BlockSpec(memory_space=pl.ANY)
    scratch = [
        pltpu.VMEM((4, hb, bs), BF16),
        pltpu.VMEM((4, hb, bs), BF16),
        pltpu.VMEM((8, 2, seqs, hb), BF16),
        pltpu.VMEM((seqs, bs), F32),
        pltpu.VMEM((seqs, bs), F32),
        pltpu.VMEM((2, seqs, bs), BF16),
        pltpu.VMEM((step_count, seqs, LANES), F32),
        pltpu.VMEM((seqs, LANES), F32),
        pltpu.VMEM((8, seqs), F32),
        pltpu.VMEM((nd, 8, seqs), F32),
        pltpu.VMEM((seqs, bs), BF16),
        pltpu.VMEM((2, kept, hb), F32),
        pltpu.VMEM((6, kept, hb), F32),
        pltpu.VMEM((2, seqs, hb), F32),
        pltpu.VMEM((8, kept, hb), F32),
        pltpu.VMEM((2, 2, kept, hb), F32),
        pltpu.VMEM((2, 2, 2, kept, hb), F32),
        dma((4,)), dma((4,)), dma((2,)), dma((8, 2)), dma((3, 2)), dma((8, 2)), dma((2,)), dma((nd,)), dma((nd,)), dma((2,)), dma,
        dma((2,)), dma((8,)), dma((6,)), dma((2, 2)), dma((2, 2, 2)),
    ]
    return pl.pallas_call(
        functools.partial(_recursion, caps),
        name=f"recursion{ident}",
        out_shape=[
            jax.ShapeDtypeStruct((step_count - 1, seqs, bs), BF16),
            jax.ShapeDtypeStruct((step_count - 1, seqs, bs), BF16),
            jax.ShapeDtypeStruct((seqs, bs), F32),
            jax.ShapeDtypeStruct((8, seqs), F32),
        ],
        in_specs=[hbm, hbm, vm, vm, vm],
        out_specs=[hbm, hbm, hbm, vm],
        scratch_shapes=scratch,
        compiler_params=pltpu.CompilerParams(collective_id=ident, has_side_effects=True, vmem_limit_bytes=66_000_000),
    )(trans_loc, em, init_loc[None, :], lcol, lrow)


def _capacities(seqs, step_count):
    caps = []
    for t in range(1, step_count):
        live = (step_count - t) / step_count
        room = 3.1 * math.sqrt((seqs - 1) * live * (1 - live))
        caps.append(min(seqs, 8 * math.ceil(((seqs - 1) * live + 1 + room) / 8)))
    return tuple(caps)


def solution(mesh):
    nd = mesh.shape[AXIS]

    def local_run(trans_loc, emit_loc, init_loc, tokens_loc, lengths_loc):
        seqs, step_count = tokens_loc.shape
        bs = trans_loc.shape[1]
        ids = jnp.arange(seqs)
        ahead = (lengths_loc[:, None] > lengths_loc[None, :]) | (
            (lengths_loc[:, None] == lengths_loc[None, :]) & (ids[:, None] < ids[None, :]))
        rank = jnp.sum(ahead.astype(jnp.int32), axis=0)
        pick = (rank[None, :] == ids[:, None]).astype(jnp.int32)
        tokens = jnp.sum(pick[:, :, None] * tokens_loc[None, :, :], axis=1)
        lengths = jnp.sum(pick * lengths_loc[None, :], axis=1)

        em = jnp.take(emit_loc.T, tokens.T.reshape(-1), axis=0, mode="clip").reshape(step_count, seqs, bs)
        caps = _capacities(seqs, step_count)
        fits = True
        for t in range(1, step_count):
            fits = fits & (jnp.sum((lengths_loc > t).astype(jnp.int32)) <= caps[t - 1])
        alphas, ws, post, ll = lax.cond(
            fits,
            functools.partial(_run_recursion, nd, caps, 0),
            functools.partial(_run_recursion, nd, (seqs,) * (step_count - 1), 1),
            trans_loc, em, init_loc, lengths)
        pair_sum = lax.dot_general(alphas.reshape(-1, bs), ws.reshape(-1, bs), (((0,), (0,)), ((), ())), preferred_element_type=F32)
        diag = lax.dynamic_slice_in_dim(trans_loc, lax.axis_index(AXIS) * bs, bs, axis=0)
        loglik = jnp.sum(pick.astype(F32) * ll[0][:, None], axis=0)
        return loglik, jnp.take(post, rank, axis=0, mode="clip"), diag.astype(F32) * pair_sum

    return jax.shard_map(
        local_run,
        mesh=mesh,
        in_specs=(P(None, AXIS), P(AXIS, None), P(AXIS), P("seqs", None), P("seqs")),
        out_specs=(P("seqs"), P("seqs", AXIS), P(("seqs", AXIS), None)),
        check_vma=False,
    )
```

```python
import functools
import math

import jax
import jax.numpy as jnp
from jax import lax
from jax.experimental import pallas as pl
from jax.experimental.pallas import tpu as pltpu
from jax.sharding import PartitionSpec as P

AXIS = "states"
LANES = 128
F32 = jnp.float32
BF16 = jnp.bfloat16


def _loop(n, body):
    def step(i, carry):
        body(i)
        return carry

    lax.fori_loop(0, n, step, 0)


def _recursion(caps, a_hbm, em_hbm, pi_ref, lcol_ref, lrow_ref, al_hbm, w_hbm, post_hbm, ll_ref,
               held, ring, al, acc, cur, emv, rcs, sbuf, csend, cbuf, wv, ost, sst, own, dbuf, trans, fin,
               held_sem, ring_sem, em_sem, al_recv, own_send, part_send, on_send, c_send, c_recv, save_sem, post_sem,
               d_send, d_recv, s_send, t_recv, f_recv):
    nd = cbuf.shape[0]
    nx = nd // 2
    step_count, seqs, bs = em_hbm.shape
    hb = bs // 2
    firsts = [sum(caps[:t]) for t in range(step_count)]
    slab = min(512, hb)
    tiles = bs // LANES
    kept = max(caps[1:])
    g = lax.axis_index(AXIS)
    x, c = g // 2, g % 2

    def dev(dx, flip):
        return ((x + dx) % nx) * 2 + (c + flip) % 2

    partner, right, left = dev(0, 1), dev(1, 0), dev(nx - 1, 0)

    def remote(src, dst, send, recv, to):
        return pltpu.make_async_remote_copy(
            src_ref=src, dst_ref=dst, send_sem=send, recv_sem=recv,
            device_id={AXIS: to}, device_id_type=pl.DeviceIdType.MESH)

    def for_each(t, fn):
        for tt in range(1, step_count):
            pl.when(t == tt)(functools.partial(fn, tt, caps[tt - 1]))

    def for_caps(t, fn, first=1):
        if len(set(caps)) == 1:
            fn(caps[0])
            return
        for tt in range(first, step_count):
            pl.when(t == tt)(functools.partial(fn, caps[tt - 1]))

    def fwd_row(group, i):
        if group == 0:
            src, half = dev(0, i // 2), i % 2
        elif group == 3:
            src, half = dev(2, i // 2), i % 2
        else:
            src, half = dev(nx - 1 - 2 * (i % 2), i // 2), (group - 1 + i % 2) % 2
        return src * bs + half * hb

    def bwd_row(group, i):
        q, flip = i // 2, 1 - i % 2
        if group == 0:
            src, half = dev(2, flip), q
        elif group == 3:
            src, half = dev(0, flip), q
        else:
            src, half = dev(1 + 2 * q, flip), (1 - q if group == 1 else q)
        return src * bs + half * hb

    def tile_copy(row, slot):
        return pltpu.make_async_copy(a_hbm.at[pl.ds(pl.multiple_of(row, hb), hb)], ring.at[slot], ring_sem.at[slot])

    def held_copy(i):
        return pltpu.make_async_copy(a_hbm.at[pl.ds(pl.multiple_of(fwd_row(0, i), hb), hb)], held.at[i], held_sem.at[i])

    def em_copy(t):
        return pltpu.make_async_copy(em_hbm.at[t], emv.at[t % 2], em_sem.at[t % 2])

    em_copy(0).start()
    em_copy(1).start()
    _loop(4, lambda i: held_copy(i).start())
    _loop(4, lambda i: tile_copy(fwd_row(1, i), i).start())

    barrier = pltpu.get_barrier_semaphore()
    for k in range(1, nd):
        pl.semaphore_signal(barrier, inc=1, device_id={AXIS: (g + k) % nd}, device_id_type=pl.DeviceIdType.MESH)
    pl.semaphore_wait(barrier, nd - 1)

    def rows_of(i):
        return pl.ds(pl.multiple_of(i * 16, 16), 16)

    def lane(k):
        return pl.ds(k * LANES, LANES)

    def inner(k):
        return (k * LANES) // hb, pl.ds((k * LANES) % hb, LANES)

    def weigh(t, first):
        def body(i):
            r = rows_of(i)
            total = jnp.zeros((16, LANES), F32)
            for k in range(tiles):
                e = emv[t % 2, r, lane(k)].astype(F32)
                mass = (pi_ref[:, lane(k)] * e) if first else acc[r, lane(k)] * e
                acc[r, lane(k)] = mass
                total = total + mass
            sbuf[r, :] = total

        _loop(seqs // 16, body)

    def normalise(t):
        row = jnp.sum(jnp.transpose(sbuf[...]), axis=0, keepdims=True)
        wide = jnp.broadcast_to(row, csend.shape)
        csend[...] = wide
        cbuf[g] = wide
        copies = [remote(csend, cbuf.at[g], c_send.at[k - 1], c_recv.at[g], (g + k) % nd) for k in range(1, nd)]
        for cp in copies:
            cp.start()
        for k in range(1, nd):
            frm = (g + k) % nd
            remote(csend, cbuf.at[frm], c_send.at[k - 1], c_recv.at[frm], frm).wait_recv()
        norm = cbuf[0, 0:1, :]
        for d in range(1, nd):
            norm = norm + cbuf[d, 0:1, :]
        rcs[t] = 1.0 / jnp.transpose(jnp.broadcast_to(norm, (LANES, LANES)))
        ll_ref[...] = ll_ref[...] + jnp.where(t < lrow_ref[...], jnp.log(jnp.broadcast_to(norm, ll_ref.shape)), 0.0)

        def body(i):
            r = rows_of(i)
            rc = rcs[t, r, :]
            live = t < lcol_ref[r, :]
            for k in range(tiles):
                h, col = inner(k)
                val = jnp.where(live, acc[r, lane(k)] * rc, cur[r, lane(k)])
                cur[r, lane(k)] = val
                al[0, h, r, col] = val.astype(BF16)

        _loop(seqs // 16, body)
        for cp in copies:
            cp.wait_send()

    ll_ref[...] = jnp.zeros_like(ll_ref)
    em_copy(0).wait()
    weigh(0, True)
    normalise(0)

    def own_copies(rows):
        m = pl.ds(0, rows)
        out = [remote(al.at[0, h, m], al.at[1, h, m], own_send.at[0, h], al_recv.at[1, h], partner) for h in (0, 1)]
        for h in (0, 1):
            out.append(remote(al.at[0, h, m], al.at[2, h, m], own_send.at[1, h], al_recv.at[2, h], right))
            out.append(remote(al.at[0, 1 - h, m], al.at[3, 1 - h, m], own_send.at[2, 1 - h], al_recv.at[3, 1 - h], left))
        return out

    def to_partner(slot, to_slot, half, rows):
        m = pl.ds(0, rows)
        return remote(al.at[slot, half, m], al.at[to_slot, half, m], part_send.at[slot, half], al_recv.at[to_slot, half], partner)

    def onward(s, rows):
        m = pl.ds(0, rows)
        return remote(al.at[2 + s, s, m], al.at[6, s, m], on_send.at[s], al_recv.at[6, s], dev(1 + (nx - 2) * s, 0))

    def arrived(slot, half, rows):
        m = pl.ds(0, rows)
        remote(al.at[slot, half, m], al.at[slot, half, m], part_send.at[slot, half], al_recv.at[slot, half], partner).wait_recv()

    def save_copies(t, rows):
        to = pl.ds(firsts[t - 1], rows)
        return [pltpu.make_async_copy(al.at[0, h, pl.ds(0, rows)], al_hbm.at[to, pl.ds(h * hb, hb)], save_sem.at[h])
                for h in (0, 1)]

    def multiply(slot, half, tile):
        lhs = al[slot, half]
        for n in range(bs // slab):
            cols = pl.ds(n * slab, slab)
            acc[:, cols] = acc[:, cols] + jnp.dot(lhs, tile[:, cols], preferred_element_type=F32)

    def next_pass(t, i):
        @pl.when(t < step_count - 1)
        def _():
            tile_copy(fwd_row(1, i), i).start()

        @pl.when(t == step_count - 1)
        def _():
            tile_copy(bwd_row(0, i), i).start()

    def forward(idx):
        t = idx + 1
        for_caps(t, lambda rows: [cp.start() for cp in own_copies(rows)] and None)
        for_each(t, lambda tt, rows: [cp.start() for cp in save_copies(tt, rows)] and None)

        @pl.when(t + 1 < step_count)
        def _():
            em_copy(t + 1).start()

        acc[...] = jnp.zeros_like(acc)

        def group0(i):
            slot, half = i // 2, i % 2
            pl.when(i >= 2)(lambda: for_caps(t, lambda rows: arrived(1, half, rows)))
            pl.when(t == 1)(lambda: held_copy(i).wait())
            multiply(slot, half, held.at[i])

        def group12(i, k):
            slot, half = 2 + i, (k + i % 2) % 2
            for_caps(t, lambda rows: arrived(slot, half, rows))

            @pl.when(i < 2)
            def _():
                def send(rows):
                    to_partner(slot, slot + 2, half, rows).start()
                    if k == 0:
                        onward(i, rows).start()

                for_caps(t, send)

            tile_copy(0, i).wait()
            multiply(slot, half, ring.at[i])
            tile_copy(fwd_row(2 + k, i), i).start()

        def group3(i):
            slot, half = 6 + i // 2, i % 2

            def ready(rows):
                arrived(slot, half, rows)
                pl.when(i < 2)(lambda: to_partner(6, 7, half, rows).start())

            for_caps(t, ready)
            tile_copy(0, i).wait()
            multiply(slot, half, ring.at[i])
            next_pass(t, i)

        _loop(4, group0)
        _loop(4, lambda i: group12(i, 0))
        _loop(4, lambda i: group12(i, 1))
        _loop(4, group3)

        def drained(rows):
            for cp in own_copies(rows):
                cp.wait_send()
            for half in (0, 1):
                to_partner(2, 4, half, rows).wait_send()
                to_partner(3, 5, half, rows).wait_send()
                to_partner(6, 7, half, rows).wait_send()
                onward(half, rows).wait_send()

        for_caps(t, drained)
        for_each(t, lambda tt, rows: [cp.wait() for cp in save_copies(tt, rows)] and None)
        em_copy(t).wait()
        weigh(t, False)
        normalise(t)

    _loop(step_count - 1, forward)

    post_copy = pltpu.make_async_copy(cur, post_hbm, post_sem)
    post_copy.start()

    def weights(t):
        def body(i):
            r = rows_of(i)
            rc = rcs[t, r, :]
            live = t < lcol_ref[r, :]
            for k in range(tiles):
                h, col = inner(k)
                val = emv[t % 2, r, lane(k)].astype(F32) * own[h, r, col] * rc
                wv[r, lane(k)] = jnp.where(live, val, 0.0).astype(BF16)

        _loop(seqs // 16, body)

    def w_copy(t, rows):
        return pltpu.make_async_copy(wv.at[pl.ds(0, rows)], w_hbm.at[pl.ds(firsts[t - 1], rows)], save_sem.at[0])

    def partial_sums(out, tile):
        for n in range(hb // slab):
            rows = pl.ds(n * slab, slab)
            out[0:kept, rows] = lax.dot_general(
                wv[0:kept, :], tile[rows, :], (((1,), (1,)), ((), ())), preferred_element_type=F32)

    def add_into(out, *terms):
        def body(i):
            r = pl.ds(pl.multiple_of(i * 8, 8), 8)
            val = out[r, :]
            for term in terms:
                val = val + term[r, :]
            out[r, :] = val

        _loop(kept // 8, body)

    def to_core(p, q, rows):
        m = pl.ds(0, rows)
        return remote(ost.at[q, m], dbuf.at[p, m], d_send.at[q], d_recv.at[p], partner)

    def ring_copy(t, stage, q, rows):
        m, par, to = pl.ds(0, rows), t % 2, dev(1 + (nx - 2) * q, 0)
        if stage == 0:
            return remote(sst.at[q, m], trans.at[par, q, m], s_send.at[q], t_recv.at[par, q], to)
        half = 1 - q if stage == 1 else q
        p = stage * 2 + q
        return remote(sst.at[p, m], fin.at[par, q, half, m], s_send.at[p], f_recv.at[par, q, half], to)

    def backward(idx):
        t = step_count - 1 - idx
        par = t % 2
        weights(t)
        for_each(t, lambda tt, rows: w_copy(tt, rows).start())

        @pl.when(t > 2)
        def _():
            em_copy(t - 2).start()

        def stage(n):
            def pair(q):
                p = n * 2 + q
                buf = 2 * q
                if n > 0:
                    for_caps(t, lambda rows: to_core(p, q, rows).wait_send(), 2)
                if n < 3:
                    tile_copy(0, buf).wait()
                    partial_sums(ost.at[q], ring.at[buf])
                else:
                    partial_sums(ost.at[q], held.at[2 + q])
                for_caps(t, lambda rows: to_core(p, q, rows).start(), 2)

                def refill(i):
                    row = bwd_row((n + 1) % 3, buf + i)
                    if n < 2:
                        tile_copy(row, buf + i).start()
                    elif n == 2:
                        pl.when(t > 2)(lambda: tile_copy(row, buf + i).start())

                refill(0)
                out = own.at[q] if n == 3 else sst.at[p]
                if n < 3:
                    tile_copy(0, buf + 1).wait()
                    partial_sums(out, ring.at[buf + 1])
                else:
                    partial_sums(out, held.at[q])
                refill(1)
                for_caps(t, lambda rows: to_core(p, q, rows).wait_recv(), 2)
                if n == 2:
                    for_caps(t, lambda rows: ring_copy(t, 0, q, rows).wait_recv(), 2)
                    add_into(out, dbuf.at[p], trans.at[par, q])
                else:
                    add_into(out, dbuf.at[p])
                if n < 3:
                    for_caps(t, lambda rows: ring_copy(t, n, q, rows).start(), 2)

            _loop(2, pair)

        for n in range(4):
            stage(n)

        def landed(rows):
            for n in (1, 2):
                for q in (0, 1):
                    ring_copy(t, n, q, rows).wait_recv()

        for_caps(t, landed, 2)

        def body(i):
            r = pl.ds(pl.multiple_of(i * 8, 8), 8)
            live = t < lcol_ref[r, :]
            for k in range(tiles):
                h, col = inner(k)
                val = own[h, r, col] + fin[par, 0, h, r, col] + fin[par, 1, h, r, col]
                own[h, r, col] = jnp.where(live, val, 1.0)

        _loop(kept // 8, body)

        def drained(rows):
            for q in (0, 1):
                to_core(6 + q, q, rows).wait_send()
                for n in range(3):
                    ring_copy(t, n, q, rows).wait_send()

        for_caps(t, drained, 2)
        for_each(t, lambda tt, rows: w_copy(tt, rows).wait())

        @pl.when(t > 2)
        def _():
            em_copy(t - 2).wait()

    own[...] = jnp.ones_like(own)
    _loop(step_count - 2, backward)
    weights(1)
    w_copy(1, caps[0]).start()
    w_copy(1, caps[0]).wait()
    post_copy.wait()


def _run_recursion(nd, caps, ident, trans_loc, em, init_loc, lcol, lrow):
    step_count, seqs, bs = em.shape
    hb = bs // 2
    kept = max(caps[1:])
    dma = pltpu.SemaphoreType.DMA
    vm, hbm = pl.BlockSpec(memory_space=pltpu.VMEM), pl.BlockSpec(memory_space=pl.ANY)
    scratch = [
        pltpu.VMEM((4, hb, bs), BF16),
        pltpu.VMEM((4, hb, bs), BF16),
        pltpu.VMEM((8, 2, seqs, hb), BF16),
        pltpu.VMEM((seqs, bs), F32),
        pltpu.VMEM((seqs, bs), F32),
        pltpu.VMEM((2, seqs, bs), BF16),
        pltpu.VMEM((step_count, seqs, LANES), F32),
        pltpu.VMEM((seqs, LANES), F32),
        pltpu.VMEM((8, seqs), F32),
        pltpu.VMEM((nd, 8, seqs), F32),
        pltpu.VMEM((seqs, bs), BF16),
        pltpu.VMEM((2, kept, hb), F32),
        pltpu.VMEM((6, kept, hb), F32),
        pltpu.VMEM((2, seqs, hb), F32),
        pltpu.VMEM((8, kept, hb), F32),
        pltpu.VMEM((2, 2, kept, hb), F32),
        pltpu.VMEM((2, 2, 2, kept, hb), F32),
        dma((4,)), dma((4,)), dma((2,)), dma((8, 2)), dma((3, 2)), dma((8, 2)), dma((2,)), dma((nd,)), dma((nd,)), dma((2,)), dma,
        dma((2,)), dma((8,)), dma((6,)), dma((2, 2)), dma((2, 2, 2)),
    ]
    return pl.pallas_call(
        functools.partial(_recursion, caps),
        name=f"recursion{ident}",
        out_shape=[
            jax.ShapeDtypeStruct((sum(caps), bs), BF16),
            jax.ShapeDtypeStruct((sum(caps), bs), BF16),
            jax.ShapeDtypeStruct((seqs, bs), F32),
            jax.ShapeDtypeStruct((8, seqs), F32),
        ],
        in_specs=[hbm, hbm, vm, vm, vm],
        out_specs=[hbm, hbm, hbm, vm],
        scratch_shapes=scratch,
        compiler_params=pltpu.CompilerParams(collective_id=ident, has_side_effects=True, vmem_limit_bytes=66_000_000),
    )(trans_loc, em, init_loc[None, :], lcol, lrow)


def _prepare(caps, tok_ref, len_ref, emt_hbm, em_hbm, lcol_ref, lrow_ref, rank_ref, fits_ref,
             table, stable, picked, blocks, stage, table_sem, block_sem, stage_sem):
    step_count, seqs, bs = em_hbm.shape
    deep = blocks.shape[0]
    part = 32
    slab = min(512, bs)
    sub = lax.broadcasted_iota(jnp.int32, (seqs, LANES), 0)
    lan = lax.broadcasted_iota(jnp.int32, (seqs, LANES), 1)
    across = jnp.broadcast_to(len_ref[...].astype(F32), (seqs, seqs))
    down = jnp.transpose(across)
    ahead = (down > across) | ((down == across) & (sub < lan))
    rank = jnp.sum(jnp.where(ahead, 1.0, 0.0), axis=0, keepdims=True)
    rank_ref[...] = jnp.broadcast_to(rank, rank_ref.shape)
    pick = rank == sub.astype(F32)
    lcol = jnp.broadcast_to(jnp.sum(jnp.where(pick, across, 0.0), axis=1, keepdims=True), (seqs, LANES))
    lcol_ref[...] = lcol.astype(jnp.int32)
    lrow_ref[...] = jnp.transpose(lcol)[0:8].astype(jnp.int32)
    mat = jnp.zeros((seqs, LANES), F32)
    for t in range(step_count):
        tok = jnp.sum(jnp.where(pick, tok_ref[t : t + 1, :].astype(F32), 0.0), axis=1, keepdims=True)
        tok = jnp.broadcast_to(tok, (seqs, LANES))
        mat = jnp.where(lan == t, tok, mat)
        picked[t] = tok.astype(jnp.int32) & 7
    table[0:8] = jnp.transpose(mat)[0:8].astype(jnp.int32)
    alive = jnp.sum(jnp.where(across[0:8] > sub[0:8].astype(F32), 1.0, 0.0), axis=1, keepdims=True)
    table[8:16] = jnp.broadcast_to(alive, (8, LANES)).astype(jnp.int32)
    copy = pltpu.make_async_copy(table, stable, table_sem)
    copy.start()
    copy.wait()
    fits = jnp.int32(1)
    for t in range(1, step_count):
        fits = jnp.where(stable[8 + t, 0] > caps[t - 1], 0, fits)
    fits_ref[0] = fits

    def parts(t):
        return (stable[8 + t, 0] + (part - 1)) // part

    def fetch(t):
        def body(p, carry):
            for k in range(part):
                s = p * part + k
                pltpu.make_async_copy(emt_hbm.at[stable[t, s] >> 3], blocks.at[t % deep, s], block_sem.at[t % deep]).start()
            return carry

        lax.fori_loop(0, parts(t), body, 0)

    def landed(t):
        def body(p, carry):
            pltpu.make_async_copy(emt_hbm.at[pl.ds(0, part)], blocks.at[t % deep, pl.ds(0, part)], block_sem.at[t % deep]).wait()
            return carry

        lax.fori_loop(0, parts(t), body, 0)

    def select(t):
        def body(p, carry):
            r = pl.ds(pl.multiple_of(p * part, part), part)
            at = picked[t, r, :] + 8 * sub[0:part]
            one = jnp.concatenate([jnp.where(lan[0:part] + off == at, 1.0, 0.0) for off in (0, LANES)], axis=1).astype(BF16)
            for n in range(bs // slab):
                cols = pl.ds(n * slab, slab)
                rows = blocks[t % deep, r, :, cols].reshape(part * 8, slab)
                stage[t % 2, r, cols] = jnp.dot(one, rows, preferred_element_type=F32).astype(BF16)
            return carry

        lax.fori_loop(0, parts(t), body, 0)

    def out_copy(t):
        return pltpu.make_async_copy(stage.at[t % 2], em_hbm.at[t], stage_sem.at[t % 2])

    for t in range(min(deep, step_count)):
        fetch(t)
    for t in range(step_count):
        if t >= 2:
            out_copy(t - 2).wait()
        landed(t)
        select(t)
        out_copy(t).start()
        if t + deep < step_count:
            fetch(t + deep)
    for t in range(step_count - 2, step_count):
        out_copy(t).wait()


def _run_prepare(caps, tokens, lengths, emit_loc):
    bs, symbols = emit_loc.shape
    seqs, step_count = tokens.shape
    dma = pltpu.SemaphoreType.DMA
    vm, hbm = pl.BlockSpec(memory_space=pltpu.VMEM), pl.BlockSpec(memory_space=pl.ANY)
    return pl.pallas_call(
        functools.partial(_prepare, caps),
        name="prepare",
        out_shape=[
            jax.ShapeDtypeStruct((step_count, seqs, bs), BF16),
            jax.ShapeDtypeStruct((seqs, LANES), jnp.int32),
            jax.ShapeDtypeStruct((8, seqs), jnp.int32),
            jax.ShapeDtypeStruct((8, seqs), F32),
            jax.ShapeDtypeStruct((1,), jnp.int32),
        ],
        in_specs=[vm, vm, hbm],
        out_specs=[hbm, vm, vm, vm, pl.BlockSpec(memory_space=pltpu.SMEM)],
        scratch_shapes=[
            pltpu.VMEM((16, LANES), jnp.int32),
            pltpu.SMEM((16, LANES), jnp.int32),
            pltpu.VMEM((step_count, seqs, LANES), jnp.int32),
            pltpu.VMEM((4, seqs, 8, bs), BF16),
            pltpu.VMEM((2, seqs, bs), BF16),
            dma, dma((4,)), dma((2,)),
        ],
        compiler_params=pltpu.CompilerParams(vmem_limit_bytes=60_000_000),
    )(tokens.T, lengths[None, :], emit_loc.T.reshape(symbols // 8, 8, bs))


def _counts(block_ref, alpha_ref, w_ref, diag_ref, post_ref, ll_ref, rank_ref, counts_ref, posterior_ref, loglik_ref):
    bs = w_ref.shape[1]
    slab = min(512, bs)
    lhs = alpha_ref[...]
    for n in range(bs // slab):
        cols = pl.ds(n * slab, slab)
        sums = lax.dot_general(lhs, w_ref[:, cols], (((0,), (0,)), ((), ())), preferred_element_type=F32)
        counts_ref[:, cols] = diag_ref[:, cols].astype(F32) * sums
    seqs = post_ref.shape[0]
    rank = jnp.broadcast_to(rank_ref[0:1, :], (seqs, seqs))
    sub = lax.broadcasted_iota(jnp.int32, (seqs, seqs), 0).astype(F32)
    lan = lax.broadcasted_iota(jnp.int32, (seqs, seqs), 1).astype(F32)
    back = jnp.where(jnp.transpose(rank) == lan, 1.0, 0.0).astype(BF16)
    rest = post_ref[...]
    total = jnp.zeros(posterior_ref.shape, F32)
    for _ in range(3):
        head = rest.astype(BF16)
        rest = rest - head.astype(F32)
        total = total + jnp.dot(back, head, preferred_element_type=F32)
    posterior_ref[...] = total
    lls = jnp.transpose(jnp.broadcast_to(ll_ref[0:1, :], (seqs, seqs)))
    loglik_ref[...] = jnp.sum(jnp.where(rank == sub, lls, 0.0), axis=0, keepdims=True)


def _run_counts(alphas, ws, trans_loc, post, ll, rank):
    rows, bs = alphas.shape
    seqs = post.shape[0]
    tile = min(256, bs)
    steps = bs // tile
    block = lax.axis_index(AXIS).astype(jnp.int32)[None]
    return pl.pallas_call(
        _counts,
        name="counts",
        out_shape=[
            jax.ShapeDtypeStruct((bs, bs), F32),
            jax.ShapeDtypeStruct((seqs, bs), F32),
            jax.ShapeDtypeStruct((1, seqs), F32),
        ],
        grid_spec=pltpu.PrefetchScalarGridSpec(
            num_scalar_prefetch=1,
            grid=(steps,),
            in_specs=[
                pl.BlockSpec((rows, tile), lambda i, b: (0, i)),
                pl.BlockSpec((rows, bs), lambda i, b: (0, 0)),
                pl.BlockSpec((tile, bs), lambda i, b: (b[0] * steps + i, 0)),
                pl.BlockSpec((seqs, tile), lambda i, b: (0, i)),
                pl.BlockSpec((8, seqs), lambda i, b: (0, 0)),
                pl.BlockSpec((8, seqs), lambda i, b: (0, 0)),
            ],
            out_specs=[
                pl.BlockSpec((tile, bs), lambda i, b: (i, 0)),
                pl.BlockSpec((seqs, tile), lambda i, b: (0, i)),
                pl.BlockSpec((1, seqs), lambda i, b: (0, 0)),
            ],
        ),
        compiler_params=pltpu.CompilerParams(vmem_limit_bytes=60_000_000),
    )(block, alphas, ws, trans_loc, post, ll, rank)


def _capacities(seqs, step_count):
    caps = []
    for t in range(1, step_count):
        live = (step_count - t) / step_count
        room = 3.1 * math.sqrt((seqs - 1) * live * (1 - live))
        caps.append(min(seqs, 8 * math.ceil(((seqs - 1) * live + 1 + room) / 8)))
    return tuple(caps)


def solution(mesh):
    nd = mesh.shape[AXIS]

    def local_run(trans_loc, emit_loc, init_loc, tokens_loc, lengths_loc):
        seqs, step_count = tokens_loc.shape
        caps = _capacities(seqs, step_count)
        em, lcol, lrow, rank, fits = _run_prepare(caps, tokens_loc, lengths_loc, emit_loc)

        def run(caps, ident, trans, em, init, lcol, lrow, rank):
            alphas, ws, post, ll = _run_recursion(nd, caps, ident, trans, em, init, lcol, lrow)
            return _run_counts(alphas, ws, trans, post, ll, rank)

        counts, posterior, loglik = lax.cond(
            fits[0] == 1,
            functools.partial(run, caps, 0),
            functools.partial(run, (seqs,) * (step_count - 1), 1),
            trans_loc, em, init_loc, lcol, lrow, rank)
        return loglik[0], posterior, counts

    return jax.shard_map(
        local_run,
        mesh=mesh,
        in_specs=(P(None, AXIS), P(AXIS, None), P(AXIS), P("seqs", None), P("seqs")),
        out_specs=(P("seqs"), P("seqs", AXIS), P(("seqs", AXIS), None)),
        check_vma=False,
    )
```

```python
import functools
import math

import jax
import jax.numpy as jnp
from jax import lax
from jax.experimental import pallas as pl
from jax.experimental.pallas import tpu as pltpu
from jax.sharding import PartitionSpec as P

AXIS = "states"
LANES = 128
BOTH = (0, 1)
F32 = jnp.float32
BF16 = jnp.bfloat16


def _dot(a, b, over_a=1, over_b=0):
    dims = (((over_a,), (over_b,)), ((), ()))
    return lax.dot_general(a, b, dims, preferred_element_type=F32)


def _start(copies):
    for cp in copies:
        cp.start()


def _wait(copies):
    for cp in copies:
        cp.wait()


def _loop(n, body):
    def step(i, carry):
        body(i)
        return carry

    lax.fori_loop(0, n, step, 0)


def _recursion(caps, a_hbm, em_hbm, pi_ref, lcol_ref, lrow_ref, al_hbm, w_hbm, post_hbm, ll_ref, turned_hbm,
               held, ring, al, acc, cur, emv, rcs, sbuf, csend, cbuf, strips, ost, sst, dbuf, trans, fin,
               held_sem, ring_sem, em_sem, al_recv, own_send, part_send, on_send, c_send, c_recv, save_sem, post_sem,
               strip_sem, d_send, d_recv, s_send, t_recv, f_recv, t_free, f_free):
    nd = cbuf.shape[0]
    nx = nd // 2
    step_count, seqs, bs = em_hbm.shape
    hb = bs // 2
    firsts = [sum(caps[:t]) for t in range(step_count)]
    slab = min(512, hb)
    tiles = bs // LANES
    kept = max(caps[1:])
    sent = pl.ds(0, kept)
    final = step_count - 1
    g = lax.axis_index(AXIS)
    x, c = g // 2, g % 2

    def dev(dx, flip):
        return ((x + dx) % nx) * 2 + (c + flip) % 2

    partner, right, left = dev(0, 1), dev(1, 0), dev(nx - 1, 0)

    def remote(src, dst, send, recv, to):
        return pltpu.make_async_remote_copy(
            src_ref=src, dst_ref=dst, send_sem=send, recv_sem=recv,
            device_id={AXIS: to}, device_id_type=pl.DeviceIdType.MESH)

    def for_each(t, fn):
        for tt in range(1, step_count):
            pl.when(t == tt)(functools.partial(fn, tt, caps[tt - 1]))

    def for_caps(t, fn, first=1):
        if len(set(caps)) == 1:
            fn(caps[0])
            return
        for tt in range(first, step_count):
            pl.when(t == tt)(functools.partial(fn, caps[tt - 1]))

    def tile_row(group, i):
        if group == 0:
            src, half = dev(0, i // 2), i % 2
        elif group == 1:
            src, half = dev(nx - 1, i % 2), i // 2
        elif group == 2:
            src, half = dev(1, i % 2), 1 - i // 2
        else:
            src, half = dev(2, i // 2), i % 2
        return src * bs + half * hb

    def tile_copy(group, i, turned):
        if turned:
            src = turned_hbm.at[pl.ds(pl.multiple_of((4 * group + i) * hb, hb), hb)]
        else:
            src = a_hbm.at[pl.ds(pl.multiple_of(tile_row(group, i), hb), hb)]
        if group in (1, 3):
            at = i + (4 if group == 3 else 0)
            return pltpu.make_async_copy(src, held.at[at], held_sem.at[at])
        return pltpu.make_async_copy(src, ring.at[i], ring_sem.at[i])

    def in_ring(i):
        tile_copy(0, i, True).wait()

    def in_held(at):
        pltpu.make_async_copy(turned_hbm.at[pl.ds(0, hb)], held.at[at], held_sem.at[at]).wait()

    depth = strips.shape[0]

    def strip_copy(number, unit, k):
        rows = pl.ds(pl.multiple_of(number * hb + (unit % (tiles // 2)) * LANES, LANES), LANES)
        cols = pl.ds(pl.multiple_of((unit // (tiles // 2)) * hb, hb), hb)
        return pltpu.make_async_copy(strips.at[k], turned_hbm.at[rows, cols], strip_sem.at[k])

    def turn(buf, first, number):
        def body(i):
            units = [4 * i + e for e in range(4)]

            @pl.when(4 * i >= depth)
            def _():
                for u in units:
                    strip_copy(number, 0, u % depth).wait()

            for u in units:
                cols = pl.ds(pl.multiple_of(u % tiles * LANES, LANES), LANES)
                strips[u % depth] = jnp.transpose(buf[first + u // tiles, :, cols])
            for u in units:
                strip_copy(number + u // tiles, u % tiles, u % depth).start()

        _loop(tiles // 2, body)

    def turn_ends():
        _loop(depth, lambda k: strip_copy(0, 0, k).wait())

    windows = -(-6 // final)

    def turn_some(t):
        for e in range(windows):
            at = t * windows + e
            if e > 0:
                pl.when(at < 6)(turn_ends)
            pl.when(at < 2)(lambda: turn(ring, 2 * at, 2 * at))
            pl.when((at >= 2) & (at < 6))(lambda: turn(held, 2 * at - 4, 2 * at + 4 * (at // 4)))

    def em_copy(t):
        return pltpu.make_async_copy(em_hbm.at[t], emv.at[t % 2], em_sem.at[t % 2])

    _loop(2, lambda t: em_copy(t).start())
    for group in (0, 1, 3):
        _loop(4, lambda i, group=group: tile_copy(group, i, False).start())

    barrier = pltpu.get_barrier_semaphore()
    for k in range(1, nd):
        pl.semaphore_signal(barrier, inc=1, device_id={AXIS: (g + k) % nd}, device_id_type=pl.DeviceIdType.MESH)
    pl.semaphore_wait(barrier, nd - 1)

    def rows_of(i):
        return pl.ds(pl.multiple_of(i * 16, 16), 16)

    def lane(k):
        return pl.ds(k * LANES, LANES)

    def inner(k):
        return (k * LANES) // hb, pl.ds((k * LANES) % hb, LANES)

    def weigh(t):
        def body(i):
            r = rows_of(i)
            total = jnp.zeros((16, LANES), F32)
            for k in range(tiles):
                e = emv[t % 2, r, lane(k)].astype(F32)
                h, col = inner(k)
                mass = acc[h, r, col] * e
                acc[h, r, col] = mass
                total = total + mass
            sbuf[r, :] = total

        _loop(seqs // 16, body)

    def normalise(t):
        row = jnp.sum(jnp.transpose(sbuf[...]), axis=0, keepdims=True)
        wide = jnp.broadcast_to(row, csend.shape)
        csend[...] = wide
        cbuf[g] = wide
        peers = [dev(dx, flip) for dx in (2, 1, nx - 1, 0) for flip in BOTH][: nd - 2] + [partner]
        copies = [remote(csend, cbuf.at[g], c_send.at[k], c_recv.at[g], to) for k, to in enumerate(peers)]
        _start(copies)

        with jax.named_scope("ft"):
            @pl.when(t < final)
            def _():
                _loop(4, in_ring)
                turn_some(t)

        with jax.named_scope("fx"):
            for k, frm in enumerate(peers):
                remote(csend, cbuf.at[frm], c_send.at[k], c_recv.at[frm], frm).wait_recv()
        norm = cbuf[0, 0:1, :]
        for d in range(1, nd):
            norm = norm + cbuf[d, 0:1, :]
        rcs[t] = 1.0 / jnp.transpose(jnp.broadcast_to(norm, (LANES, LANES)))
        ll_ref[...] = ll_ref[...] + jnp.where(t < lrow_ref[...], jnp.log(jnp.broadcast_to(norm, ll_ref.shape)), 0.0)

        def body(i):
            r = rows_of(i)
            rc = rcs[t, r, :]
            live = t < lcol_ref[r, :]
            for k in range(tiles):
                h, col = inner(k)
                val = jnp.where(live, acc[h, r, col] * rc, cur[h, r, col])
                cur[h, r, col] = val
                al[0, h, r, col] = val.astype(BF16)

        _loop(seqs // 16, body)
        for cp in copies:
            cp.wait_send()

    ll_ref[...] = jnp.zeros_like(ll_ref)
    for h in BOTH:
        acc[h] = jnp.broadcast_to(pi_ref[:, h * hb : (h + 1) * hb], (seqs, hb))

    def own_copies(rows):
        m = pl.ds(0, rows)
        out = [remote(al.at[0, h, m], al.at[1, h, m], own_send.at[0, h], al_recv.at[1, h], partner) for h in BOTH]
        for h in BOTH:
            out.append(remote(al.at[0, h, m], al.at[2, h, m], own_send.at[1, h], al_recv.at[2, h], right))
            out.append(remote(al.at[0, 1 - h, m], al.at[3, 1 - h, m], own_send.at[2, 1 - h], al_recv.at[3, 1 - h], left))
        return out

    def to_partner(slot, to_slot, half, rows):
        m = pl.ds(0, rows)
        return remote(al.at[slot, half, m], al.at[to_slot, half, m], part_send.at[slot, half], al_recv.at[to_slot, half], partner)

    def onward(s, rows):
        m = pl.ds(0, rows)
        return remote(al.at[2 + s, s, m], al.at[6, s, m], on_send.at[s], al_recv.at[6, s], dev(1 + (nx - 2) * s, 0))

    def arrived(slot, half, rows):
        m = pl.ds(0, rows)
        remote(al.at[slot, half, m], al.at[slot, half, m], part_send.at[slot, half], al_recv.at[slot, half], partner).wait_recv()

    def save_copies(t, rows):
        to = pl.ds(firsts[t - 1], rows)
        return [pltpu.make_async_copy(al.at[0, h, pl.ds(0, rows)], al_hbm.at[to, pl.ds(h * hb, hb)], save_sem.at[h])
                for h in BOTH]

    def multiply(one, two):
        (slot1, half1, tile1), (slot2, half2, tile2) = one, two
        lhs1, lhs2 = al[slot1, half1], al[slot2, half2]
        for h in BOTH:
            for n in range(hb // slab):
                cols, at = pl.ds(h * hb + n * slab, slab), pl.ds(n * slab, slab)
                acc[h, :, at] = acc[h, :, at] + (
                    _dot(lhs1, tile1[:, cols]) + _dot(lhs2, tile2[:, cols]))

    def forward(t):
        pl.when(t > 0)(lambda: predict(t))
        em_copy(t).wait()
        with jax.named_scope("fw"):
            weigh(t)
        normalise(t)

    def predict(t):
        for_caps(t, lambda rows: _start(own_copies(rows)))
        for_each(t, lambda tt, rows: _start(save_copies(tt, rows)))

        @pl.when(t + 1 < step_count)
        def _():
            em_copy(t + 1).start()

        acc[...] = jnp.zeros_like(acc)

        def group0(j):
            def ready(rows):
                for half in BOTH:
                    arrived(1, half, rows)

            pl.when(j > 0)(lambda: for_caps(t, ready))
            multiply(*((j, e, ring.at[2 * j + e]) for e in BOTH))
            for e in BOTH:
                tile_copy(2, 2 * j + e, False).start()

        def group12(k, j):
            def ready(rows):
                arrived(2 + 2 * j, k, rows)
                arrived(3 + 2 * j, 1 - k, rows)

                @pl.when(j == 0)
                def _():
                    to_partner(2, 4, k, rows).start()
                    to_partner(3, 5, 1 - k, rows).start()

                pl.when(k + j == 0)(lambda: _start([onward(0, rows), onward(1, rows)]))

            for_caps(t, ready)
            at = 2 * k + j
            in_ring(at)
            pl.when(t == 1)(lambda: in_held(at))
            multiply((2 + 2 * j, k, held.at[at]), (3 + 2 * j, 1 - k, ring.at[at]))

        def turn_right(k):
            @pl.when(t == 1)
            def _():
                turn_ends()
                turn(ring, 2 * k, 8 + 2 * k)

        def next_tiles(k):
            @pl.when(t < final)
            def _():
                _loop(2, lambda e: tile_copy(0, 2 * k + e, False).start())

            @pl.when(t == final)
            def _():
                for e in BOTH:
                    tile_copy(2, 2 * k + e, True).start()
                    tile_copy(1, 2 * k + e, True).start()

        def group3(j):
            def ready(rows):
                for half in BOTH:
                    arrived(6 + j, half, rows)

                @pl.when(j == 0)
                def _():
                    for half in BOTH:
                        to_partner(6, 7, half, rows).start()

            for_caps(t, ready)
            pl.when(t == 1)(lambda: _loop(2, lambda e: in_held(4 + 2 * j + e)))
            multiply(*((6 + j, e, held.at[4 + 2 * j + e]) for e in BOTH))

        with jax.named_scope("f0"):
            _loop(2, group0)
        pl.when((t >= 2) & ((t - 1) * windows < 6))(turn_ends)

        def groups12(k):
            with jax.named_scope("f1"):
                _loop(2, functools.partial(group12, k))
            with jax.named_scope("fr"):
                turn_right(k)
            next_tiles(k)

        _loop(2, groups12)
        with jax.named_scope("f3"):
            _loop(2, group3)
        pl.when(t == 1)(turn_ends)

        @pl.when(t == final)
        def _():
            _loop(4, lambda i: tile_copy(3, i, True).start())

        def drained(rows):
            for cp in own_copies(rows):
                cp.wait_send()
            for half in BOTH:
                to_partner(2, 4, half, rows).wait_send()
                to_partner(3, 5, half, rows).wait_send()
                to_partner(6, 7, half, rows).wait_send()
                onward(half, rows).wait_send()

        for_caps(t, drained)
        for_each(t, lambda tt, rows: _wait(save_copies(tt, rows)))

    _loop(step_count, forward)

    def post_copy(h):
        return pltpu.make_async_copy(cur.at[h], post_hbm.at[:, pl.ds(pl.multiple_of(h * hb, hb), hb)], post_sem.at[h])

    _loop(2, lambda h: post_copy(h).start())

    back_caps = functools.partial(for_caps, first=2)

    def weights(t):
        def body(i):
            r = rows_of(i)
            rc = rcs[t, r, :]
            live = t < lcol_ref[r, :]
            for k in range(tiles):
                h, col = inner(k)
                val = emv[t % 2, r, lane(k)].astype(F32) * acc[h, r, col] * rc
                strips[h, r, col] = jnp.where(live, val, 0.0).astype(BF16)

        _loop(seqs // 16, body)

    def w_copies(t, rows):
        to = pl.ds(firsts[t - 1], rows)
        return [pltpu.make_async_copy(strips.at[h, pl.ds(0, rows)], w_hbm.at[to, pl.ds(h * hb, hb)], save_sem.at[h])
                for h in BOTH]

    def partial_sums(out, tile):
        for n in range(hb // slab):
            cols = pl.ds(n * slab, slab)
            more = pl.ds(hb + n * slab, slab)
            out[sent, cols] = _dot(strips[0, sent, :], tile[:, cols]) + _dot(strips[1, sent, :], tile[:, more])

    def add_into(out, *terms):
        def body(i):
            r = pl.ds(pl.multiple_of(i * 8, 8), 8)
            val = out[r, :]
            for term in terms:
                val = val + term[r, :]
            out[r, :] = val

        _loop(kept // 8, body)

    def to_core(q, rows):
        m = pl.ds(0, rows)
        return remote(ost.at[q, m], dbuf.at[q, m], d_send.at[q], d_recv.at[q], partner)

    def staged(n, q):
        return (sst, acc, cur, acc)[n].at[q]

    def ring_copy(stage, q, rows):
        m, to = pl.ds(0, rows), dev(1 + (nx - 2) * q, 0)
        src, send = staged(stage, q).at[m], s_send.at[2 * stage + q]
        if stage == 0:
            return remote(src, trans.at[q, m], send, t_recv.at[q], to)
        half = 1 - q if stage == 1 else q
        return remote(src, fin.at[q, half, m], send, f_recv.at[q, half], to)

    def freed(sem, q):
        pl.semaphore_signal(sem.at[q], inc=1, device_id={AXIS: dev(nx - 1 - (nx - 2) * q, 0)},
                            device_id_type=pl.DeviceIdType.MESH)

    def backward(idx):
        t = step_count - 1 - idx
        with jax.named_scope("bw"):
            weights(t)
        for_each(t, lambda tt, rows: _start(w_copies(tt, rows)))

        @pl.when(t > 2)
        def _():
            em_copy(t - 2).start()

        def tile(n, q, flip):
            if n == 0:
                return held.at[4 + 2 * flip + q]
            if n == 3:
                return ring.at[2 * flip + q]
            return (held if q else ring).at[2 * (n - 1) + flip]

        def pair(n, q):
            def use(flip, out):
                at = 2 * flip + q if n == 3 else 2 * (n - 1) + flip
                if n == 0:
                    pl.when(idx == 0)(lambda: in_held(4 + 2 * flip + q))
                elif n < 3 and q:
                    pl.when(idx == 0)(lambda: in_held(at))
                else:
                    in_ring(at)
                partial_sums(out, tile(n, q, flip))
                if n == 3:
                    pl.when(t > 2)(lambda: tile_copy(2, at, True).start())
                elif n > 0 and not q:
                    tile_copy(0, at, True).start()

            if n > 0:
                back_caps(t, lambda rows: to_core(q, rows).wait_send())
            use(1, ost.at[q])
            back_caps(t, lambda rows: to_core(q, rows).start())
            out = staged(n, q)
            if n == 2:
                pl.when(idx == 0)(lambda: post_copy(q).wait())
            if n == 3:
                back_caps(t, lambda rows: ring_copy(1, q, rows).wait_send())
            use(0, out)
            back_caps(t, lambda rows: to_core(q, rows).wait_recv())
            if n == 2:
                back_caps(t, lambda rows: ring_copy(0, q, rows).wait_recv())
                add_into(out, dbuf.at[q], trans.at[q])
                pl.when(t > 2)(lambda: freed(t_free, q))
            else:
                add_into(out, dbuf.at[q])
            if n < 2:
                credit = t_free if n == 0 else f_free
                pl.when(idx > 0)(lambda: pl.semaphore_wait(credit.at[q], 1))
            if n < 3:
                back_caps(t, lambda rows: ring_copy(n, q, rows).start())

        with jax.named_scope("b0"):
            _loop(2, functools.partial(pair, 0))
        for n in (1, 2):
            for q in BOTH:
                with jax.named_scope(f"b{n}"):
                    pair(n, q)
        with jax.named_scope("b3"):
            _loop(2, functools.partial(pair, 3))

        def landed(rows):
            for n in (1, 2):
                for q in BOTH:
                    ring_copy(n, q, rows).wait_recv()

        with jax.named_scope("bl"):
            back_caps(t, landed)

        def body(i):
            r = pl.ds(pl.multiple_of(i * 8, 8), 8)
            live = t < lcol_ref[r, :]
            for k in range(tiles):
                h, col = inner(k)
                val = acc[h, r, col] + fin[0, h, r, col] + fin[1, h, r, col]
                acc[h, r, col] = jnp.where(live, val, 1.0)

        _loop(kept // 8, body)

        @pl.when(t > 2)
        def _():
            _loop(2, functools.partial(freed, f_free))

        def drained(rows):
            for q in BOTH:
                to_core(q, rows).wait_send()
                ring_copy(0, q, rows).wait_send()
                ring_copy(2, q, rows).wait_send()

        with jax.named_scope("bd"):
            back_caps(t, drained)
        for_each(t, lambda tt, rows: _wait(w_copies(tt, rows)))

        @pl.when(t > 2)
        def _():
            em_copy(t - 2).wait()

    acc[...] = jnp.ones_like(acc)
    _loop(step_count - 2, backward)
    weights(1)
    _start(w_copies(1, caps[0]))
    _wait(w_copies(1, caps[0]))


def _run_recursion(nd, caps, ident, trans_loc, em, init_loc, lcol, lrow):
    step_count, seqs, bs = em.shape
    hb = bs // 2
    kept = max(caps[1:])
    depth = min(8 if kept < seqs else 4, 2 * bs // LANES)
    dma = pltpu.SemaphoreType.DMA
    two, credit = dma((2,)), pltpu.SemaphoreType.REGULAR((2,))
    vm, hbm = pl.BlockSpec(memory_space=pltpu.VMEM), pl.BlockSpec(memory_space=pl.ANY)
    scratch = [
        pltpu.VMEM((8, hb, bs), BF16),
        pltpu.VMEM((4, hb, bs), BF16),
        pltpu.VMEM((8, 2, seqs, hb), BF16),
        pltpu.VMEM((2, seqs, hb), F32),
        pltpu.VMEM((2, seqs, hb), F32),
        pltpu.VMEM((2, seqs, bs), BF16),
        pltpu.VMEM((step_count, seqs, LANES), F32),
        pltpu.VMEM((seqs, LANES), F32),
        pltpu.VMEM((8, seqs), F32),
        pltpu.VMEM((nd, 8, seqs), F32),
        pltpu.VMEM((depth, LANES, hb), BF16),
        pltpu.VMEM((2, kept, hb), F32),
        pltpu.VMEM((2, kept, hb), F32),
        pltpu.VMEM((2, kept, hb), F32),
        pltpu.VMEM((2, kept, hb), F32),
        pltpu.VMEM((2, 2, kept, hb), F32),
        dma((nd,)), dma((4,)), two, dma((nd, 2)), dma((3, 2)), dma((nd, 2)), two, dma((nd,)), dma((nd,)), two,
        two, dma((depth,)), two, two, dma((6,)), two, dma((2, 2)), credit, credit,
    ]
    return pl.pallas_call(
        functools.partial(_recursion, caps),
        name=f"recursion{ident}",
        out_shape=[
            jax.ShapeDtypeStruct((sum(caps), bs), BF16),
            jax.ShapeDtypeStruct((sum(caps), bs), BF16),
            jax.ShapeDtypeStruct((seqs, bs), F32),
            jax.ShapeDtypeStruct((8, seqs), F32),
            jax.ShapeDtypeStruct(trans_loc.shape, BF16),
        ],
        in_specs=[hbm, hbm, vm, vm, vm],
        out_specs=[hbm, hbm, hbm, vm, hbm],
        scratch_shapes=scratch,
        compiler_params=pltpu.CompilerParams(collective_id=ident, has_side_effects=True, vmem_limit_bytes=67_043_328),
    )(trans_loc, em, init_loc[None, :], lcol, lrow)


def _prepare(caps, tok_ref, len_ref, emt_hbm, em_hbm, lcol_ref, lrow_ref, rank_ref, fits_ref,
             table, stable, picked, blocks, stage, table_sem, block_sem, stage_sem):
    step_count, seqs, bs = em_hbm.shape
    deep = blocks.shape[0]
    part = 32
    slab = min(512, bs)
    sub = lax.broadcasted_iota(jnp.int32, (seqs, LANES), 0)
    lan = lax.broadcasted_iota(jnp.int32, (seqs, LANES), 1)
    across = jnp.broadcast_to(len_ref[...].astype(F32), (seqs, seqs))
    down = jnp.transpose(across)
    ahead = (down > across) | ((down == across) & (sub < lan))
    rank = jnp.sum(jnp.where(ahead, 1.0, 0.0), axis=0, keepdims=True)
    rank_ref[...] = jnp.broadcast_to(rank, rank_ref.shape)
    pick = rank == sub.astype(F32)
    lcol = jnp.broadcast_to(jnp.sum(jnp.where(pick, across, 0.0), axis=1, keepdims=True), (seqs, LANES))
    lcol_ref[...] = lcol.astype(jnp.int32)
    lrow_ref[...] = jnp.transpose(lcol)[0:8].astype(jnp.int32)
    mat = jnp.zeros((seqs, LANES), F32)
    for t in range(step_count):
        tok = jnp.sum(jnp.where(pick, tok_ref[t : t + 1, :].astype(F32), 0.0), axis=1, keepdims=True)
        tok = jnp.broadcast_to(tok, (seqs, LANES))
        mat = jnp.where(lan == t, tok, mat)
        picked[t] = tok.astype(jnp.int32) & 7
    table[0:8] = jnp.transpose(mat)[0:8].astype(jnp.int32)
    alive = jnp.sum(jnp.where(across[0:8] > sub[0:8].astype(F32), 1.0, 0.0), axis=1, keepdims=True)
    table[8:16] = jnp.broadcast_to(alive, (8, LANES)).astype(jnp.int32)
    copy = pltpu.make_async_copy(table, stable, table_sem)
    copy.start()
    copy.wait()
    fits = jnp.int32(1)
    for t in range(1, step_count):
        fits = jnp.where(stable[8 + t, 0] > caps[t - 1], 0, fits)
    fits_ref[0] = fits

    def parts(t):
        return (stable[8 + t, 0] + (part - 1)) // part

    def fetch(t):
        def body(p, carry):
            for k in range(part):
                s = p * part + k
                pltpu.make_async_copy(emt_hbm.at[stable[t, s] >> 3], blocks.at[t % deep, s], block_sem.at[t % deep]).start()
            return carry

        lax.fori_loop(0, parts(t), body, 0)

    def landed(t):
        def body(p, carry):
            pltpu.make_async_copy(emt_hbm.at[pl.ds(0, part)], blocks.at[t % deep, pl.ds(0, part)], block_sem.at[t % deep]).wait()
            return carry

        lax.fori_loop(0, parts(t), body, 0)

    def select(t):
        def body(p, carry):
            r = pl.ds(pl.multiple_of(p * part, part), part)
            at = picked[t, r, :] + 8 * sub[0:part]
            one = jnp.concatenate([jnp.where(lan[0:part] + off == at, 1.0, 0.0) for off in (0, LANES)], axis=1).astype(BF16)
            for n in range(bs // slab):
                cols = pl.ds(n * slab, slab)
                rows = blocks[t % deep, r, :, cols].reshape(part * 8, slab)
                stage[t % 2, r, cols] = _dot(one, rows).astype(BF16)
            return carry

        lax.fori_loop(0, parts(t), body, 0)

    def out_copy(t):
        return pltpu.make_async_copy(stage.at[t % 2], em_hbm.at[t], stage_sem.at[t % 2])

    def position(t):
        pl.when(t >= 2)(lambda: out_copy(t - 2).wait())
        landed(t)
        select(t)
        out_copy(t).start()
        pl.when(t + deep < step_count)(lambda: fetch(t + deep))

    _loop(deep, fetch)
    _loop(step_count, position)
    _loop(2, lambda e: out_copy(step_count - 1 - e).wait())


def _run_prepare(caps, tokens, lengths, emit_loc):
    bs, symbols = emit_loc.shape
    seqs, step_count = tokens.shape
    dma = pltpu.SemaphoreType.DMA
    vm, hbm = pl.BlockSpec(memory_space=pltpu.VMEM), pl.BlockSpec(memory_space=pl.ANY)
    return pl.pallas_call(
        functools.partial(_prepare, caps),
        name="prepare",
        out_shape=[
            jax.ShapeDtypeStruct((step_count, seqs, bs), BF16),
            jax.ShapeDtypeStruct((seqs, LANES), jnp.int32),
            jax.ShapeDtypeStruct((8, seqs), jnp.int32),
            jax.ShapeDtypeStruct((8, seqs), F32),
            jax.ShapeDtypeStruct((1,), jnp.int32),
        ],
        in_specs=[vm, vm, hbm],
        out_specs=[hbm, vm, vm, vm, pl.BlockSpec(memory_space=pltpu.SMEM)],
        scratch_shapes=[
            pltpu.VMEM((16, LANES), jnp.int32),
            pltpu.SMEM((16, LANES), jnp.int32),
            pltpu.VMEM((step_count, seqs, LANES), jnp.int32),
            pltpu.VMEM((4, seqs, 8, bs), BF16),
            pltpu.VMEM((2, seqs, bs), BF16),
            dma, dma((4,)), dma((2,)),
        ],
        compiler_params=pltpu.CompilerParams(vmem_limit_bytes=60_000_000),
    )(tokens.T, lengths[None, :], emit_loc.T.reshape(symbols // 8, 8, bs))


def _counts(block_ref, alpha_ref, w_ref, diag_ref, post_ref, ll_ref, rank_ref, counts_ref, posterior_ref, loglik_ref):
    bs = w_ref.shape[1]
    slab = min(512, bs)
    lhs = alpha_ref[...]
    for n in range(bs // slab):
        cols = pl.ds(n * slab, slab)
        sums = _dot(lhs, w_ref[:, cols], 0)
        counts_ref[:, cols] = diag_ref[:, cols].astype(F32) * sums
    seqs = post_ref.shape[0]
    rank = jnp.broadcast_to(rank_ref[0:1, :], (seqs, seqs))
    sub = lax.broadcasted_iota(jnp.int32, (seqs, seqs), 0).astype(F32)
    lan = lax.broadcasted_iota(jnp.int32, (seqs, seqs), 1).astype(F32)
    back = jnp.where(jnp.transpose(rank) == lan, 1.0, 0.0).astype(BF16)
    rest = post_ref[...]
    total = jnp.zeros(posterior_ref.shape, F32)
    for _ in range(3):
        head = rest.astype(BF16)
        rest = rest - head.astype(F32)
        total = total + _dot(back, head)
    posterior_ref[...] = total
    lls = jnp.transpose(jnp.broadcast_to(ll_ref[0:1, :], (seqs, seqs)))
    loglik_ref[...] = jnp.sum(jnp.where(rank == sub, lls, 0.0), axis=0, keepdims=True)


def _run_counts(alphas, ws, trans_loc, post, ll, rank):
    rows, bs = alphas.shape
    seqs = post.shape[0]
    tile = min(256, bs)
    steps = bs // tile
    block = lax.axis_index(AXIS).astype(jnp.int32)[None]
    return pl.pallas_call(
        _counts,
        name="counts",
        out_shape=[
            jax.ShapeDtypeStruct((bs, bs), F32),
            jax.ShapeDtypeStruct((seqs, bs), F32),
            jax.ShapeDtypeStruct((1, seqs), F32),
        ],
        grid_spec=pltpu.PrefetchScalarGridSpec(
            num_scalar_prefetch=1,
            grid=(steps,),
            in_specs=[
                pl.BlockSpec((rows, tile), lambda i, b: (0, i)),
                pl.BlockSpec((rows, bs), lambda i, b: (0, 0)),
                pl.BlockSpec((tile, bs), lambda i, b: (b[0] * steps + i, 0)),
                pl.BlockSpec((seqs, tile), lambda i, b: (0, i)),
                pl.BlockSpec((8, seqs), lambda i, b: (0, 0)),
                pl.BlockSpec((8, seqs), lambda i, b: (0, 0)),
            ],
            out_specs=[
                pl.BlockSpec((tile, bs), lambda i, b: (i, 0)),
                pl.BlockSpec((seqs, tile), lambda i, b: (0, i)),
                pl.BlockSpec((1, seqs), lambda i, b: (0, 0)),
            ],
        ),
        compiler_params=pltpu.CompilerParams(vmem_limit_bytes=60_000_000),
    )(block, alphas, ws, trans_loc, post, ll, rank)


def _capacities(seqs, step_count):
    caps = []
    for t in range(1, step_count):
        live = (step_count - t) / step_count
        room = 3.1 * math.sqrt((seqs - 1) * live * (1 - live))
        caps.append(min(seqs, 8 * math.ceil(((seqs - 1) * live + 1 + room) / 8)))
    return tuple(caps)


def solution(mesh):
    nd = mesh.shape[AXIS]

    def local_run(trans_loc, emit_loc, init_loc, tokens_loc, lengths_loc):
        seqs, step_count = tokens_loc.shape
        caps = _capacities(seqs, step_count)
        em, lcol, lrow, rank, fits = _run_prepare(caps, tokens_loc, lengths_loc, emit_loc)

        def run(caps, ident, trans, em, init, lcol, lrow, rank):
            alphas, ws, post, ll, _ = _run_recursion(nd, caps, ident, trans, em, init, lcol, lrow)
            return _run_counts(alphas, ws, trans, post, ll, rank)

        counts, posterior, loglik = lax.cond(
            fits[0] == 1,
            functools.partial(run, caps, 0),
            functools.partial(run, (seqs,) * (step_count - 1), 1),
            trans_loc, em, init_loc, lcol, lrow, rank)
        return loglik[0], posterior, counts

    return jax.shard_map(
        local_run,
        mesh=mesh,
        in_specs=(P(None, AXIS), P(AXIS, None), P(AXIS), P("seqs", None), P("seqs")),
        out_specs=(P("seqs"), P("seqs", AXIS), P(("seqs", AXIS), None)),
        check_vma=False,
    )
```

```python
import functools
import math

import jax
import jax.numpy as jnp
from jax import lax
from jax.experimental import pallas as pl
from jax.experimental.pallas import tpu as pltpu
from jax.sharding import PartitionSpec as P

AXIS = "states"
LANES = 128
BOTH = (0, 1)
F32 = jnp.float32
BF16 = jnp.bfloat16


def _dot(a, b, over_a=1, over_b=0):
    dims = (((over_a,), (over_b,)), ((), ()))
    return lax.dot_general(a, b, dims, preferred_element_type=F32)


def _start(copies):
    for cp in copies:
        cp.start()


def _wait(copies):
    for cp in copies:
        cp.wait()


def _loop(n, body):
    def step(i, carry):
        body(i)
        return carry

    lax.fori_loop(0, n, step, 0)


def _recursion(caps, a_hbm, em_hbm, pi_ref, lcol_ref, lrow_ref, al_hbm, w_hbm, post_hbm, ll_ref, turned_hbm,
               bank, al, work, emv, rcs, sbuf, csend, cbuf, strips, ost, dbuf, trans, fin,
               bank_sem, em_sem, al_recv, own_send, part_send, on_send, c_send, c_recv, save_sem, post_sem,
               strip_sem, d_send, d_recv, s_send, t_recv, f_recv, t_free, f_free, d_free):
    nd = cbuf.shape[0]
    nx = nd // 2
    step_count, seqs, bs = em_hbm.shape
    hb = bs // 2
    firsts = [sum(caps[:t]) for t in range(step_count)]
    slab = min(512, hb)
    tiles = bs // LANES
    kept = max(caps[1:])
    sent = pl.ds(0, kept)
    final = step_count - 1
    g = lax.axis_index(AXIS)
    x, c = g // 2, g % 2

    def dev(dx, flip):
        return ((x + dx) % nx) * 2 + (c + flip) % 2

    partner, right, left = dev(0, 1), dev(1, 0), dev(nx - 1, 0)

    def remote(src, dst, send, recv, to):
        return pltpu.make_async_remote_copy(
            src_ref=src, dst_ref=dst, send_sem=send, recv_sem=recv,
            device_id={AXIS: to}, device_id_type=pl.DeviceIdType.MESH)

    def for_each(t, fn):
        for tt in range(1, step_count):
            pl.when(t == tt)(functools.partial(fn, tt, caps[tt - 1]))

    def for_caps(t, fn, first=1):
        if len(set(caps)) == 1:
            fn(caps[0])
            return
        for tt in range(first, step_count):
            pl.when(t == tt)(functools.partial(fn, caps[tt - 1]))

    acc, cur = work.at[pl.ds(0, 2)], work.at[pl.ds(4, 2)]

    def tile_row(group, i):
        if group == 0:
            src, half = dev(0, i // 2), i % 2
        elif group == 1:
            src, half = dev(nx - 1, i % 2), i // 2
        elif group == 2:
            src, half = dev(1, i % 2), 1 - i // 2
        else:
            src, half = dev(2, i // 2), i % 2
        return src * bs + half * hb

    def load(slot, row, src):
        pltpu.make_async_copy(src.at[pl.ds(pl.multiple_of(row, hb), hb)], bank.at[slot], bank_sem.at[slot]).start()

    def load_tile(slot, group, i):
        load(slot, tile_row(group, i), a_hbm)

    def load_turned(slot, number):
        load(slot, number * hb, turned_hbm)

    def in_bank(slot):
        pltpu.make_async_copy(a_hbm.at[pl.ds(0, hb)], bank.at[slot], bank_sem.at[slot]).wait()

    depth = strips.shape[0]
    bunch = min(4, depth)

    def strip_copy(number, unit, k):
        rows = pl.ds(pl.multiple_of(number * hb + (unit % (tiles // 2)) * LANES, LANES), LANES)
        cols = pl.ds(pl.multiple_of((unit // (tiles // 2)) * hb, hb), hb)
        return pltpu.make_async_copy(strips.at[k], turned_hbm.at[rows, cols], strip_sem.at[k])

    def turn(slot, number, first):
        def body(i):
            units = [bunch * i + e for e in range(bunch)]

            @pl.when(jnp.logical_not(first) | (bunch * i >= depth))
            def _():
                for u in units:
                    strip_copy(0, 0, u % depth).wait()

            for u in units:
                strips[u % depth] = jnp.transpose(bank[slot, :, pl.ds(pl.multiple_of(u * LANES, LANES), LANES)])
            for u in units:
                strip_copy(number, u, u % depth).start()

        _loop(tiles // bunch, body)

    def turn_own(t):
        each = -(-7 // final)

        def body(e):
            n = t * each + e
            far = n // 4
            pl.when(n < 7)(lambda: turn(8 + n - far * 7, n + far * 9, n == 0))

        _loop(each, body)

    def turn_others(t):
        each = -(-5 // (final - 1))

        def body(e):
            n = (t - 1) * each + e
            pl.when((t < final) & (n < 5))(lambda: turn(n, 4 + n + 4 * (n // 4), False))

        _loop(each, body)

        def right(r):
            @pl.when(turned_at(t, r))
            def _():
                in_bank(8 + r)
                turn(8 + r, 8 + r, False)

        _loop(4, right)

    def turned_at(t, r):
        return (t == r) | ((t == 1) & (r == 0))

    def em_copy(t):
        return pltpu.make_async_copy(em_hbm.at[t], emv.at[t % 2], em_sem.at[t % 2])

    _loop(2, lambda t: em_copy(t).start())
    _loop(4, lambda i: load_tile(8 + i, 0, i))
    _loop(4, lambda i: load_tile(i, 1, i))
    _loop(4, lambda i: load_tile(4 + i, 3, i))

    barrier = pltpu.get_barrier_semaphore()
    for k in range(1, nd):
        pl.semaphore_signal(barrier, inc=1, device_id={AXIS: (g + k) % nd}, device_id_type=pl.DeviceIdType.MESH)
    pl.semaphore_wait(barrier, nd - 1)

    def rows_of(i):
        return pl.ds(pl.multiple_of(i * 16, 16), 16)

    def lane(k):
        return pl.ds(k * LANES, LANES)

    def inner(k):
        return (k * LANES) // hb, pl.ds((k * LANES) % hb, LANES)

    def weigh(t):
        def body(i):
            r = rows_of(i)
            total = jnp.zeros((16, LANES), F32)
            for k in range(tiles):
                e = emv[t % 2, r, lane(k)].astype(F32)
                h, col = inner(k)
                mass = acc[h, r, col] * e
                acc[h, r, col] = mass
                total = total + mass
            sbuf[r, :] = total

        _loop(seqs // 16, body)

    def normalise(t):
        row = jnp.sum(jnp.transpose(sbuf[...]), axis=0, keepdims=True)
        wide = jnp.broadcast_to(row, csend.shape)
        csend[...] = wide
        cbuf[g] = wide
        peers = [dev(dx, flip) for dx in (2, 1, nx - 1, 0) for flip in BOTH][: nd - 2] + [partner]
        copies = [remote(csend, cbuf.at[g], c_send.at[k], c_recv.at[g], to) for k, to in enumerate(peers)]
        _start(copies)

        with jax.named_scope("ft"):
            @pl.when(t < final)
            def _():
                _loop(4, lambda i: in_bank(8 + i))
                turn_own(t)

        with jax.named_scope("fx"):
            for k, frm in enumerate(peers):
                remote(csend, cbuf.at[frm], c_send.at[k], c_recv.at[frm], frm).wait_recv()
        norm = cbuf[0, 0:1, :]
        for d in range(1, nd):
            norm = norm + cbuf[d, 0:1, :]
        rcs[t] = 1.0 / jnp.transpose(jnp.broadcast_to(norm, (LANES, LANES)))
        ll_ref[...] = ll_ref[...] + jnp.where(t < lrow_ref[...], jnp.log(jnp.broadcast_to(norm, ll_ref.shape)), 0.0)

        def body(i):
            r = rows_of(i)
            rc = rcs[t, r, :]
            live = t < lcol_ref[r, :]
            for k in range(tiles):
                h, col = inner(k)
                val = jnp.where(live, acc[h, r, col] * rc, cur[h, r, col])
                cur[h, r, col] = val
                al[0, h, r, col] = val.astype(BF16)

        _loop(seqs // 16, body)
        for cp in copies:
            cp.wait_send()

    ll_ref[...] = jnp.zeros_like(ll_ref)
    for h in BOTH:
        acc[h] = jnp.broadcast_to(pi_ref[:, h * hb : (h + 1) * hb], (seqs, hb))

    def own_copies(rows):
        m = pl.ds(0, rows)
        out = [remote(al.at[0, h, m], al.at[1, h, m], own_send.at[0, h], al_recv.at[1, h], partner) for h in BOTH]
        for h in BOTH:
            out.append(remote(al.at[0, h, m], al.at[2, h, m], own_send.at[1, h], al_recv.at[2, h], right))
            out.append(remote(al.at[0, 1 - h, m], al.at[3, 1 - h, m], own_send.at[2, 1 - h], al_recv.at[3, 1 - h], left))
        return out

    def to_partner(slot, to_slot, half, rows):
        m = pl.ds(0, rows)
        return remote(al.at[slot, half, m], al.at[to_slot, half, m], part_send.at[slot, half], al_recv.at[to_slot, half], partner)

    def onward(s, rows):
        m = pl.ds(0, rows)
        return remote(al.at[2 + s, s, m], al.at[6, s, m], on_send.at[s], al_recv.at[6, s], dev(1 + (nx - 2) * s, 0))

    def arrived(slot, half, rows):
        m = pl.ds(0, rows)
        remote(al.at[slot, half, m], al.at[slot, half, m], part_send.at[slot, half], al_recv.at[slot, half], partner).wait_recv()

    def save_copies(t, rows):
        to = pl.ds(firsts[t - 1], rows)
        return [pltpu.make_async_copy(al.at[0, h, pl.ds(0, rows)], al_hbm.at[to, pl.ds(h * hb, hb)], save_sem.at[h])
                for h in BOTH]

    def multiply(one, two):
        (slot1, half1, tile1), (slot2, half2, tile2) = one, two
        lhs1, lhs2 = al[slot1, half1], al[slot2, half2]
        for h in BOTH:
            for n in range(hb // slab):
                cols, at = pl.ds(h * hb + n * slab, slab), pl.ds(n * slab, slab)
                acc[h, :, at] = acc[h, :, at] + (
                    _dot(lhs1, tile1[:, cols]) + _dot(lhs2, tile2[:, cols]))

    def forward(t):
        pl.when(t > 0)(lambda: predict(t))
        em_copy(t).wait()
        with jax.named_scope("fw"):
            weigh(t)
        normalise(t)

    def predict(t):
        for_caps(t, lambda rows: _start(own_copies(rows)))
        for_each(t, lambda tt, rows: _start(save_copies(tt, rows)))

        @pl.when(t + 1 < step_count)
        def _():
            em_copy(t + 1).start()

        acc[...] = jnp.zeros(acc.shape, F32)

        def group0(j):
            def ready(rows):
                for half in BOTH:
                    arrived(1, half, rows)

            pl.when(j > 0)(lambda: for_caps(t, ready))
            multiply(*((j, e, bank.at[8 + 2 * j + e]) for e in BOTH))
            for e in BOTH:
                load_tile(8 + 2 * j + e, 2, 2 * j + e)

        def group12(k, j):
            def ready(rows):
                arrived(2 + 2 * j, k, rows)
                arrived(3 + 2 * j, 1 - k, rows)

                @pl.when(j == 0)
                def _():
                    to_partner(2, 4, k, rows).start()
                    to_partner(3, 5, 1 - k, rows).start()

                pl.when(k + j == 0)(lambda: _start([onward(0, rows), onward(1, rows)]))

            for_caps(t, ready)
            at = 2 * k + j
            pl.when(jnp.logical_not(turned_at(t, at)))(lambda: in_bank(8 + at))
            multiply((2 + 2 * j, k, bank.at[at]), (3 + 2 * j, 1 - k, bank.at[8 + at]))

        def next_tiles(k):
            def body(e):
                i = 2 * k + e
                pl.when(t < final)(lambda: load_tile(8 + i, 0, i))

                @pl.when(t == final)
                def _():
                    load_turned(8 + i, 12 + i)
                    load_turned(i, 4 + i)

            _loop(2, body)

        def group3(j):
            def ready(rows):
                for half in BOTH:
                    arrived(6 + j, half, rows)

                @pl.when(j == 0)
                def _():
                    for half in BOTH:
                        to_partner(6, 7, half, rows).start()

            for_caps(t, ready)
            multiply(*((6 + j, e, bank.at[4 + 2 * j + e]) for e in BOTH))

        with jax.named_scope("f0"):
            _loop(2, group0)
        pl.when(t == 1)(lambda: _loop(8, in_bank))
        with jax.named_scope("ft"):
            turn_others(t)
        pl.when(t == final)(lambda: _loop(depth, lambda k: strip_copy(0, 0, k).wait()))

        def groups12(k):
            with jax.named_scope("f1"):
                _loop(2, functools.partial(group12, k))
            next_tiles(k)

        _loop(2, groups12)
        with jax.named_scope("f3"):
            _loop(2, group3)
        pl.when(t == final)(lambda: _loop(4, lambda i: load_turned(4 + i, 8 + i)))

        def drained(rows):
            for cp in own_copies(rows):
                cp.wait_send()
            for half in BOTH:
                to_partner(2, 4, half, rows).wait_send()
                to_partner(3, 5, half, rows).wait_send()
                to_partner(6, 7, half, rows).wait_send()
                onward(half, rows).wait_send()

        for_caps(t, drained)
        for_each(t, lambda tt, rows: _wait(save_copies(tt, rows)))

    _loop(step_count, forward)

    def post_copy(h):
        return pltpu.make_async_copy(cur.at[h], post_hbm.at[:, pl.ds(pl.multiple_of(h * hb, hb), hb)], post_sem.at[h])

    _loop(2, lambda h: post_copy(h).start())

    back_caps = functools.partial(for_caps, first=2)

    def weights(t):
        def body(i):
            r = rows_of(i)
            rc = rcs[t, r, :]
            live = t < lcol_ref[r, :]
            for k in range(tiles):
                h, col = inner(k)
                val = emv[t % 2, r, lane(k)].astype(F32) * acc[h, r, col] * rc
                strips[h, r, col] = jnp.where(live, val, 0.0).astype(BF16)

        _loop(seqs // 16, body)

    def w_copies(t, rows):
        to = pl.ds(firsts[t - 1], rows)
        return [pltpu.make_async_copy(strips.at[h, pl.ds(0, rows)], w_hbm.at[to, pl.ds(h * hb, hb)], save_sem.at[h])
                for h in BOTH]

    def partial_sums(out, tile):
        for n in range(hb // slab):
            cols = pl.ds(n * slab, slab)
            more = pl.ds(hb + n * slab, slab)
            out[sent, cols] = _dot(strips[0, sent, :], tile[:, cols]) + _dot(strips[1, sent, :], tile[:, more])

    def add_into(out, *terms):
        def body(i):
            r = pl.ds(pl.multiple_of(i * 8, 8), 8)
            val = out[r, :]
            for term in terms:
                val = val + term[r, :]
            out[r, :] = val

        _loop(kept // 8, body)

    def to_core(q, rows):
        m = pl.ds(0, rows)
        return remote(ost.at[q, m], dbuf.at[q, m], d_send.at[q], d_recv.at[q], partner)

    def staged(p):
        n, q = p // 2, p % 2
        return (1 - n % 2) * (2 + n) + q

    def ring_copy(far, p, rows):
        m, q = pl.ds(0, rows), p % 2
        to = dev(1 + (nx - 2) * q, 0)
        src, send = work.at[staged(p), m], s_send.at[p]
        if far:
            return remote(src, trans.at[q, m], send, t_recv.at[q], to)
        half = (p // 2 + q) % 2
        return remote(src, fin.at[q, half, m], send, f_recv.at[q, half], to)

    def freed(sem, q):
        pl.semaphore_signal(sem.at[q], inc=1, device_id={AXIS: dev(nx - 1 - (nx - 2) * q, 0)},
                            device_id_type=pl.DeviceIdType.MESH)

    def backward(idx):
        t = step_count - 1 - idx
        with jax.named_scope("bw"):
            weights(t)
        for_each(t, lambda tt, rows: _start(w_copies(tt, rows)))

        @pl.when(t > 2)
        def _():
            em_copy(t - 2).start()

        def slot_of(p, flip):
            n, q = p // 2, p % 2
            inner = ((n + 1) % 4) // 2
            return inner == 0, (1 - inner) * (8 + 2 * flip + q) + inner * (4 * (1 - q) + 2 * (n - 1) + flip)

        def use(p, flip, out):
            outer, slot = slot_of(p, flip)
            pl.when(outer | (idx == 0))(lambda: in_bank(slot))
            partial_sums(out, bank.at[slot])
            pl.when(p < 2)(lambda: load_turned(slot, slot - 8))
            pl.when((p >= 6) & (t > 2))(lambda: load_turned(slot, slot + 4))

        def for_other(p):
            q = p % 2
            pl.when(p >= 2)(lambda: back_caps(t, lambda rows: to_core(q, rows).wait_send()))
            use(p, 1, ost.at[q])
            pl.when((p >= 2) | (idx > 0))(lambda: pl.semaphore_wait(d_free.at[q], 1))
            back_caps(t, lambda rows: to_core(q, rows).start())

        def for_this(p):
            q = p % 2
            out = work.at[staged(p)]
            pl.when((p // 2 == 2) & (idx == 0))(lambda: post_copy(q).wait())
            pl.when(p >= 6)(lambda: back_caps(t, lambda rows: ring_copy(False, p - 4, rows).wait_send()))
            use(p, 0, out)
            back_caps(t, lambda rows: to_core(q, rows).wait_recv())

            @pl.when(p // 2 == 2)
            def _():
                back_caps(t, lambda rows: ring_copy(True, q, rows).wait_recv())
                add_into(out, dbuf.at[q], trans.at[q])
                pl.when(t > 2)(lambda: freed(t_free, q))

            pl.when(p // 2 != 2)(lambda: add_into(out, dbuf.at[q]))

            @pl.when((p < 6) | (t > 2))
            def _():
                pl.semaphore_signal(d_free.at[q], inc=1, device_id={AXIS: partner}, device_id_type=pl.DeviceIdType.MESH)

            @pl.when(p < 2)
            def _():
                pl.when(idx > 0)(lambda: pl.semaphore_wait(t_free.at[q], 1))
                back_caps(t, lambda rows: ring_copy(True, p, rows).start())

            @pl.when((p >= 2) & (p < 6))
            def _():
                pl.when((idx > 0) & (p < 4))(lambda: pl.semaphore_wait(f_free.at[q], 1))
                back_caps(t, lambda rows: ring_copy(False, p, rows).start())

        def pair(p):
            with jax.named_scope("bo"):
                pl.when(p < 8)(lambda: for_other(p))
            with jax.named_scope("bt"):
                pl.when(p > 0)(lambda: for_this(p - 1))

        _loop(9, pair)

        def landed(rows):
            for p in range(2, 6):
                ring_copy(False, p, rows).wait_recv()

        with jax.named_scope("bl"):
            back_caps(t, landed)

        def body(i):
            r = pl.ds(pl.multiple_of(i * 8, 8), 8)
            live = t < lcol_ref[r, :]
            for k in range(tiles):
                h, col = inner(k)
                val = acc[h, r, col] + fin[0, h, r, col] + fin[1, h, r, col]
                acc[h, r, col] = jnp.where(live, val, 1.0)

        _loop(kept // 8, body)

        @pl.when(t > 2)
        def _():
            _loop(2, functools.partial(freed, f_free))

        def drained(rows):
            for q in BOTH:
                to_core(q, rows).wait_send()
                ring_copy(True, q, rows).wait_send()
                ring_copy(False, 4 + q, rows).wait_send()

        with jax.named_scope("bd"):
            back_caps(t, drained)
        for_each(t, lambda tt, rows: _wait(w_copies(tt, rows)))

        @pl.when(t > 2)
        def _():
            em_copy(t - 2).wait()

    acc[...] = jnp.ones(acc.shape, F32)
    _loop(step_count - 2, backward)
    weights(1)
    _start(w_copies(1, caps[0]))
    _wait(w_copies(1, caps[0]))


def _run_recursion(nd, caps, ident, trans_loc, em, init_loc, lcol, lrow):
    step_count, seqs, bs = em.shape
    hb = bs // 2
    kept = max(caps[1:])
    depth = min(8 if kept < seqs else 4, bs // LANES)
    dma = pltpu.SemaphoreType.DMA
    two, credit = dma((2,)), pltpu.SemaphoreType.REGULAR((2,))
    vm, hbm = pl.BlockSpec(memory_space=pltpu.VMEM), pl.BlockSpec(memory_space=pl.ANY)
    scratch = [
        pltpu.VMEM((12, hb, bs), BF16),
        pltpu.VMEM((8, 2, seqs, hb), BF16),
        pltpu.VMEM((6, seqs, hb), F32),
        pltpu.VMEM((2, seqs, bs), BF16),
        pltpu.VMEM((step_count, seqs, LANES), F32),
        pltpu.VMEM((seqs, LANES), F32),
        pltpu.VMEM((8, seqs), F32),
        pltpu.VMEM((nd, 8, seqs), F32),
        pltpu.VMEM((depth, LANES, hb), BF16),
        pltpu.VMEM((2, kept, hb), F32),
        pltpu.VMEM((2, kept, hb), F32),
        pltpu.VMEM((2, kept, hb), F32),
        pltpu.VMEM((2, 2, kept, hb), F32),
        dma((12,)), two, dma((nd, 2)), dma((3, 2)), dma((nd, 2)), two, dma((nd,)), dma((nd,)), two,
        two, dma((depth,)), two, two, dma((6,)), two, dma((2, 2)), credit, credit, credit,
    ]
    return pl.pallas_call(
        functools.partial(_recursion, caps),
        name=f"recursion{ident}",
        out_shape=[
            jax.ShapeDtypeStruct((sum(caps), bs), BF16),
            jax.ShapeDtypeStruct((sum(caps), bs), BF16),
            jax.ShapeDtypeStruct((seqs, bs), F32),
            jax.ShapeDtypeStruct((8, seqs), F32),
            jax.ShapeDtypeStruct(trans_loc.shape, BF16),
        ],
        in_specs=[hbm, hbm, vm, vm, vm],
        out_specs=[hbm, hbm, hbm, vm, hbm],
        scratch_shapes=scratch,
        compiler_params=pltpu.CompilerParams(collective_id=ident, has_side_effects=True, vmem_limit_bytes=67_043_328),
    )(trans_loc, em, init_loc[None, :], lcol, lrow)


def _prepare(caps, tok_ref, len_ref, emt_hbm, em_hbm, lcol_ref, lrow_ref, rank_ref, fits_ref,
             table, stable, picked, blocks, stage, table_sem, block_sem, stage_sem):
    step_count, seqs, bs = em_hbm.shape
    deep = blocks.shape[0]
    part = 32
    slab = min(512, bs)
    sub = lax.broadcasted_iota(jnp.int32, (seqs, LANES), 0)
    lan = lax.broadcasted_iota(jnp.int32, (seqs, LANES), 1)
    across = jnp.broadcast_to(len_ref[...].astype(F32), (seqs, seqs))
    down = jnp.transpose(across)
    ahead = (down > across) | ((down == across) & (sub < lan))
    rank = jnp.sum(jnp.where(ahead, 1.0, 0.0), axis=0, keepdims=True)
    rank_ref[...] = jnp.broadcast_to(rank, rank_ref.shape)
    pick = rank == sub.astype(F32)
    lcol = jnp.broadcast_to(jnp.sum(jnp.where(pick, across, 0.0), axis=1, keepdims=True), (seqs, LANES))
    lcol_ref[...] = lcol.astype(jnp.int32)
    lrow_ref[...] = jnp.transpose(lcol)[0:8].astype(jnp.int32)
    mat = jnp.zeros((seqs, LANES), F32)
    for t in range(step_count):
        tok = jnp.sum(jnp.where(pick, tok_ref[t : t + 1, :].astype(F32), 0.0), axis=1, keepdims=True)
        tok = jnp.broadcast_to(tok, (seqs, LANES))
        mat = jnp.where(lan == t, tok, mat)
        picked[t] = tok.astype(jnp.int32) & 7
    table[0:8] = jnp.transpose(mat)[0:8].astype(jnp.int32)
    alive = jnp.sum(jnp.where(across[0:8] > sub[0:8].astype(F32), 1.0, 0.0), axis=1, keepdims=True)
    table[8:16] = jnp.broadcast_to(alive, (8, LANES)).astype(jnp.int32)
    copy = pltpu.make_async_copy(table, stable, table_sem)
    copy.start()
    copy.wait()
    fits = jnp.int32(1)
    for t in range(1, step_count):
        fits = jnp.where(stable[8 + t, 0] > caps[t - 1], 0, fits)
    fits_ref[0] = fits

    def parts(t):
        return (stable[8 + t, 0] + (part - 1)) // part

    def fetch(t):
        def body(p, carry):
            for k in range(part):
                s = p * part + k
                pltpu.make_async_copy(emt_hbm.at[stable[t, s] >> 3], blocks.at[t % deep, s], block_sem.at[t % deep]).start()
            return carry

        lax.fori_loop(0, parts(t), body, 0)

    def landed(t):
        def body(p, carry):
            pltpu.make_async_copy(emt_hbm.at[pl.ds(0, part)], blocks.at[t % deep, pl.ds(0, part)], block_sem.at[t % deep]).wait()
            return carry

        lax.fori_loop(0, parts(t), body, 0)

    def select(t):
        def body(p, carry):
            r = pl.ds(pl.multiple_of(p * part, part), part)
            at = picked[t, r, :] + 8 * sub[0:part]
            one = jnp.concatenate([jnp.where(lan[0:part] + off == at, 1.0, 0.0) for off in (0, LANES)], axis=1).astype(BF16)
            for n in range(bs // slab):
                cols = pl.ds(n * slab, slab)
                rows = blocks[t % deep, r, :, cols].reshape(part * 8, slab)
                stage[t % 2, r, cols] = _dot(one, rows).astype(BF16)
            return carry

        lax.fori_loop(0, parts(t), body, 0)

    def out_copy(t):
        return pltpu.make_async_copy(stage.at[t % 2], em_hbm.at[t], stage_sem.at[t % 2])

    def position(t):
        pl.when(t >= 2)(lambda: out_copy(t - 2).wait())
        landed(t)
        select(t)
        out_copy(t).start()
        pl.when(t + deep < step_count)(lambda: fetch(t + deep))

    _loop(deep, fetch)
    _loop(step_count, position)
    _loop(2, lambda e: out_copy(step_count - 1 - e).wait())


def _run_prepare(caps, tokens, lengths, emit_loc):
    bs, symbols = emit_loc.shape
    seqs, step_count = tokens.shape
    dma = pltpu.SemaphoreType.DMA
    vm, hbm = pl.BlockSpec(memory_space=pltpu.VMEM), pl.BlockSpec(memory_space=pl.ANY)
    return pl.pallas_call(
        functools.partial(_prepare, caps),
        name="prepare",
        out_shape=[
            jax.ShapeDtypeStruct((step_count, seqs, bs), BF16),
            jax.ShapeDtypeStruct((seqs, LANES), jnp.int32),
            jax.ShapeDtypeStruct((8, seqs), jnp.int32),
            jax.ShapeDtypeStruct((8, seqs), F32),
            jax.ShapeDtypeStruct((1,), jnp.int32),
        ],
        in_specs=[vm, vm, hbm],
        out_specs=[hbm, vm, vm, vm, pl.BlockSpec(memory_space=pltpu.SMEM)],
        scratch_shapes=[
            pltpu.VMEM((16, LANES), jnp.int32),
            pltpu.SMEM((16, LANES), jnp.int32),
            pltpu.VMEM((step_count, seqs, LANES), jnp.int32),
            pltpu.VMEM((4, seqs, 8, bs), BF16),
            pltpu.VMEM((2, seqs, bs), BF16),
            dma, dma((4,)), dma((2,)),
        ],
        compiler_params=pltpu.CompilerParams(vmem_limit_bytes=60_000_000),
    )(tokens.T, lengths[None, :], emit_loc.T.reshape(symbols // 8, 8, bs))


def _counts(trans_hbm, alpha_hbm, w_hbm, post_hbm, ll_ref, rank_ref, counts_hbm, posterior_hbm, loglik_ref,
            alpha, w, diag, out, post, back, in_sem, diag_sem, out_sem, back_sem):
    rows, bs = w.shape
    seqs = post.shape[0]
    steps, tile, _ = diag.shape
    slab = min(512, bs)
    first = lax.axis_index(AXIS) * bs
    loads = [pltpu.make_async_copy(src, dst, in_sem.at[k])
             for k, (src, dst) in enumerate(((post_hbm, post), (w_hbm, w), (alpha_hbm, alpha)))]
    _start(loads)

    def diag_copy(i):
        at = pl.multiple_of(first + i * tile, tile)
        return pltpu.make_async_copy(trans_hbm.at[pl.ds(at, tile)], diag.at[i], diag_sem.at[i])

    def out_copy(i):
        at = pl.multiple_of(i * tile, tile)
        return pltpu.make_async_copy(out.at[i], counts_hbm.at[pl.ds(at, tile)], out_sem.at[i])

    _loop(steps, lambda i: diag_copy(i).start())

    rank = jnp.broadcast_to(rank_ref[0:1, :], (seqs, seqs))
    sub = lax.broadcasted_iota(jnp.int32, (seqs, seqs), 0).astype(F32)
    lan = lax.broadcasted_iota(jnp.int32, (seqs, seqs), 1).astype(F32)
    lls = jnp.transpose(jnp.broadcast_to(ll_ref[0:1, :], (seqs, seqs)))
    loglik_ref[...] = jnp.sum(jnp.where(rank == sub, lls, 0.0), axis=0, keepdims=True)
    order = jnp.where(jnp.transpose(rank) == lan, 1.0, 0.0).astype(BF16)
    loads[0].wait()
    for n in range(bs // slab):
        cols = pl.ds(n * slab, slab)
        rest = post[:, cols]
        total = jnp.zeros(rest.shape, F32)
        for _ in range(3):
            head = rest.astype(BF16)
            rest = rest - head.astype(F32)
            total = total + _dot(order, head)
        back[:, cols] = total
    back_copy = pltpu.make_async_copy(back, posterior_hbm, back_sem)
    back_copy.start()
    _wait(loads[1:])

    def step(i):
        lhs = alpha[:, pl.ds(pl.multiple_of(i * tile, tile), tile)]
        diag_copy(i).wait()
        for n in range(bs // slab):
            cols = pl.ds(n * slab, slab)
            out[i, :, cols] = diag[i, :, cols].astype(F32) * _dot(lhs, w[:, cols], 0)
        out_copy(i).start()

    _loop(steps, step)
    _loop(steps, lambda i: out_copy(i).wait())
    back_copy.wait()


def _run_counts(alphas, ws, trans_loc, post, ll, rank):
    rows, bs = alphas.shape
    seqs = post.shape[0]
    tile = min(256, bs)
    steps = bs // tile
    dma = pltpu.SemaphoreType.DMA
    vm, hbm = pl.BlockSpec(memory_space=pltpu.VMEM), pl.BlockSpec(memory_space=pl.ANY)
    return pl.pallas_call(
        _counts,
        name="counts",
        out_shape=[
            jax.ShapeDtypeStruct((bs, bs), F32),
            jax.ShapeDtypeStruct((seqs, bs), F32),
            jax.ShapeDtypeStruct((1, seqs), F32),
        ],
        in_specs=[hbm, hbm, hbm, hbm, vm, vm],
        out_specs=[hbm, hbm, vm],
        scratch_shapes=[
            pltpu.VMEM((rows, bs), BF16),
            pltpu.VMEM((rows, bs), BF16),
            pltpu.VMEM((steps, tile, bs), BF16),
            pltpu.VMEM((steps, tile, bs), F32),
            pltpu.VMEM((seqs, bs), F32),
            pltpu.VMEM((seqs, bs), F32),
            dma((3,)), dma((steps,)), dma((steps,)), dma,
        ],
        compiler_params=pltpu.CompilerParams(vmem_limit_bytes=60_000_000),
    )(trans_loc, alphas, ws, post, ll, rank)


def _capacities(seqs, step_count):
    caps = []
    for t in range(1, step_count):
        live = (step_count - t) / step_count
        room = 3.1 * math.sqrt((seqs - 1) * live * (1 - live))
        caps.append(min(seqs, 8 * math.ceil(((seqs - 1) * live + 1 + room) / 8)))
    return tuple(caps)


def solution(mesh):
    nd = mesh.shape[AXIS]

    def local_run(trans_loc, emit_loc, init_loc, tokens_loc, lengths_loc):
        seqs, step_count = tokens_loc.shape
        caps = _capacities(seqs, step_count)
        em, lcol, lrow, rank, fits = _run_prepare(caps, tokens_loc, lengths_loc, emit_loc)

        def run(caps, ident, trans, em, init, lcol, lrow, rank):
            alphas, ws, post, ll, _ = _run_recursion(nd, caps, ident, trans, em, init, lcol, lrow)
            return _run_counts(alphas, ws, trans, post, ll, rank)

        counts, posterior, loglik = lax.cond(
            fits[0] == 1,
            functools.partial(run, caps, 0),
            functools.partial(run, (seqs,) * (step_count - 1), 1),
            trans_loc, em, init_loc, lcol, lrow, rank)
        return loglik[0], posterior, counts

    return jax.shard_map(
        local_run,
        mesh=mesh,
        in_specs=(P(None, AXIS), P(AXIS, None), P(AXIS), P("seqs", None), P("seqs")),
        out_specs=(P("seqs"), P("seqs", AXIS), P(("seqs", AXIS), None)),
        check_vma=False,
    )
```

```python
import functools
import math

import jax
import jax.numpy as jnp
from jax import lax
from jax.experimental import pallas as pl
from jax.experimental.pallas import tpu as pltpu
from jax.sharding import PartitionSpec as P

AXIS = "states"
LANES = 128
BOTH = (0, 1)
F32 = jnp.float32
BF16 = jnp.bfloat16


def _dot(a, b, over_a=1, over_b=0):
    dims = (((over_a,), (over_b,)), ((), ()))
    return lax.dot_general(a, b, dims, preferred_element_type=F32)


def _start(copies):
    for cp in copies:
        cp.start()


def _wait(copies):
    for cp in copies:
        cp.wait()


def _loop(n, body):
    def step(i, carry):
        body(i)
        return carry

    lax.fori_loop(0, n, step, 0)


def _recursion(caps, a_hbm, em_hbm, pi_ref, lcol_ref, lrow_ref, al_hbm, w_hbm, post_hbm, ll_ref, turned_hbm,
               bank, al, work, emv, rcs, sbuf, csend, cbuf, strips, ost, dbuf, trans, fin,
               bank_sem, em_sem, al_recv, own_send, part_send, on_send, c_send, c_recv, save_sem, post_sem,
               strip_sem, d_send, d_recv, s_send, t_recv, f_recv, t_free, f_free, d_free):
    nd = cbuf.shape[0]
    nx = nd // 2
    step_count, seqs, bs = em_hbm.shape
    hb = bs // 2
    firsts = [sum(caps[:t]) for t in range(step_count)]
    slab = min(512, hb)
    tiles = bs // LANES
    kept = max(caps[1:])
    sent = pl.ds(0, kept)
    final = step_count - 1
    g = lax.axis_index(AXIS)
    x, c = g // 2, g % 2

    def dev(dx, flip):
        return ((x + dx) % nx) * 2 + (c + flip) % 2

    partner, right, left = dev(0, 1), dev(1, 0), dev(nx - 1, 0)

    def remote(src, dst, send, recv, to):
        return pltpu.make_async_remote_copy(
            src_ref=src, dst_ref=dst, send_sem=send, recv_sem=recv,
            device_id={AXIS: to}, device_id_type=pl.DeviceIdType.MESH)

    def pick(t, fn, lo, hi):
        if hi - lo == 1:
            fn(lo)
        else:
            mid = (lo + hi) // 2
            lax.cond(t < mid, lambda: pick(t, fn, lo, mid), lambda: pick(t, fn, mid, hi))

    def for_each(t, fn):
        pick(t, lambda tt: fn(tt, caps[tt - 1]), 1, step_count)

    def for_caps(t, fn, first=1):
        if len(set(caps)) == 1:
            fn(caps[0])
        else:
            pick(t, lambda tt: fn(caps[tt - 1]), first, step_count)

    acc, cur = work.at[pl.ds(0, 2)], work.at[pl.ds(4, 2)]

    def tile_row(group, i):
        if group == 0:
            src, half = dev(0, i // 2), i % 2
        elif group == 1:
            src, half = dev(nx - 1, i % 2), i // 2
        elif group == 2:
            src, half = dev(1, i % 2), 1 - i // 2
        else:
            src, half = dev(2, i // 2), i % 2
        return src * bs + half * hb

    def load(slot, row, src):
        pltpu.make_async_copy(src.at[pl.ds(pl.multiple_of(row, hb), hb)], bank.at[slot], bank_sem.at[slot]).start()

    def load_tile(slot, group, i):
        load(slot, tile_row(group, i), a_hbm)

    def load_turned(slot, number):
        load(slot, number * hb, turned_hbm)

    def in_bank(slot):
        pltpu.make_async_copy(a_hbm.at[pl.ds(0, hb)], bank.at[slot], bank_sem.at[slot]).wait()

    depth = strips.shape[0]
    bunch = min(4, depth)

    def strip_copy(number, unit, k):
        rows = pl.ds(pl.multiple_of(number * hb + (unit % (tiles // 2)) * LANES, LANES), LANES)
        cols = pl.ds(pl.multiple_of((unit // (tiles // 2)) * hb, hb), hb)
        return pltpu.make_async_copy(strips.at[k], turned_hbm.at[rows, cols], strip_sem.at[k])

    def turn(slot, number, first):
        def body(i):
            units = [bunch * i + e for e in range(bunch)]

            @pl.when(jnp.logical_not(first) | (bunch * i >= depth))
            def _():
                for u in units:
                    strip_copy(0, 0, u % depth).wait()

            for u in units:
                strips[u % depth] = jnp.transpose(bank[slot, :, pl.ds(pl.multiple_of(u * LANES, LANES), LANES)])
            for u in units:
                strip_copy(number, u, u % depth).start()

        _loop(tiles // bunch, body)

    def turn_own(t):
        each = -(-7 // final)

        def body(e):
            n = t * each + e
            far = n // 4
            pl.when(far == 0)(lambda: in_bank(8 + n))
            pl.when(n < 7)(lambda: turn(8 + n - far * 7, n + far * 9, n == 0))

        _loop(each, body)
        _loop(4, lambda i: pl.when((i < t * each) | (i >= t * each + each))(lambda: in_bank(8 + i)))

    def turn_others(t):
        each = -(-5 // (final - 1))

        def body(e):
            n = (t - 1) * each + e
            pl.when((t < final) & (n < 5))(lambda: turn(n, 4 + n + 4 * (n // 4), False))

        _loop(each, body)

        def right(r):
            in_bank(8 + r)
            turn(8 + r, 8 + r, False)

        pl.when(t == 1)(lambda: _loop(2, right))

    def em_copy(t):
        return pltpu.make_async_copy(em_hbm.at[t], emv.at[t % 2], em_sem.at[t % 2])

    _loop(2, lambda t: em_copy(t).start())
    _loop(4, lambda i: load_tile(8 + i, 0, i))
    _loop(4, lambda i: load_tile(i, 1, i))
    _loop(4, lambda i: load_tile(4 + i, 3, i))

    barrier = pltpu.get_barrier_semaphore()
    for k in range(1, nd):
        pl.semaphore_signal(barrier, inc=1, device_id={AXIS: (g + k) % nd}, device_id_type=pl.DeviceIdType.MESH)
    pl.semaphore_wait(barrier, nd - 1)

    def rows_of(i):
        return pl.ds(pl.multiple_of(i * 16, 16), 16)

    def lane(k):
        return pl.ds(k * LANES, LANES)

    def inner(k):
        return (k * LANES) // hb, pl.ds((k * LANES) % hb, LANES)

    def weigh(t):
        def body(i):
            r = rows_of(i)
            total = jnp.zeros((16, LANES), F32)
            for k in range(tiles):
                e = emv[t % 2, r, lane(k)].astype(F32)
                h, col = inner(k)
                mass = acc[h, r, col] * e
                acc[h, r, col] = mass
                total = total + mass
            sbuf[r, :] = total

        _loop(seqs // 16, body)

    def normalise(t):
        row = jnp.sum(jnp.transpose(sbuf[...]), axis=0, keepdims=True)
        wide = jnp.broadcast_to(row, csend.shape)
        csend[...] = wide
        cbuf[g] = wide
        peers = [dev(dx, flip) for dx in (2, 1, nx - 1, 0) for flip in BOTH][: nd - 2] + [partner]
        copies = [remote(csend, cbuf.at[g], c_send.at[k], c_recv.at[g], to) for k, to in enumerate(peers)]
        _start(copies)

        with jax.named_scope("ft"):
            @pl.when(t < final)
            def _():
                turn_own(t)

        with jax.named_scope("fx"):
            for k, frm in enumerate(peers):
                remote(csend, cbuf.at[frm], c_send.at[k], c_recv.at[frm], frm).wait_recv()
        norm = cbuf[0, 0:1, :]
        for d in range(1, nd):
            norm = norm + cbuf[d, 0:1, :]
        rcs[t] = 1.0 / jnp.transpose(jnp.broadcast_to(norm, (LANES, LANES)))
        ll_ref[...] = ll_ref[...] + jnp.where(t < lrow_ref[...], jnp.log(jnp.broadcast_to(norm, ll_ref.shape)), 0.0)

        def body(i):
            r = rows_of(i)
            rc = rcs[t, r, :]
            live = t < lcol_ref[r, :]
            for k in range(tiles):
                h, col = inner(k)
                val = jnp.where(live, acc[h, r, col] * rc, cur[h, r, col])
                cur[h, r, col] = val
                al[0, h, r, col] = val.astype(BF16)

        _loop(seqs // 16, body)
        for cp in copies:
            cp.wait_send()

    ll_ref[...] = jnp.zeros_like(ll_ref)
    for h in BOTH:
        acc[h] = jnp.broadcast_to(pi_ref[:, h * hb : (h + 1) * hb], (seqs, hb))

    def own_copies(rows):
        m = pl.ds(0, rows)
        out = [remote(al.at[0, h, m], al.at[1, h, m], own_send.at[0, h], al_recv.at[1, h], partner) for h in BOTH]
        for h in BOTH:
            out.append(remote(al.at[0, h, m], al.at[2, h, m], own_send.at[1, h], al_recv.at[2, h], right))
            out.append(remote(al.at[0, 1 - h, m], al.at[3, 1 - h, m], own_send.at[2, 1 - h], al_recv.at[3, 1 - h], left))
        return out

    def to_partner(slot, to_slot, half, rows):
        m = pl.ds(0, rows)
        return remote(al.at[slot, half, m], al.at[to_slot, half, m], part_send.at[slot, half], al_recv.at[to_slot, half], partner)

    def onward(s, rows):
        m = pl.ds(0, rows)
        return remote(al.at[2 + s, s, m], al.at[6, s, m], on_send.at[s], al_recv.at[6, s], dev(1 + (nx - 2) * s, 0))

    def arrived(slot, half, rows):
        m = pl.ds(0, rows)
        remote(al.at[slot, half, m], al.at[slot, half, m], part_send.at[slot, half], al_recv.at[slot, half], partner).wait_recv()

    def save_copies(t, rows):
        to = pl.ds(firsts[t - 1], rows)
        return [pltpu.make_async_copy(al.at[0, h, pl.ds(0, rows)], al_hbm.at[to, pl.ds(h * hb, hb)], save_sem.at[h])
                for h in BOTH]

    def multiply(one, two):
        (slot1, half1, tile1), (slot2, half2, tile2) = one, two
        lhs1, lhs2 = al[slot1, half1], al[slot2, half2]
        for h in BOTH:
            for n in range(hb // slab):
                cols, at = pl.ds(h * hb + n * slab, slab), pl.ds(n * slab, slab)
                acc[h, :, at] = acc[h, :, at] + (
                    _dot(lhs1, tile1[:, cols]) + _dot(lhs2, tile2[:, cols]))

    def forward(t):
        pl.when(t > 0)(lambda: predict(t))
        em_copy(t).wait()
        with jax.named_scope("fw"):
            weigh(t)
        normalise(t)

    def predict(t):
        for_caps(t, lambda rows: _start(own_copies(rows)))
        for_each(t, lambda tt, rows: _start(save_copies(tt, rows)))

        @pl.when(t + 1 < step_count)
        def _():
            em_copy(t + 1).start()

        acc[...] = jnp.zeros(acc.shape, F32)

        def group0(j):
            def ready(rows):
                for half in BOTH:
                    arrived(1, half, rows)

            pl.when(j > 0)(lambda: for_caps(t, ready))
            multiply(*((j, e, bank.at[8 + 2 * j + e]) for e in BOTH))
            for e in BOTH:
                load_tile(8 + 2 * j + e, 2, 2 * j + e)

        def group12(k, j):
            def ready(rows):
                arrived(2 + 2 * j, k, rows)
                arrived(3 + 2 * j, 1 - k, rows)

                @pl.when(j == 0)
                def _():
                    to_partner(2, 4, k, rows).start()
                    to_partner(3, 5, 1 - k, rows).start()

                pl.when(k + j == 0)(lambda: _start([onward(0, rows), onward(1, rows)]))

            for_caps(t, ready)
            at = 2 * k + j
            pl.when((t > 1) | (at > 1))(lambda: in_bank(8 + at))
            multiply((2 + 2 * j, k, bank.at[at]), (3 + 2 * j, 1 - k, bank.at[8 + at]))

        def next_tiles(k):
            def body(e):
                i = 2 * k + e
                pl.when(t < final)(lambda: load_tile(8 + i, 0, i))

                @pl.when(t == final)
                def _():
                    load_turned(8 + i, 12 + i)
                    load_turned(i, 4 + i)

            _loop(2, body)

        def group3(j):
            def ready(rows):
                for half in BOTH:
                    arrived(6 + j, half, rows)

                @pl.when(j == 0)
                def _():
                    for half in BOTH:
                        to_partner(6, 7, half, rows).start()

            for_caps(t, ready)
            multiply(*((6 + j, e, bank.at[4 + 2 * j + e]) for e in BOTH))

        with jax.named_scope("f0"):
            _loop(2, group0)
        pl.when(t == 1)(lambda: _loop(4, in_bank))
        with jax.named_scope("ft"):
            turn_others(t)
        pl.when(t == final)(lambda: _loop(depth, lambda k: strip_copy(0, 0, k).wait()))

        def groups12(k):
            with jax.named_scope("f1"):
                _loop(2, functools.partial(group12, k))
            pl.when((k == 1) & (t > 1) & (t < 4))(lambda: turn(8 + t, 8 + t, False))
            next_tiles(k)

        _loop(2, groups12)
        pl.when(t == 1)(lambda: _loop(4, lambda i: in_bank(4 + i)))
        with jax.named_scope("f3"):
            _loop(2, group3)
        pl.when(t == final)(lambda: _loop(4, lambda i: load_turned(4 + i, 8 + i)))

        def drained(rows):
            for cp in own_copies(rows):
                cp.wait_send()
            for half in BOTH:
                to_partner(2, 4, half, rows).wait_send()
                to_partner(3, 5, half, rows).wait_send()
                to_partner(6, 7, half, rows).wait_send()
                onward(half, rows).wait_send()

        for_caps(t, drained)
        for_each(t, lambda tt, rows: _wait(save_copies(tt, rows)))

    _loop(step_count, forward)

    def post_copy(h):
        return pltpu.make_async_copy(cur.at[h], post_hbm.at[:, pl.ds(pl.multiple_of(h * hb, hb), hb)], post_sem.at[h])

    _loop(2, lambda h: post_copy(h).start())

    back_caps = functools.partial(for_caps, first=2)

    def weights(t):
        def body(i):
            r = rows_of(i)
            rc = rcs[t, r, :]
            live = t < lcol_ref[r, :]
            for k in range(tiles):
                h, col = inner(k)
                val = emv[t % 2, r, lane(k)].astype(F32) * acc[h, r, col] * rc
                strips[h, r, col] = jnp.where(live, val, 0.0).astype(BF16)

        _loop(seqs // 16, body)

    def w_copies(t, rows):
        to = pl.ds(firsts[t - 1], rows)
        return [pltpu.make_async_copy(strips.at[h, pl.ds(0, rows)], w_hbm.at[to, pl.ds(h * hb, hb)], save_sem.at[h])
                for h in BOTH]

    def partial_sums(out, tile):
        for n in range(hb // slab):
            cols = pl.ds(n * slab, slab)
            more = pl.ds(hb + n * slab, slab)
            out[sent, cols] = _dot(strips[0, sent, :], tile[:, cols]) + _dot(strips[1, sent, :], tile[:, more])

    def add_into(out, *terms):
        def body(i):
            r = pl.ds(pl.multiple_of(i * 8, 8), 8)
            val = out[r, :]
            for term in terms:
                val = val + term[r, :]
            out[r, :] = val

        _loop(kept // 8, body)

    def to_core(q, rows):
        m = pl.ds(0, rows)
        return remote(ost.at[q, m], dbuf.at[q, m], d_send.at[q], d_recv.at[q], partner)

    def staged(p):
        n, q = p // 2, p % 2
        return (1 - n % 2) * (2 + n) + q

    def ring_copy(far, p, rows):
        m, q = pl.ds(0, rows), p % 2
        to = dev(1 + (nx - 2) * q, 0)
        src, send = work.at[staged(p), m], s_send.at[p]
        if far:
            return remote(src, trans.at[q, m], send, t_recv.at[q], to)
        half = (p // 2 + q) % 2
        return remote(src, fin.at[q, half, m], send, f_recv.at[q, half], to)

    def freed(sem, q):
        pl.semaphore_signal(sem.at[q], inc=1, device_id={AXIS: dev(nx - 1 - (nx - 2) * q, 0)},
                            device_id_type=pl.DeviceIdType.MESH)

    def backward(idx):
        t = step_count - 1 - idx
        with jax.named_scope("bw"):
            weights(t)
        for_each(t, lambda tt, rows: _start(w_copies(tt, rows)))

        @pl.when(t > 2)
        def _():
            em_copy(t - 2).start()

        def slot_of(p, flip):
            n, q = p // 2, p % 2
            inner = ((n + 1) % 4) // 2
            return inner == 0, (1 - inner) * (8 + 2 * flip + q) + inner * (4 * (1 - q) + 2 * (n - 1) + flip)

        def use(p, flip, out):
            outer, slot = slot_of(p, flip)
            pl.when(outer | (idx == 0))(lambda: in_bank(slot))
            partial_sums(out, bank.at[slot])
            pl.when(p < 2)(lambda: load_turned(slot, slot - 8))
            pl.when((p >= 6) & (t > 2))(lambda: load_turned(slot, slot + 4))

        def for_other(p):
            q = p % 2
            pl.when(p >= 2)(lambda: back_caps(t, lambda rows: to_core(q, rows).wait_send()))
            use(p, 1, ost.at[q])
            pl.when((p >= 2) | (idx > 0))(lambda: pl.semaphore_wait(d_free.at[q], 1))
            back_caps(t, lambda rows: to_core(q, rows).start())

        def for_this(p):
            q = p % 2
            out = work.at[staged(p)]
            pl.when((p // 2 == 2) & (idx == 0))(lambda: post_copy(q).wait())
            pl.when(p >= 6)(lambda: back_caps(t, lambda rows: ring_copy(False, p - 4, rows).wait_send()))
            use(p, 0, out)
            back_caps(t, lambda rows: to_core(q, rows).wait_recv())

            @pl.when(p // 2 == 2)
            def _():
                back_caps(t, lambda rows: ring_copy(True, q, rows).wait_recv())
                add_into(out, dbuf.at[q], trans.at[q])
                pl.when(t > 2)(lambda: freed(t_free, q))

            pl.when(p // 2 != 2)(lambda: add_into(out, dbuf.at[q]))

            @pl.when((p < 6) | (t > 2))
            def _():
                pl.semaphore_signal(d_free.at[q], inc=1, device_id={AXIS: partner}, device_id_type=pl.DeviceIdType.MESH)

            @pl.when(p < 2)
            def _():
                pl.when(idx > 0)(lambda: pl.semaphore_wait(t_free.at[q], 1))
                back_caps(t, lambda rows: ring_copy(True, p, rows).start())

            @pl.when((p >= 2) & (p < 6))
            def _():
                pl.when((idx > 0) & (p < 4))(lambda: pl.semaphore_wait(f_free.at[q], 1))
                back_caps(t, lambda rows: ring_copy(False, p, rows).start())

        def stage(n):
            with jax.named_scope("bo"):
                _loop(2, lambda q: for_other(2 * n + q))
            with jax.named_scope("bt"):
                _loop(2, lambda q: for_this(2 * n + q))

        _loop(4, stage)

        def landed(rows):
            for p in range(2, 6):
                ring_copy(False, p, rows).wait_recv()

        with jax.named_scope("bl"):
            back_caps(t, landed)

        def body(i):
            r = pl.ds(pl.multiple_of(i * 8, 8), 8)
            live = t < lcol_ref[r, :]
            for k in range(tiles):
                h, col = inner(k)
                val = acc[h, r, col] + fin[0, h, r, col] + fin[1, h, r, col]
                acc[h, r, col] = jnp.where(live, val, 1.0)

        _loop(kept // 8, body)

        @pl.when(t > 2)
        def _():
            _loop(2, functools.partial(freed, f_free))

        def drained(rows):
            for q in BOTH:
                to_core(q, rows).wait_send()
                ring_copy(True, q, rows).wait_send()
                ring_copy(False, 4 + q, rows).wait_send()

        with jax.named_scope("bd"):
            back_caps(t, drained)
        for_each(t, lambda tt, rows: _wait(w_copies(tt, rows)))

        @pl.when(t > 2)
        def _():
            em_copy(t - 2).wait()

    acc[...] = jnp.ones(acc.shape, F32)
    _loop(step_count - 2, backward)
    weights(1)
    _start(w_copies(1, caps[0]))
    _wait(w_copies(1, caps[0]))


def _run_recursion(nd, caps, ident, trans_loc, em, init_loc, lcol, lrow):
    step_count, seqs, bs = em.shape
    hb = bs // 2
    kept = max(caps[1:])
    depth = min(8 if kept < seqs else 4, bs // LANES)
    dma = pltpu.SemaphoreType.DMA
    two, credit = dma((2,)), pltpu.SemaphoreType.REGULAR((2,))
    vm, hbm = pl.BlockSpec(memory_space=pltpu.VMEM), pl.BlockSpec(memory_space=pl.ANY)
    scratch = [
        pltpu.VMEM((12, hb, bs), BF16),
        pltpu.VMEM((8, 2, seqs, hb), BF16),
        pltpu.VMEM((6, seqs, hb), F32),
        pltpu.VMEM((2, seqs, bs), BF16),
        pltpu.VMEM((step_count, seqs, LANES), F32),
        pltpu.VMEM((seqs, LANES), F32),
        pltpu.VMEM((8, seqs), F32),
        pltpu.VMEM((nd, 8, seqs), F32),
        pltpu.VMEM((depth, LANES, hb), BF16),
        pltpu.VMEM((2, kept, hb), F32),
        pltpu.VMEM((2, kept, hb), F32),
        pltpu.VMEM((2, kept, hb), F32),
        pltpu.VMEM((2, 2, kept, hb), F32),
        dma((12,)), two, dma((nd, 2)), dma((3, 2)), dma((nd, 2)), two, dma((nd,)), dma((nd,)), two,
        two, dma((depth,)), two, two, dma((6,)), two, dma((2, 2)), credit, credit, credit,
    ]
    return pl.pallas_call(
        functools.partial(_recursion, caps),
        name=f"recursion{ident}",
        out_shape=[
            jax.ShapeDtypeStruct((sum(caps), bs), BF16),
            jax.ShapeDtypeStruct((sum(caps), bs), BF16),
            jax.ShapeDtypeStruct((seqs, bs), F32),
            jax.ShapeDtypeStruct((8, seqs), F32),
            jax.ShapeDtypeStruct(trans_loc.shape, BF16),
        ],
        in_specs=[hbm, hbm, vm, vm, vm],
        out_specs=[hbm, hbm, hbm, vm, hbm],
        scratch_shapes=scratch,
        compiler_params=pltpu.CompilerParams(collective_id=ident, has_side_effects=True, vmem_limit_bytes=67_043_328),
    )(trans_loc, em, init_loc[None, :], lcol, lrow)


def _prepare(choices, tok_ref, len_ref, emt_hbm, em_hbm, lcol_ref, lrow_ref, rank_ref, level_ref,
             table, stable, picked, blocks, stage, table_sem, block_sem, stage_sem):
    step_count, seqs, bs = em_hbm.shape
    deep = blocks.shape[0]
    part = 32
    slab = min(512, bs)
    sub = lax.broadcasted_iota(jnp.int32, (seqs, LANES), 0)
    lan = lax.broadcasted_iota(jnp.int32, (seqs, LANES), 1)
    across = jnp.broadcast_to(len_ref[...].astype(F32), (seqs, seqs))
    down = jnp.transpose(across)
    ahead = (down > across) | ((down == across) & (sub < lan))
    rank = jnp.sum(jnp.where(ahead, 1.0, 0.0), axis=0, keepdims=True)
    rank_ref[...] = jnp.broadcast_to(rank, rank_ref.shape)
    pick = rank == sub.astype(F32)
    lcol = jnp.broadcast_to(jnp.sum(jnp.where(pick, across, 0.0), axis=1, keepdims=True), (seqs, LANES))
    lcol_ref[...] = lcol.astype(jnp.int32)
    lrow_ref[...] = jnp.transpose(lcol)[0:8].astype(jnp.int32)
    mat = jnp.zeros((seqs, LANES), F32)
    for t in range(step_count):
        tok = jnp.sum(jnp.where(pick, tok_ref[t : t + 1, :].astype(F32), 0.0), axis=1, keepdims=True)
        tok = jnp.broadcast_to(tok, (seqs, LANES))
        mat = jnp.where(lan == t, tok, mat)
        picked[t] = tok.astype(jnp.int32) & 7
    table[0:8] = jnp.transpose(mat)[0:8].astype(jnp.int32)
    alive = jnp.sum(jnp.where(across[0:8] > sub[0:8].astype(F32), 1.0, 0.0), axis=1, keepdims=True)
    table[8:16] = jnp.broadcast_to(alive, (8, LANES)).astype(jnp.int32)
    copy = pltpu.make_async_copy(table, stable, table_sem)
    copy.start()
    copy.wait()
    level = jnp.int32(0)
    for k, caps in enumerate(choices):
        for t in range(1, step_count):
            level = jnp.where(stable[8 + t, 0] > caps[t - 1], k + 1, level)
    level_ref[0] = level

    def parts(t):
        return (stable[8 + t, 0] + (part - 1)) // part

    def fetch(t):
        def body(p, carry):
            for k in range(part):
                s = p * part + k
                pltpu.make_async_copy(emt_hbm.at[stable[t, s] >> 3], blocks.at[t % deep, s], block_sem.at[t % deep]).start()
            return carry

        lax.fori_loop(0, parts(t), body, 0)

    def landed(t):
        def body(p, carry):
            pltpu.make_async_copy(emt_hbm.at[pl.ds(0, part)], blocks.at[t % deep, pl.ds(0, part)], block_sem.at[t % deep]).wait()
            return carry

        lax.fori_loop(0, parts(t), body, 0)

    def select(t):
        def body(p, carry):
            r = pl.ds(pl.multiple_of(p * part, part), part)
            at = picked[t, r, :] + 8 * sub[0:part]
            one = jnp.concatenate([jnp.where(lan[0:part] + off == at, 1.0, 0.0) for off in (0, LANES)], axis=1).astype(BF16)
            for n in range(bs // slab):
                cols = pl.ds(n * slab, slab)
                rows = blocks[t % deep, r, :, cols].reshape(part * 8, slab)
                stage[t % 2, r, cols] = _dot(one, rows).astype(BF16)
            return carry

        lax.fori_loop(0, parts(t), body, 0)

    def out_copy(t):
        return pltpu.make_async_copy(stage.at[t % 2], em_hbm.at[t], stage_sem.at[t % 2])

    def position(t):
        pl.when(t >= 2)(lambda: out_copy(t - 2).wait())
        landed(t)
        select(t)
        out_copy(t).start()
        pl.when(t + deep < step_count)(lambda: fetch(t + deep))

    _loop(deep, fetch)
    _loop(step_count, position)
    _loop(2, lambda e: out_copy(step_count - 1 - e).wait())


def _run_prepare(choices, tokens, lengths, emit_loc):
    bs, symbols = emit_loc.shape
    seqs, step_count = tokens.shape
    dma = pltpu.SemaphoreType.DMA
    vm, hbm = pl.BlockSpec(memory_space=pltpu.VMEM), pl.BlockSpec(memory_space=pl.ANY)
    return pl.pallas_call(
        functools.partial(_prepare, choices),
        name="prepare",
        out_shape=[
            jax.ShapeDtypeStruct((step_count, seqs, bs), BF16),
            jax.ShapeDtypeStruct((seqs, LANES), jnp.int32),
            jax.ShapeDtypeStruct((8, seqs), jnp.int32),
            jax.ShapeDtypeStruct((8, seqs), F32),
            jax.ShapeDtypeStruct((1,), jnp.int32),
        ],
        in_specs=[vm, vm, hbm],
        out_specs=[hbm, vm, vm, vm, pl.BlockSpec(memory_space=pltpu.SMEM)],
        scratch_shapes=[
            pltpu.VMEM((16, LANES), jnp.int32),
            pltpu.SMEM((16, LANES), jnp.int32),
            pltpu.VMEM((step_count, seqs, LANES), jnp.int32),
            pltpu.VMEM((4, seqs, 8, bs), BF16),
            pltpu.VMEM((2, seqs, bs), BF16),
            dma, dma((4,)), dma((2,)),
        ],
        compiler_params=pltpu.CompilerParams(vmem_limit_bytes=60_000_000),
    )(tokens.T, lengths[None, :], emit_loc.T.reshape(symbols // 8, 8, bs))


def _counts(trans_hbm, alpha_hbm, w_hbm, post_hbm, ll_ref, rank_ref, counts_hbm, posterior_hbm, loglik_ref,
            alpha, w, diag, out, post, back, in_sem, diag_sem, out_sem, back_sem):
    rows, bs = w.shape
    seqs = post.shape[0]
    steps, tile, _ = diag.shape
    slab = min(512, bs)
    first = lax.axis_index(AXIS) * bs
    loads = [pltpu.make_async_copy(src, dst, in_sem.at[k])
             for k, (src, dst) in enumerate(((post_hbm, post), (w_hbm, w), (alpha_hbm, alpha)))]
    _start(loads)

    def diag_copy(i):
        at = pl.multiple_of(first + i * tile, tile)
        return pltpu.make_async_copy(trans_hbm.at[pl.ds(at, tile)], diag.at[i], diag_sem.at[i])

    def out_copy(i):
        at = pl.multiple_of(i * tile, tile)
        return pltpu.make_async_copy(out.at[i], counts_hbm.at[pl.ds(at, tile)], out_sem.at[i])

    _loop(steps, lambda i: diag_copy(i).start())

    rank = jnp.broadcast_to(rank_ref[0:1, :], (seqs, seqs))
    sub = lax.broadcasted_iota(jnp.int32, (seqs, seqs), 0).astype(F32)
    lan = lax.broadcasted_iota(jnp.int32, (seqs, seqs), 1).astype(F32)
    lls = jnp.transpose(jnp.broadcast_to(ll_ref[0:1, :], (seqs, seqs)))
    loglik_ref[...] = jnp.sum(jnp.where(rank == sub, lls, 0.0), axis=0, keepdims=True)
    order = jnp.where(jnp.transpose(rank) == lan, 1.0, 0.0).astype(BF16)
    loads[0].wait()
    for n in range(bs // slab):
        cols = pl.ds(n * slab, slab)
        rest = post[:, cols]
        total = jnp.zeros(rest.shape, F32)
        for _ in range(3):
            head = rest.astype(BF16)
            rest = rest - head.astype(F32)
            total = total + _dot(order, head)
        back[:, cols] = total
    back_copy = pltpu.make_async_copy(back, posterior_hbm, back_sem)
    back_copy.start()
    _wait(loads[1:])

    def step(i):
        lhs = alpha[:, pl.ds(pl.multiple_of(i * tile, tile), tile)]
        diag_copy(i).wait()
        for n in range(bs // slab):
            cols = pl.ds(n * slab, slab)
            out[i, :, cols] = diag[i, :, cols].astype(F32) * _dot(lhs, w[:, cols], 0)
        out_copy(i).start()

    _loop(steps, step)
    _loop(steps, lambda i: out_copy(i).wait())
    back_copy.wait()


def _run_counts(alphas, ws, trans_loc, post, ll, rank):
    rows, bs = alphas.shape
    seqs = post.shape[0]
    tile = min(256, bs)
    steps = bs // tile
    dma = pltpu.SemaphoreType.DMA
    vm, hbm = pl.BlockSpec(memory_space=pltpu.VMEM), pl.BlockSpec(memory_space=pl.ANY)
    return pl.pallas_call(
        _counts,
        name="counts",
        out_shape=[
            jax.ShapeDtypeStruct((bs, bs), F32),
            jax.ShapeDtypeStruct((seqs, bs), F32),
            jax.ShapeDtypeStruct((1, seqs), F32),
        ],
        in_specs=[hbm, hbm, hbm, hbm, vm, vm],
        out_specs=[hbm, hbm, vm],
        scratch_shapes=[
            pltpu.VMEM((rows, bs), BF16),
            pltpu.VMEM((rows, bs), BF16),
            pltpu.VMEM((steps, tile, bs), BF16),
            pltpu.VMEM((steps, tile, bs), F32),
            pltpu.VMEM((seqs, bs), F32),
            pltpu.VMEM((seqs, bs), F32),
            dma((3,)), dma((steps,)), dma((steps,)), dma,
        ],
        compiler_params=pltpu.CompilerParams(vmem_limit_bytes=60_000_000),
    )(trans_loc, alphas, ws, post, ll, rank)


def _capacities(seqs, step_count, spread):
    caps = []
    for t in range(1, step_count):
        live = (step_count - t) / step_count
        room = spread * math.sqrt((seqs - 1) * live * (1 - live))
        caps.append(min(seqs, 8 * math.ceil(((seqs - 1) * live + 1 + room) / 8)))
    return tuple(caps)


def solution(mesh):
    nd = mesh.shape[AXIS]

    def local_run(trans_loc, emit_loc, init_loc, tokens_loc, lengths_loc):
        seqs, step_count = tokens_loc.shape
        choices = [_capacities(seqs, step_count, spread) for spread in (2.7, 4.1)]
        em, lcol, lrow, rank, level = _run_prepare(choices, tokens_loc, lengths_loc, emit_loc)

        def run(ident, caps, trans, em, init, lcol, lrow, rank):
            alphas, ws, post, ll, _ = _run_recursion(nd, caps, ident, trans, em, init, lcol, lrow)
            return _run_counts(alphas, ws, trans, post, ll, rank)

        choices.append((seqs,) * (step_count - 1))
        runs = [functools.partial(run, k, caps) for k, caps in enumerate(choices)]
        counts, posterior, loglik = lax.switch(level[0], runs, trans_loc, em, init_loc, lcol, lrow, rank)
        return loglik[0], posterior, counts

    return jax.shard_map(
        local_run,
        mesh=mesh,
        in_specs=(P(None, AXIS), P(AXIS, None), P(AXIS), P("seqs", None), P("seqs")),
        out_specs=(P("seqs"), P("seqs", AXIS), P(("seqs", AXIS), None)),
        check_vma=False,
    )
```

```python
import functools
import math

import jax
import jax.numpy as jnp
from jax import lax
from jax.experimental import pallas as pl
from jax.experimental.pallas import tpu as pltpu
from jax.sharding import PartitionSpec as P

AXIS = "states"
LANES = 128
BOTH = (0, 1)
F32 = jnp.float32
BF16 = jnp.bfloat16


def _dot(a, b, over_a=1, over_b=0):
    dims = (((over_a,), (over_b,)), ((), ()))
    return lax.dot_general(a, b, dims, preferred_element_type=F32)


def _start(copies):
    for cp in copies:
        cp.start()


def _wait(copies):
    for cp in copies:
        cp.wait()


def _loop(n, body):
    def step(i, carry):
        body(i)
        return carry

    lax.fori_loop(0, n, step, 0)


def _recursion(caps, a_hbm, em_hbm, pi_ref, lcol_ref, lrow_ref, al_hbm, w_hbm, post_hbm, ll_ref, turned_hbm,
               bank, al, work, emv, rcs, sbuf, csend, cbuf, strips, ost, dbuf, trans, fin,
               bank_sem, em_sem, al_recv, own_send, part_send, on_send, c_send, c_recv, save_sem, post_sem,
               strip_sem, d_send, d_recv, s_send, t_recv, f_recv, t_free, f_free, d_free):
    nd = cbuf.shape[0]
    nx = nd // 2
    step_count, seqs, bs = em_hbm.shape
    hb = bs // 2
    firsts = [sum(caps[:t]) for t in range(step_count)]
    slab = min(512, hb)
    tiles = bs // LANES
    kept = max(caps[1:])
    sent = pl.ds(0, kept)
    final = step_count - 1
    g = lax.axis_index(AXIS)
    x, c = g // 2, g % 2

    def dev(dx, flip):
        return ((x + dx) % nx) * 2 + (c + flip) % 2

    partner, right, left = dev(0, 1), dev(1, 0), dev(nx - 1, 0)

    def remote(src, dst, send, recv, to):
        return pltpu.make_async_remote_copy(
            src_ref=src, dst_ref=dst, send_sem=send, recv_sem=recv,
            device_id={AXIS: to}, device_id_type=pl.DeviceIdType.MESH)

    def pick(t, fn, lo, hi):
        if hi - lo == 1:
            fn(lo)
        else:
            mid = (lo + hi) // 2
            lax.cond(t < mid, lambda: pick(t, fn, lo, mid), lambda: pick(t, fn, mid, hi))

    def for_each(t, fn):
        pick(t, lambda tt: fn(tt, caps[tt - 1]), 1, step_count)

    def for_caps(t, fn, first=1):
        if len(set(caps)) == 1:
            fn(caps[0])
        else:
            pick(t, lambda tt: fn(caps[tt - 1]), first, step_count)

    acc, cur = work.at[pl.ds(0, 2)], work.at[pl.ds(4, 2)]

    def tile_row(group, i):
        if group == 0:
            src, half = dev(0, i // 2), i % 2
        elif group == 1:
            src, half = dev(nx - 1, i % 2), i // 2
        elif group == 2:
            src, half = dev(1, i % 2), 1 - i // 2
        else:
            src, half = dev(2, i // 2), i % 2
        return src * bs + half * hb

    def load(slot, row, src):
        pltpu.make_async_copy(src.at[pl.ds(pl.multiple_of(row, hb), hb)], bank.at[slot], bank_sem.at[slot]).start()

    def load_tile(slot, group, i):
        load(slot, tile_row(group, i), a_hbm)

    def load_turned(slot, number):
        load(slot, number * hb, turned_hbm)

    def in_bank(slot):
        pltpu.make_async_copy(a_hbm.at[pl.ds(0, hb)], bank.at[slot], bank_sem.at[slot]).wait()

    depth = strips.shape[0]
    bunch = min(2, depth)

    def strip_copy(number, unit, k):
        rows = pl.ds(pl.multiple_of(number * hb + (unit % (tiles // 2)) * LANES, LANES), LANES)
        cols = pl.ds(pl.multiple_of((unit // (tiles // 2)) * hb, hb), hb)
        return pltpu.make_async_copy(strips.at[k], turned_hbm.at[rows, cols], strip_sem.at[k])

    def turn(slot, number, first):
        def body(i):
            units = [bunch * i + e for e in range(bunch)]

            @pl.when(jnp.logical_not(first) | (bunch * i >= depth))
            def _():
                for u in units:
                    strip_copy(0, 0, u % depth).wait()

            for u in units:
                strips[u % depth] = jnp.transpose(bank[slot, :, pl.ds(pl.multiple_of(u * LANES, LANES), LANES)])
            for u in units:
                strip_copy(number, u, u % depth).start()

        _loop(tiles // bunch, body)

    def turn_own(t):
        each = -(-7 // final)

        def body(e):
            n = t * each + e
            far = n // 4
            pl.when(far == 0)(lambda: in_bank(8 + n))
            pl.when(n < 7)(lambda: turn(8 + n - far * 7, n + far * 9, n == 0))

        _loop(each, body)
        _loop(4, lambda i: pl.when((i < t * each) | (i >= t * each + each))(lambda: in_bank(8 + i)))

    def turn_others(t):
        each = -(-5 // (final - 1))

        def body(e):
            n = (t - 1) * each + e
            right = (e + LANES - each) // LANES
            slot = (1 - right) * n + right * (8 + e - each)
            number = (1 - right) * (4 + n + 4 * (n // 4)) + right * slot
            pl.when((right == 1) & (t == 1))(lambda: in_bank(slot))
            pl.when(((right == 1) & (t == 1)) | ((right == 0) & (n < 5)))(lambda: turn(slot, number, False))

        pl.when(t < final)(lambda: _loop(each + 2, body))

    def em_copy(t):
        return pltpu.make_async_copy(em_hbm.at[t], emv.at[t % 2], em_sem.at[t % 2])

    _loop(2, lambda t: em_copy(t).start())
    _loop(4, lambda i: load_tile(8 + i, 0, i))
    _loop(4, lambda i: load_tile(i, 1, i))

    barrier = pltpu.get_barrier_semaphore()
    for k in range(1, nd):
        pl.semaphore_signal(barrier, inc=1, device_id={AXIS: (g + k) % nd}, device_id_type=pl.DeviceIdType.MESH)
    pl.semaphore_wait(barrier, nd - 1)

    def rows_of(i):
        return pl.ds(pl.multiple_of(i * 16, 16), 16)

    def lane(k):
        return pl.ds(k * LANES, LANES)

    def inner(k):
        return (k * LANES) // hb, pl.ds((k * LANES) % hb, LANES)

    def weigh(t):
        def body(i):
            r = rows_of(i)
            total = jnp.zeros((16, LANES), F32)
            for k in range(tiles):
                e = emv[t % 2, r, lane(k)].astype(F32)
                h, col = inner(k)
                mass = acc[h, r, col] * e
                acc[h, r, col] = mass
                total = total + mass
            sbuf[r, :] = total

        _loop(seqs // 16, body)

    def normalise(t):
        row = jnp.sum(jnp.transpose(sbuf[...]), axis=0, keepdims=True)
        wide = jnp.broadcast_to(row, csend.shape)
        csend[...] = wide
        cbuf[g] = wide
        peers = [dev(dx, flip) for dx in (2, 1, nx - 1, 0) for flip in BOTH][: nd - 2] + [partner]
        copies = [remote(csend, cbuf.at[g], c_send.at[k], c_recv.at[g], to) for k, to in enumerate(peers)]
        _start(copies)

        with jax.named_scope("ft"):
            @pl.when(t < final)
            def _():
                turn_own(t)

        with jax.named_scope("fx"):
            for k, frm in enumerate(peers):
                remote(csend, cbuf.at[frm], c_send.at[k], c_recv.at[frm], frm).wait_recv()
        norm = cbuf[0, 0:1, :]
        for d in range(1, nd):
            norm = norm + cbuf[d, 0:1, :]
        rcs[t] = 1.0 / jnp.transpose(jnp.broadcast_to(norm, (LANES, LANES)))
        ll_ref[...] = ll_ref[...] + jnp.where(t < lrow_ref[...], jnp.log(jnp.broadcast_to(norm, ll_ref.shape)), 0.0)

        def body(i):
            r = rows_of(i)
            rc = rcs[t, r, :]
            live = t < lcol_ref[r, :]
            for k in range(tiles):
                h, col = inner(k)
                val = jnp.where(live, acc[h, r, col] * rc, cur[h, r, col])
                cur[h, r, col] = val
                al[0, h, r, col] = val.astype(BF16)

        _loop(seqs // 16, body)
        for cp in copies:
            cp.wait_send()

    ll_ref[...] = jnp.zeros_like(ll_ref)
    for h in BOTH:
        acc[h] = jnp.broadcast_to(pi_ref[:, h * hb : (h + 1) * hb], (seqs, hb))

    def own_copies(rows):
        m = pl.ds(0, rows)
        out = [remote(al.at[0, h, m], al.at[1, h, m], own_send.at[0, h], al_recv.at[1, h], partner) for h in BOTH]
        for h in BOTH:
            out.append(remote(al.at[0, h, m], al.at[2, h, m], own_send.at[1, h], al_recv.at[2, h], right))
            out.append(remote(al.at[0, 1 - h, m], al.at[3, 1 - h, m], own_send.at[2, 1 - h], al_recv.at[3, 1 - h], left))
        return out

    def to_partner(slot, to_slot, half, rows):
        m = pl.ds(0, rows)
        return remote(al.at[slot, half, m], al.at[to_slot, half, m], part_send.at[slot, half], al_recv.at[to_slot, half], partner)

    def onward(s, rows):
        m = pl.ds(0, rows)
        return remote(al.at[2 + s, s, m], al.at[6, s, m], on_send.at[s], al_recv.at[6, s], dev(1 + (nx - 2) * s, 0))

    def arrived(slot, half, rows):
        m = pl.ds(0, rows)
        remote(al.at[slot, half, m], al.at[slot, half, m], part_send.at[slot, half], al_recv.at[slot, half], partner).wait_recv()

    def save_copies(t, rows):
        to = pl.ds(firsts[t - 1], rows)
        return [pltpu.make_async_copy(al.at[0, h, pl.ds(0, rows)], al_hbm.at[to, pl.ds(h * hb, hb)], save_sem.at[h])
                for h in BOTH]

    def multiply(one, two):
        (slot1, half1, tile1), (slot2, half2, tile2) = one, two
        lhs1, lhs2 = al[slot1, half1], al[slot2, half2]
        for h in BOTH:
            for n in range(hb // slab):
                cols, at = pl.ds(h * hb + n * slab, slab), pl.ds(n * slab, slab)
                acc[h, :, at] = acc[h, :, at] + (
                    _dot(lhs1, tile1[:, cols]) + _dot(lhs2, tile2[:, cols]))

    def forward(t):
        pl.when(t > 0)(lambda: predict(t))
        em_copy(t).wait()
        with jax.named_scope("fw"):
            weigh(t)
        normalise(t)

    def predict(t):
        for_caps(t, lambda rows: _start(own_copies(rows)))
        for_each(t, lambda tt, rows: _start(save_copies(tt, rows)))

        @pl.when(t + 1 < step_count)
        def _():
            em_copy(t + 1).start()

        acc[...] = jnp.zeros(acc.shape, F32)

        def group0(j):
            def ready(rows):
                for half in BOTH:
                    arrived(1, half, rows)

            pl.when(j > 0)(lambda: for_caps(t, ready))
            multiply(*((j, e, bank.at[8 + 2 * j + e]) for e in BOTH))
            for e in BOTH:
                load_tile(8 + 2 * j + e, 2, 2 * j + e)

        def group12(k, j):
            def ready(rows):
                arrived(2 + 2 * j, k, rows)
                arrived(3 + 2 * j, 1 - k, rows)

                @pl.when(j == 0)
                def _():
                    to_partner(2, 4, k, rows).start()
                    to_partner(3, 5, 1 - k, rows).start()

                pl.when(k + j == 0)(lambda: _start([onward(0, rows), onward(1, rows)]))

            for_caps(t, ready)
            at = 2 * k + j
            pl.when((t > 1) | (at > 1))(lambda: in_bank(8 + at))
            multiply((2 + 2 * j, k, bank.at[at]), (3 + 2 * j, 1 - k, bank.at[8 + at]))

        def next_tiles(k):
            def body(e):
                i = 2 * k + e
                pl.when(t < final)(lambda: load_tile(8 + i, 0, i))

                @pl.when(t == final)
                def _():
                    load_turned(8 + i, 12 + i)
                    load_turned(i, 4 + i)

            _loop(2, body)

        def group3(j):
            def ready(rows):
                for half in BOTH:
                    arrived(6 + j, half, rows)

                @pl.when(j == 0)
                def _():
                    for half in BOTH:
                        to_partner(6, 7, half, rows).start()

            for_caps(t, ready)
            multiply(*((6 + j, e, bank.at[4 + 2 * j + e]) for e in BOTH))

        with jax.named_scope("f0"):
            _loop(2, group0)

        @pl.when(t == 1)
        def _():
            _loop(4, lambda i: load_tile(4 + i, 3, i))
            _loop(4, in_bank)

        with jax.named_scope("ft"):
            turn_others(t)
        pl.when(t == final)(lambda: _loop(depth, lambda k: strip_copy(0, 0, k).wait()))

        def groups12(k):
            with jax.named_scope("f1"):
                _loop(2, functools.partial(group12, k))
            pl.when((k == 1) & (t > 1) & (t < 4))(lambda: turn(8 + t, 8 + t, False))
            next_tiles(k)

        _loop(2, groups12)
        pl.when(t == 1)(lambda: _loop(4, lambda i: in_bank(4 + i)))
        with jax.named_scope("f3"):
            _loop(2, group3)
        pl.when(t == final)(lambda: _loop(4, lambda i: load_turned(4 + i, 8 + i)))

        def drained(rows):
            for cp in own_copies(rows):
                cp.wait_send()
            for half in BOTH:
                to_partner(2, 4, half, rows).wait_send()
                to_partner(3, 5, half, rows).wait_send()
                to_partner(6, 7, half, rows).wait_send()
                onward(half, rows).wait_send()

        for_caps(t, drained)
        for_each(t, lambda tt, rows: _wait(save_copies(tt, rows)))

    _loop(step_count, forward)

    def post_copy(h):
        return pltpu.make_async_copy(cur.at[h], post_hbm.at[:, pl.ds(pl.multiple_of(h * hb, hb), hb)], post_sem.at[h])

    _loop(2, lambda h: post_copy(h).start())

    back_caps = functools.partial(for_caps, first=2)

    def weights(t):
        def body(i):
            r = rows_of(i)
            rc = rcs[t, r, :]
            live = t < lcol_ref[r, :]
            for k in range(tiles):
                h, col = inner(k)
                val = emv[t % 2, r, lane(k)].astype(F32) * acc[h, r, col] * rc
                strips[h, r, col] = jnp.where(live, val, 0.0).astype(BF16)

        _loop(seqs // 16, body)

    def w_copies(t, rows):
        to = pl.ds(firsts[t - 1], rows)
        return [pltpu.make_async_copy(strips.at[h, pl.ds(0, rows)], w_hbm.at[to, pl.ds(h * hb, hb)], save_sem.at[h])
                for h in BOTH]

    def partial_sums(out, tile):
        for n in range(hb // slab):
            cols = pl.ds(n * slab, slab)
            more = pl.ds(hb + n * slab, slab)
            out[sent, cols] = _dot(strips[0, sent, :], tile[:, cols]) + _dot(strips[1, sent, :], tile[:, more])

    def add_into(out, *terms):
        def body(i):
            r = pl.ds(pl.multiple_of(i * 8, 8), 8)
            val = out[r, :]
            for term in terms:
                val = val + term[r, :]
            out[r, :] = val

        _loop(kept // 8, body)

    def to_core(q, rows):
        m = pl.ds(0, rows)
        return remote(ost.at[q, m], dbuf.at[q, m], d_send.at[q], d_recv.at[q], partner)

    def staged(p):
        n, q = p // 2, p % 2
        return (1 - n % 2) * (2 + n) + q

    def ring_copy(far, p, rows):
        m, q = pl.ds(0, rows), p % 2
        to = dev(1 + (nx - 2) * q, 0)
        src, send = work.at[staged(p), m], s_send.at[p]
        if far:
            return remote(src, trans.at[q, m], send, t_recv.at[q], to)
        half = (p // 2 + q) % 2
        return remote(src, fin.at[q, half, m], send, f_recv.at[q, half], to)

    def freed(sem, q):
        pl.semaphore_signal(sem.at[q], inc=1, device_id={AXIS: dev(nx - 1 - (nx - 2) * q, 0)},
                            device_id_type=pl.DeviceIdType.MESH)

    def backward(idx):
        t = step_count - 1 - idx
        with jax.named_scope("bw"):
            weights(t)
        for_each(t, lambda tt, rows: _start(w_copies(tt, rows)))

        @pl.when(t > 2)
        def _():
            em_copy(t - 2).start()

        def slot_of(p, flip):
            n, q = p // 2, p % 2
            inner = ((n + 1) % 4) // 2
            return inner == 0, (1 - inner) * (8 + 2 * flip + q) + inner * (4 * (1 - q) + 2 * (n - 1) + flip)

        def products(n, flip, outs):
            outer, _ = slot_of(2 * n, flip)
            slots = [slot_of(2 * n + q, flip)[1] for q in BOTH]

            @pl.when(outer | (idx == 0))
            def _():
                for slot in slots:
                    in_bank(slot)

            for slot, out in zip(slots, outs):
                partial_sums(out, bank.at[slot])

            @pl.when(n == 0)
            def _():
                for slot in slots:
                    load_turned(slot, slot - 8)

            @pl.when((n == 3) & (t > 2))
            def _():
                for slot in slots:
                    load_turned(slot, slot + 4)

        def for_other(n):
            def drain(rows):
                for q in BOTH:
                    to_core(q, rows).wait_send()

            pl.when(n > 0)(lambda: back_caps(t, drain))
            products(n, 1, [ost.at[q] for q in BOTH])

            @pl.when((n > 0) | (idx > 0))
            def _():
                for q in BOTH:
                    pl.semaphore_wait(d_free.at[q], 1)

            back_caps(t, lambda rows: _start([to_core(q, rows) for q in BOTH]))

        def for_this(n):
            outs = [work.at[staged(2 * n + q)] for q in BOTH]
            pl.when((n == 2) & (idx == 0))(lambda: _wait([post_copy(q) for q in BOTH]))

            def drain(rows):
                for q in BOTH:
                    ring_copy(False, 2 + q, rows).wait_send()

            pl.when(n == 3)(lambda: back_caps(t, drain))
            products(n, 0, outs)
            for q, out in enumerate(outs):
                p = 2 * n + q
                back_caps(t, lambda rows: to_core(q, rows).wait_recv())

                @pl.when(n == 2)
                def _():
                    back_caps(t, lambda rows: ring_copy(True, q, rows).wait_recv())
                    add_into(out, dbuf.at[q], trans.at[q])
                    pl.when(t > 2)(lambda: freed(t_free, q))

                pl.when(n != 2)(lambda: add_into(out, dbuf.at[q]))

                @pl.when((n < 3) | (t > 2))
                def _():
                    pl.semaphore_signal(d_free.at[q], inc=1, device_id={AXIS: partner}, device_id_type=pl.DeviceIdType.MESH)

                @pl.when(n == 0)
                def _():
                    pl.when(idx > 0)(lambda: pl.semaphore_wait(t_free.at[q], 1))
                    back_caps(t, lambda rows: ring_copy(True, q, rows).start())

                @pl.when((n == 1) | (n == 2))
                def _():
                    pl.when((idx > 0) & (n == 1))(lambda: pl.semaphore_wait(f_free.at[q], 1))
                    back_caps(t, lambda rows: ring_copy(False, p, rows).start())

        def stage(n):
            with jax.named_scope("bo"):
                for_other(n)
            with jax.named_scope("bt"):
                for_this(n)

        _loop(4, stage)

        def landed(rows):
            for p in range(2, 6):
                ring_copy(False, p, rows).wait_recv()

        with jax.named_scope("bl"):
            back_caps(t, landed)

        def body(i):
            r = pl.ds(pl.multiple_of(i * 8, 8), 8)
            live = t < lcol_ref[r, :]
            for k in range(tiles):
                h, col = inner(k)
                val = acc[h, r, col] + fin[0, h, r, col] + fin[1, h, r, col]
                acc[h, r, col] = jnp.where(live, val, 1.0)

        _loop(kept // 8, body)

        @pl.when(t > 2)
        def _():
            _loop(2, functools.partial(freed, f_free))

        def drained(rows):
            for q in BOTH:
                to_core(q, rows).wait_send()
                ring_copy(True, q, rows).wait_send()
                ring_copy(False, 4 + q, rows).wait_send()

        with jax.named_scope("bd"):
            back_caps(t, drained)
        for_each(t, lambda tt, rows: _wait(w_copies(tt, rows)))

        @pl.when(t > 2)
        def _():
            em_copy(t - 2).wait()

    acc[...] = jnp.ones(acc.shape, F32)
    _loop(step_count - 2, backward)
    weights(1)
    _start(w_copies(1, caps[0]))
    _wait(w_copies(1, caps[0]))


def _run_recursion(nd, caps, ident, trans_loc, em, init_loc, lcol, lrow):
    step_count, seqs, bs = em.shape
    hb = bs // 2
    kept = max(caps[1:])
    depth = min(8 if kept < seqs else 4, bs // LANES)
    dma = pltpu.SemaphoreType.DMA
    two, credit = dma((2,)), pltpu.SemaphoreType.REGULAR((2,))
    vm, hbm = pl.BlockSpec(memory_space=pltpu.VMEM), pl.BlockSpec(memory_space=pl.ANY)
    scratch = [
        pltpu.VMEM((12, hb, bs), BF16),
        pltpu.VMEM((8, 2, seqs, hb), BF16),
        pltpu.VMEM((6, seqs, hb), F32),
        pltpu.VMEM((2, seqs, bs), BF16),
        pltpu.VMEM((step_count, seqs, LANES), F32),
        pltpu.VMEM((seqs, LANES), F32),
        pltpu.VMEM((8, seqs), F32),
        pltpu.VMEM((nd, 8, seqs), F32),
        pltpu.VMEM((depth, LANES, hb), BF16),
        pltpu.VMEM((2, kept, hb), F32),
        pltpu.VMEM((2, kept, hb), F32),
        pltpu.VMEM((2, kept, hb), F32),
        pltpu.VMEM((2, 2, kept, hb), F32),
        dma((12,)), two, dma((nd, 2)), dma((3, 2)), dma((nd, 2)), two, dma((nd,)), dma((nd,)), two,
        two, dma((depth,)), two, two, dma((6,)), two, dma((2, 2)), credit, credit, credit,
    ]
    return pl.pallas_call(
        functools.partial(_recursion, caps),
        name=f"recursion{ident}",
        out_shape=[
            jax.ShapeDtypeStruct((sum(caps), bs), BF16),
            jax.ShapeDtypeStruct((sum(caps), bs), BF16),
            jax.ShapeDtypeStruct((seqs, bs), F32),
            jax.ShapeDtypeStruct((8, seqs), F32),
            jax.ShapeDtypeStruct(trans_loc.shape, BF16),
        ],
        in_specs=[hbm, hbm, vm, vm, vm],
        out_specs=[hbm, hbm, hbm, vm, hbm],
        scratch_shapes=scratch,
        compiler_params=pltpu.CompilerParams(collective_id=ident, has_side_effects=True, vmem_limit_bytes=67_043_328),
    )(trans_loc, em, init_loc[None, :], lcol, lrow)


def _prepare(choices, tok_ref, len_ref, emt_hbm, em_hbm, lcol_ref, lrow_ref, rank_ref, level_ref,
             table, stable, picked, blocks, stage, table_sem, block_sem, stage_sem):
    step_count, seqs, bs = em_hbm.shape
    deep = blocks.shape[0]
    part = 32
    slab = min(512, bs)
    sub = lax.broadcasted_iota(jnp.int32, (seqs, LANES), 0)
    lan = lax.broadcasted_iota(jnp.int32, (seqs, LANES), 1)
    across = jnp.broadcast_to(len_ref[...].astype(F32), (seqs, seqs))
    down = jnp.transpose(across)
    ahead = (down > across) | ((down == across) & (sub < lan))
    rank = jnp.sum(jnp.where(ahead, 1.0, 0.0), axis=0, keepdims=True)
    rank_ref[...] = jnp.broadcast_to(rank, rank_ref.shape)
    pick = rank == sub.astype(F32)
    lcol = jnp.broadcast_to(jnp.sum(jnp.where(pick, across, 0.0), axis=1, keepdims=True), (seqs, LANES))
    lcol_ref[...] = lcol.astype(jnp.int32)
    lrow_ref[...] = jnp.transpose(lcol)[0:8].astype(jnp.int32)
    mat = jnp.zeros((seqs, LANES), F32)
    for t in range(step_count):
        tok = jnp.sum(jnp.where(pick, tok_ref[t : t + 1, :].astype(F32), 0.0), axis=1, keepdims=True)
        tok = jnp.broadcast_to(tok, (seqs, LANES))
        mat = jnp.where(lan == t, tok, mat)
        picked[t] = tok.astype(jnp.int32) & 7
    table[0:8] = jnp.transpose(mat)[0:8].astype(jnp.int32)
    alive = jnp.sum(jnp.where(across[0:8] > sub[0:8].astype(F32), 1.0, 0.0), axis=1, keepdims=True)
    table[8:16] = jnp.broadcast_to(alive, (8, LANES)).astype(jnp.int32)
    copy = pltpu.make_async_copy(table, stable, table_sem)
    copy.start()
    copy.wait()
    level = jnp.int32(0)
    for k, caps in enumerate(choices):
        for t in range(1, step_count):
            level = jnp.where(stable[8 + t, 0] > caps[t - 1], k + 1, level)
    level_ref[0] = level

    def parts(t):
        return (stable[8 + t, 0] + (part - 1)) // part

    def fetch(t):
        def body(p, carry):
            for k in range(part):
                s = p * part + k
                pltpu.make_async_copy(emt_hbm.at[stable[t, s] >> 3], blocks.at[t % deep, s], block_sem.at[t % deep]).start()
            return carry

        lax.fori_loop(0, parts(t), body, 0)

    def landed(t):
        def body(p, carry):
            pltpu.make_async_copy(emt_hbm.at[pl.ds(0, part)], blocks.at[t % deep, pl.ds(0, part)], block_sem.at[t % deep]).wait()
            return carry

        lax.fori_loop(0, parts(t), body, 0)

    def select(t):
        def body(p, carry):
            r = pl.ds(pl.multiple_of(p * part, part), part)
            at = picked[t, r, :] + 8 * sub[0:part]
            one = jnp.concatenate([jnp.where(lan[0:part] + off == at, 1.0, 0.0) for off in (0, LANES)], axis=1).astype(BF16)
            for n in range(bs // slab):
                cols = pl.ds(n * slab, slab)
                rows = blocks[t % deep, r, :, cols].reshape(part * 8, slab)
                stage[t % 2, r, cols] = _dot(one, rows).astype(BF16)
            return carry

        lax.fori_loop(0, parts(t), body, 0)

    def out_copy(t):
        return pltpu.make_async_copy(stage.at[t % 2], em_hbm.at[t], stage_sem.at[t % 2])

    def position(t):
        pl.when(t >= 2)(lambda: out_copy(t - 2).wait())
        landed(t)
        select(t)
        out_copy(t).start()
        pl.when(t + deep < step_count)(lambda: fetch(t + deep))

    _loop(deep, fetch)
    _loop(step_count, position)
    _loop(2, lambda e: out_copy(step_count - 1 - e).wait())


def _run_prepare(choices, tokens, lengths, emit_loc):
    bs, symbols = emit_loc.shape
    seqs, step_count = tokens.shape
    dma = pltpu.SemaphoreType.DMA
    vm, hbm = pl.BlockSpec(memory_space=pltpu.VMEM), pl.BlockSpec(memory_space=pl.ANY)
    return pl.pallas_call(
        functools.partial(_prepare, choices),
        name="prepare",
        out_shape=[
            jax.ShapeDtypeStruct((step_count, seqs, bs), BF16),
            jax.ShapeDtypeStruct((seqs, LANES), jnp.int32),
            jax.ShapeDtypeStruct((8, seqs), jnp.int32),
            jax.ShapeDtypeStruct((8, seqs), F32),
            jax.ShapeDtypeStruct((1,), jnp.int32),
        ],
        in_specs=[vm, vm, hbm],
        out_specs=[hbm, vm, vm, vm, pl.BlockSpec(memory_space=pltpu.SMEM)],
        scratch_shapes=[
            pltpu.VMEM((16, LANES), jnp.int32),
            pltpu.SMEM((16, LANES), jnp.int32),
            pltpu.VMEM((step_count, seqs, LANES), jnp.int32),
            pltpu.VMEM((4, seqs, 8, bs), BF16),
            pltpu.VMEM((2, seqs, bs), BF16),
            dma, dma((4,)), dma((2,)),
        ],
        compiler_params=pltpu.CompilerParams(vmem_limit_bytes=60_000_000),
    )(tokens.T, lengths[None, :], emit_loc.T.reshape(symbols // 8, 8, bs))


def _counts(trans_hbm, alpha_hbm, w_hbm, post_hbm, ll_ref, rank_ref, counts_hbm, posterior_hbm, loglik_ref,
            alpha, w, diag, out, post, back, in_sem, diag_sem, out_sem, back_sem):
    rows, bs = w.shape
    seqs = post.shape[0]
    steps, tile, _ = diag.shape
    slab = min(512, bs)
    first = lax.axis_index(AXIS) * bs
    loads = [pltpu.make_async_copy(src, dst, in_sem.at[k])
             for k, (src, dst) in enumerate(((post_hbm, post), (w_hbm, w), (alpha_hbm, alpha)))]
    _start(loads)

    def diag_copy(i):
        at = pl.multiple_of(first + i * tile, tile)
        return pltpu.make_async_copy(trans_hbm.at[pl.ds(at, tile)], diag.at[i], diag_sem.at[i])

    def out_copy(i):
        at = pl.multiple_of(i * tile, tile)
        return pltpu.make_async_copy(out.at[i], counts_hbm.at[pl.ds(at, tile)], out_sem.at[i])

    _loop(steps, lambda i: diag_copy(i).start())

    rank = jnp.broadcast_to(rank_ref[0:1, :], (seqs, seqs))
    sub = lax.broadcasted_iota(jnp.int32, (seqs, seqs), 0).astype(F32)
    lan = lax.broadcasted_iota(jnp.int32, (seqs, seqs), 1).astype(F32)
    lls = jnp.transpose(jnp.broadcast_to(ll_ref[0:1, :], (seqs, seqs)))
    loglik_ref[...] = jnp.sum(jnp.where(rank == sub, lls, 0.0), axis=0, keepdims=True)
    order = jnp.where(jnp.transpose(rank) == lan, 1.0, 0.0).astype(BF16)
    loads[0].wait()
    for n in range(bs // slab):
        cols = pl.ds(n * slab, slab)
        rest = post[:, cols]
        total = jnp.zeros(rest.shape, F32)
        for _ in range(3):
            head = rest.astype(BF16)
            rest = rest - head.astype(F32)
            total = total + _dot(order, head)
        back[:, cols] = total
    back_copy = pltpu.make_async_copy(back, posterior_hbm, back_sem)
    back_copy.start()
    _wait(loads[1:])

    def step(i):
        lhs = alpha[:, pl.ds(pl.multiple_of(i * tile, tile), tile)]
        diag_copy(i).wait()
        for n in range(bs // slab):
            cols = pl.ds(n * slab, slab)
            out[i, :, cols] = diag[i, :, cols].astype(F32) * _dot(lhs, w[:, cols], 0)
        out_copy(i).start()

    _loop(steps, step)
    _loop(steps, lambda i: out_copy(i).wait())
    back_copy.wait()


def _run_counts(alphas, ws, trans_loc, post, ll, rank):
    rows, bs = alphas.shape
    seqs = post.shape[0]
    tile = min(256, bs)
    steps = bs // tile
    dma = pltpu.SemaphoreType.DMA
    vm, hbm = pl.BlockSpec(memory_space=pltpu.VMEM), pl.BlockSpec(memory_space=pl.ANY)
    return pl.pallas_call(
        _counts,
        name="counts",
        out_shape=[
            jax.ShapeDtypeStruct((bs, bs), F32),
            jax.ShapeDtypeStruct((seqs, bs), F32),
            jax.ShapeDtypeStruct((1, seqs), F32),
        ],
        in_specs=[hbm, hbm, hbm, hbm, vm, vm],
        out_specs=[hbm, hbm, vm],
        scratch_shapes=[
            pltpu.VMEM((rows, bs), BF16),
            pltpu.VMEM((rows, bs), BF16),
            pltpu.VMEM((steps, tile, bs), BF16),
            pltpu.VMEM((steps, tile, bs), F32),
            pltpu.VMEM((seqs, bs), F32),
            pltpu.VMEM((seqs, bs), F32),
            dma((3,)), dma((steps,)), dma((steps,)), dma,
        ],
        compiler_params=pltpu.CompilerParams(vmem_limit_bytes=60_000_000),
    )(trans_loc, alphas, ws, post, ll, rank)


def _capacities(seqs, step_count, spread):
    caps = []
    for t in range(1, step_count):
        live = (step_count - t) / step_count
        room = spread * math.sqrt((seqs - 1) * live * (1 - live))
        caps.append(min(seqs, 8 * math.ceil(((seqs - 1) * live + 1 + room) / 8)))
    return tuple(caps)


def solution(mesh):
    nd = mesh.shape[AXIS]

    def local_run(trans_loc, emit_loc, init_loc, tokens_loc, lengths_loc):
        seqs, step_count = tokens_loc.shape
        choices = [_capacities(seqs, step_count, spread) for spread in (2.7, 4.1)]
        em, lcol, lrow, rank, level = _run_prepare(choices, tokens_loc, lengths_loc, emit_loc)

        def run(ident, caps, trans, em, init, lcol, lrow, rank):
            alphas, ws, post, ll, _ = _run_recursion(nd, caps, ident, trans, em, init, lcol, lrow)
            return _run_counts(alphas, ws, trans, post, ll, rank)

        choices.append((seqs,) * (step_count - 1))
        runs = [functools.partial(run, k, caps) for k, caps in enumerate(choices)]
        counts, posterior, loglik = lax.switch(level[0], runs, trans_loc, em, init_loc, lcol, lrow, rank)
        return loglik[0], posterior, counts

    return jax.shard_map(
        local_run,
        mesh=mesh,
        in_specs=(P(None, AXIS), P(AXIS, None), P(AXIS), P("seqs", None), P("seqs")),
        out_specs=(P("seqs"), P("seqs", AXIS), P(("seqs", AXIS), None)),
        check_vma=False,
    )
```

```python
import functools
import math

import jax
import jax.numpy as jnp
from jax import lax
from jax.experimental import pallas as pl
from jax.experimental.pallas import tpu as pltpu
from jax.sharding import PartitionSpec as P

AXIS = "states"
LANES = 128
BOTH = (0, 1)
F32 = jnp.float32
BF16 = jnp.bfloat16


def _dot(a, b, over_a=1, over_b=0):
    dims = (((over_a,), (over_b,)), ((), ()))
    return lax.dot_general(a, b, dims, preferred_element_type=F32)


def _start(copies):
    for cp in copies:
        cp.start()


def _wait(copies):
    for cp in copies:
        cp.wait()


def _loop(n, body):
    def step(i, carry):
        body(i)
        return carry

    lax.fori_loop(0, n, step, 0)


def _recursion(caps, a_hbm, em_hbm, pi_ref, lcol_ref, lrow_ref, al_hbm, w_hbm, post_hbm, ll_ref, turned_hbm,
               bank, al, work, emv, rcs, sbuf, csend, cbuf, strips, ost, dbuf, trans, fin,
               bank_sem, em_sem, al_recv, own_send, part_send, on_send, c_send, c_recv, save_sem, post_sem,
               strip_sem, d_send, d_recv, s_send, t_recv, f_recv, t_free, f_free, d_free):
    nd = cbuf.shape[0]
    nx = nd // 2
    step_count, seqs, bs = em_hbm.shape
    hb = bs // 2
    firsts = [sum(caps[:t]) for t in range(step_count)]
    slab = min(512, hb)
    tiles = bs // LANES
    kept = max(caps[1:])
    sent = pl.ds(0, kept)
    final = step_count - 1
    g = lax.axis_index(AXIS)
    x, c = g // 2, g % 2

    def dev(dx, flip):
        return ((x + dx) % nx) * 2 + (c + flip) % 2

    partner, right, left = dev(0, 1), dev(1, 0), dev(nx - 1, 0)

    def remote(src, dst, send, recv, to):
        return pltpu.make_async_remote_copy(
            src_ref=src, dst_ref=dst, send_sem=send, recv_sem=recv,
            device_id={AXIS: to}, device_id_type=pl.DeviceIdType.MESH)

    def pick(t, fn, lo, hi):
        if hi - lo == 1:
            fn(lo)
        else:
            mid = (lo + hi) // 2
            lax.cond(t < mid, lambda: pick(t, fn, lo, mid), lambda: pick(t, fn, mid, hi))

    def for_each(t, fn):
        pick(t, lambda tt: fn(tt, caps[tt - 1]), 1, step_count)

    def for_caps(t, fn, first=1):
        if len(set(caps)) == 1:
            fn(caps[0])
        else:
            pick(t, lambda tt: fn(caps[tt - 1]), first, step_count)

    acc, cur = work.at[pl.ds(0, 2)], work.at[pl.ds(4, 2)]

    def tile_row(group, i):
        if group == 0:
            src, half = dev(0, i // 2), i % 2
        elif group == 1:
            src, half = dev(nx - 1, i % 2), i // 2
        elif group == 2:
            src, half = dev(1, i % 2), 1 - i // 2
        else:
            src, half = dev(2, i // 2), i % 2
        return src * bs + half * hb

    def load(slot, row, src):
        pltpu.make_async_copy(src.at[pl.ds(pl.multiple_of(row, hb), hb)], bank.at[slot], bank_sem.at[slot]).start()

    def load_tile(slot, group, i):
        load(slot, tile_row(group, i), a_hbm)

    def load_turned(slot, number):
        load(slot, number * hb, turned_hbm)

    def in_bank(slot):
        pltpu.make_async_copy(a_hbm.at[pl.ds(0, hb)], bank.at[slot], bank_sem.at[slot]).wait()

    depth = strips.shape[0]
    bunch = min(2, depth)

    def strip_copy(number, unit, k):
        rows = pl.ds(pl.multiple_of(number * hb + (unit % (tiles // 2)) * LANES, LANES), LANES)
        cols = pl.ds(pl.multiple_of((unit // (tiles // 2)) * hb, hb), hb)
        return pltpu.make_async_copy(strips.at[k], turned_hbm.at[rows, cols], strip_sem.at[k])

    def turn(slot, number, first):
        def body(i):
            units = [bunch * i + e for e in range(bunch)]

            @pl.when(jnp.logical_not(first) | (bunch * i >= depth))
            def _():
                for u in units:
                    strip_copy(0, 0, u % depth).wait()

            for u in units:
                strips[u % depth] = jnp.transpose(bank[slot, :, pl.ds(pl.multiple_of(u * LANES, LANES), LANES)])
            for u in units:
                strip_copy(number, u, u % depth).start()

        _loop(tiles // bunch, body)

    own_each, other_each = -(-7 // final), -(-5 // (final - 1))

    def turn_own(t):
        each = own_each

        def body(e):
            n = t * each + e
            far = n // 4
            pl.when(far == 0)(lambda: in_bank(8 + n))
            pl.when(n < 7)(lambda: turn(8 + n - far * 7, n + far * 9, n == 0))

        _loop(each, body)
        _loop(4, lambda i: pl.when((t > 0) & ((i < t * each) | (i >= t * each + each)))(lambda: in_bank(8 + i)))

    def turn_others(t):
        each = other_each

        def body(e):
            n = (t - 1) * each + e
            right = (e + LANES - each) // LANES
            slot = (1 - right) * n + right * (8 + e - each)
            number = (1 - right) * (4 + n + 4 * (n // 4)) + right * slot
            pl.when((right == 1) & (t == 1))(lambda: in_bank(slot))
            pl.when(((right == 1) & (t == 1)) | ((right == 0) & (n < 5)))(lambda: turn(slot, number, False))

        pl.when(t < final)(lambda: _loop(each + 2, body))

    def em_copy(t):
        return pltpu.make_async_copy(em_hbm.at[t], emv.at[t % 2], em_sem.at[t % 2])

    _loop(2, lambda t: em_copy(t).start())
    _loop(4, lambda i: load_tile(8 + i, 0, i))
    _loop(4, lambda i: load_tile(i, 1, i))

    barrier = pltpu.get_barrier_semaphore()
    for k in range(1, nd):
        pl.semaphore_signal(barrier, inc=1, device_id={AXIS: (g + k) % nd}, device_id_type=pl.DeviceIdType.MESH)
    pl.semaphore_wait(barrier, nd - 1)

    tall = 16

    def rows_of(i):
        return pl.ds(pl.multiple_of(i * tall, tall), tall)

    def eight(i):
        return pl.ds(pl.multiple_of(i * 8, 8), 8)

    def lane(k):
        return pl.ds(k * LANES, LANES)

    def inner(k):
        return (k * LANES) // hb, pl.ds((k * LANES) % hb, LANES)

    def weigh(t):
        def body(i):
            r = rows_of(i)
            total = jnp.zeros((tall, LANES), F32)
            for k in range(tiles):
                e = emv[t % 2, r, lane(k)].astype(F32)
                h, col = inner(k)
                mass = acc[h, r, col] * e
                acc[h, r, col] = mass
                total = total + mass
            sbuf[r, :] = total

        _loop(seqs // tall, body)

    def normalise(t):
        row = jnp.sum(jnp.transpose(sbuf[...]), axis=0, keepdims=True)
        wide = jnp.broadcast_to(row, csend.shape)
        csend[...] = wide
        cbuf[g] = wide
        peers = [dev(dx, flip) for dx in (2, 1, nx - 1, 0) for flip in BOTH][: nd - 2] + [partner]
        copies = [remote(csend, cbuf.at[g], c_send.at[k], c_recv.at[g], to) for k, to in enumerate(peers)]
        _start(copies)

        with jax.named_scope("ft"):
            @pl.when(t < final)
            def _():
                turn_own(t)

        with jax.named_scope("fx"):
            for k, frm in enumerate(peers):
                remote(csend, cbuf.at[frm], c_send.at[k], c_recv.at[frm], frm).wait_recv()
        norm = cbuf[0, 0:1, :]
        for d in range(1, nd):
            norm = norm + cbuf[d, 0:1, :]
        rcs[t] = 1.0 / jnp.transpose(jnp.broadcast_to(norm, (LANES, LANES)))
        ll_ref[...] = ll_ref[...] + jnp.where(t < lrow_ref[...], jnp.log(jnp.broadcast_to(norm, ll_ref.shape)), 0.0)

        def body(i):
            r = rows_of(i)
            rc = rcs[t, r, :]
            live = t < lcol_ref[r, :]
            for k in range(tiles):
                h, col = inner(k)
                val = jnp.where(live, acc[h, r, col] * rc, cur[h, r, col])
                cur[h, r, col] = val
                al[0, h, r, col] = val.astype(BF16)

        _loop(seqs // tall, body)
        for cp in copies:
            cp.wait_send()

    ll_ref[...] = jnp.zeros_like(ll_ref)
    for h in BOTH:
        acc[h] = jnp.broadcast_to(pi_ref[:, h * hb : (h + 1) * hb], (seqs, hb))

    def own_copies(rows):
        m = pl.ds(0, rows)
        out = [remote(al.at[0, h, m], al.at[1, h, m], own_send.at[0, h], al_recv.at[1, h], partner) for h in BOTH]
        for h in BOTH:
            out.append(remote(al.at[0, h, m], al.at[2, h, m], own_send.at[1, h], al_recv.at[2, h], right))
            out.append(remote(al.at[0, 1 - h, m], al.at[3, 1 - h, m], own_send.at[2, 1 - h], al_recv.at[3, 1 - h], left))
        return out

    def to_partner(slot, to_slot, half, rows):
        m = pl.ds(0, rows)
        return remote(al.at[slot, half, m], al.at[to_slot, half, m], part_send.at[slot, half], al_recv.at[to_slot, half], partner)

    def onward(s, rows):
        m = pl.ds(0, rows)
        return remote(al.at[2 + s, s, m], al.at[6, s, m], on_send.at[s], al_recv.at[6, s], dev(1 + (nx - 2) * s, 0))

    def arrived(slot, half, rows):
        m = pl.ds(0, rows)
        remote(al.at[slot, half, m], al.at[slot, half, m], part_send.at[slot, half], al_recv.at[slot, half], partner).wait_recv()

    def save_copies(t, rows):
        to = pl.ds(firsts[t - 1], rows)
        return [pltpu.make_async_copy(al.at[0, h, pl.ds(0, rows)], al_hbm.at[to, pl.ds(h * hb, hb)], save_sem.at[h])
                for h in BOTH]

    def multiply(one, two):
        (slot1, half1, tile1), (slot2, half2, tile2) = one, two
        lhs1, lhs2 = al[slot1, half1], al[slot2, half2]
        for h in BOTH:
            for n in range(hb // slab):
                cols, at = pl.ds(h * hb + n * slab, slab), pl.ds(n * slab, slab)
                acc[h, :, at] = acc[h, :, at] + (
                    _dot(lhs1, tile1[:, cols]) + _dot(lhs2, tile2[:, cols]))

    def forward(t):
        pl.when(t > 0)(lambda: predict(t))
        em_copy(t).wait()
        with jax.named_scope("fw"):
            weigh(t)
        normalise(t)

    def predict(t):
        for_caps(t, lambda rows: _start(own_copies(rows)))
        for_each(t, lambda tt, rows: _start(save_copies(tt, rows)))

        @pl.when(t + 1 < step_count)
        def _():
            em_copy(t + 1).start()

        acc[...] = jnp.zeros(acc.shape, F32)

        def group0(j):
            def ready(rows):
                for half in BOTH:
                    arrived(1, half, rows)

            pl.when(j > 0)(lambda: for_caps(t, ready))
            _loop(2, lambda e: pl.when((t == 1) & (2 * j + e >= own_each))(lambda: in_bank(8 + 2 * j + e)))
            multiply(*((j, e, bank.at[8 + 2 * j + e]) for e in BOTH))
            for e in BOTH:
                load_tile(8 + 2 * j + e, 2, 2 * j + e)

        def group12(k, j):
            def ready(rows):
                arrived(2 + 2 * j, k, rows)
                arrived(3 + 2 * j, 1 - k, rows)

                @pl.when(j == 0)
                def _():
                    to_partner(2, 4, k, rows).start()
                    to_partner(3, 5, 1 - k, rows).start()

                pl.when(k + j == 0)(lambda: _start([onward(0, rows), onward(1, rows)]))

            for_caps(t, ready)
            at = 2 * k + j
            pl.when((t > 1) | (at > 1))(lambda: in_bank(8 + at))
            pl.when((t == 1) & (at >= other_each))(lambda: in_bank(at))
            multiply((2 + 2 * j, k, bank.at[at]), (3 + 2 * j, 1 - k, bank.at[8 + at]))

        def next_tiles(k):
            def body(e):
                i = 2 * k + e
                pl.when(t < final)(lambda: load_tile(8 + i, 0, i))

                @pl.when(t == final)
                def _():
                    load_turned(8 + i, 12 + i)
                    load_turned(i, 4 + i)

            _loop(2, body)

        def group3(j):
            def ready(rows):
                for half in BOTH:
                    arrived(6 + j, half, rows)

                @pl.when(j == 0)
                def _():
                    for half in BOTH:
                        to_partner(6, 7, half, rows).start()

            for_caps(t, ready)
            multiply(*((6 + j, e, bank.at[4 + 2 * j + e]) for e in BOTH))

        with jax.named_scope("f0"):
            _loop(2, group0)

        @pl.when(t == 1)
        def _():
            _loop(4, lambda i: load_tile(4 + i, 3, i))
            _loop(other_each, in_bank)

        with jax.named_scope("ft"):
            turn_others(t)
        pl.when(t == final)(lambda: _loop(depth, lambda k: strip_copy(0, 0, k).wait()))

        def groups12(k):
            with jax.named_scope("f1"):
                _loop(2, functools.partial(group12, k))
            pl.when((k == 1) & (t > 1) & (t < 4))(lambda: turn(8 + t, 8 + t, False))
            next_tiles(k)

        _loop(2, groups12)
        pl.when(t == 1)(lambda: _loop(4, lambda i: in_bank(4 + i)))
        with jax.named_scope("f3"):
            _loop(2, group3)
        pl.when(t == final)(lambda: _loop(4, lambda i: load_turned(4 + i, 8 + i)))

        def drained(rows):
            for cp in own_copies(rows):
                cp.wait_send()
            for half in BOTH:
                to_partner(2, 4, half, rows).wait_send()
                to_partner(3, 5, half, rows).wait_send()
                to_partner(6, 7, half, rows).wait_send()
                onward(half, rows).wait_send()

        for_caps(t, drained)
        for_each(t, lambda tt, rows: _wait(save_copies(tt, rows)))

    _loop(step_count, forward)

    def post_copy(h):
        return pltpu.make_async_copy(cur.at[h], post_hbm.at[:, pl.ds(pl.multiple_of(h * hb, hb), hb)], post_sem.at[h])

    _loop(2, lambda h: post_copy(h).start())

    back_caps = functools.partial(for_caps, first=2)

    def weights(t):
        def body(i):
            r = eight(i)
            rc = rcs[t, r, :]
            live, later = t < lcol_ref[r, :], t + 1 < lcol_ref[r, :]
            for k in range(tiles):
                h, col = inner(k)
                beta = jnp.where(later, acc[h, r, col] + fin[0, h, r, col] + fin[1, h, r, col], 1.0)
                val = emv[t % 2, r, lane(k)].astype(F32) * beta * rc
                strips[h, r, col] = jnp.where(live, val, 0.0).astype(BF16)

        _loop(kept // 8, body)

    def w_copies(t, rows):
        to = pl.ds(firsts[t - 1], rows)
        return [pltpu.make_async_copy(strips.at[h, pl.ds(0, rows)], w_hbm.at[to, pl.ds(h * hb, hb)], save_sem.at[h])
                for h in BOTH]

    def partial_sums(out, tile):
        for n in range(hb // slab):
            cols = pl.ds(n * slab, slab)
            more = pl.ds(hb + n * slab, slab)
            out[sent, cols] = _dot(strips[0, sent, :], tile[:, cols]) + _dot(strips[1, sent, :], tile[:, more])

    def add_into(out, *terms):
        def body(i):
            r = eight(i)
            val = out[r, :]
            for term in terms:
                val = val + term[r, :]
            out[r, :] = val

        _loop(kept // 8, body)

    def to_core(q, rows):
        m = pl.ds(0, rows)
        return remote(ost.at[q, m], dbuf.at[q, m], d_send.at[q], d_recv.at[q], partner)

    def staged(p):
        n, q = p // 2, p % 2
        return (1 - n % 2) * (2 + n) + q

    def ring_copy(far, p, rows):
        m, q = pl.ds(0, rows), p % 2
        to = dev(1 + (nx - 2) * q, 0)
        src, send = work.at[staged(p), m], s_send.at[p]
        if far:
            return remote(src, trans.at[q, m], send, t_recv.at[q], to)
        half = (p // 2 + q) % 2
        return remote(src, fin.at[q, half, m], send, f_recv.at[q, half], to)

    def freed(sem, q):
        pl.semaphore_signal(sem.at[q], inc=1, device_id={AXIS: dev(nx - 1 - (nx - 2) * q, 0)},
                            device_id_type=pl.DeviceIdType.MESH)

    def backward(idx):
        t = step_count - 1 - idx
        with jax.named_scope("bw"):
            weights(t)
        _loop(2, functools.partial(freed, f_free))
        for_each(t, lambda tt, rows: _start(w_copies(tt, rows)))

        @pl.when(t > 2)
        def _():
            em_copy(t - 2).start()

        def slot_of(p, flip):
            n, q = p // 2, p % 2
            inner = ((n + 1) % 4) // 2
            return inner == 0, (1 - inner) * (8 + 2 * flip + q) + inner * (4 * (1 - q) + 2 * (n - 1) + flip)

        def products(n, flip, outs):
            outer, _ = slot_of(2 * n, flip)
            slots = [slot_of(2 * n + q, flip)[1] for q in BOTH]

            @pl.when(outer | (idx == 0))
            def _():
                for slot in slots:
                    in_bank(slot)

            for slot, out in zip(slots, outs):
                partial_sums(out, bank.at[slot])

            @pl.when(n == 0)
            def _():
                for slot in slots:
                    load_turned(slot, slot - 8)

            @pl.when((n == 3) & (t > 2))
            def _():
                for slot in slots:
                    load_turned(slot, slot + 4)

        def for_other(n):
            def drain(rows):
                for q in BOTH:
                    to_core(q, rows).wait_send()

            pl.when(n > 0)(lambda: back_caps(t, drain))
            products(n, 1, [ost.at[q] for q in BOTH])

            @pl.when((n > 0) | (idx > 0))
            def _():
                for q in BOTH:
                    pl.semaphore_wait(d_free.at[q], 1)

            back_caps(t, lambda rows: _start([to_core(q, rows) for q in BOTH]))

        def for_this(n):
            outs = [work.at[staged(2 * n + q)] for q in BOTH]
            pl.when((n == 2) & (idx == 0))(lambda: _wait([post_copy(q) for q in BOTH]))

            def drain(rows):
                for q in BOTH:
                    ring_copy(False, 2 + q, rows).wait_send()

            pl.when(n == 3)(lambda: back_caps(t, drain))
            products(n, 0, outs)
            for q, out in enumerate(outs):
                p = 2 * n + q
                back_caps(t, lambda rows: to_core(q, rows).wait_recv())

                @pl.when(n == 2)
                def _():
                    back_caps(t, lambda rows: ring_copy(True, q, rows).wait_recv())
                    add_into(out, dbuf.at[q], trans.at[q])
                    pl.when(t > 2)(lambda: freed(t_free, q))

                pl.when(n != 2)(lambda: add_into(out, dbuf.at[q]))

                @pl.when((n < 3) | (t > 2))
                def _():
                    pl.semaphore_signal(d_free.at[q], inc=1, device_id={AXIS: partner}, device_id_type=pl.DeviceIdType.MESH)

                @pl.when(n == 0)
                def _():
                    pl.when(idx > 0)(lambda: pl.semaphore_wait(t_free.at[q], 1))
                    back_caps(t, lambda rows: ring_copy(True, q, rows).start())

                @pl.when((n == 1) | (n == 2))
                def _():
                    pl.when(n == 1)(lambda: pl.semaphore_wait(f_free.at[q], 1))
                    back_caps(t, lambda rows: ring_copy(False, p, rows).start())

        def stage(n):
            with jax.named_scope("bo"):
                for_other(n)
            with jax.named_scope("bt"):
                for_this(n)

        _loop(4, stage)

        def landed(rows):
            for p in range(2, 6):
                ring_copy(False, p, rows).wait_recv()

        with jax.named_scope("bl"):
            back_caps(t, landed)

        def drained(rows):
            for q in BOTH:
                for cp in (to_core(q, rows), ring_copy(True, q, rows), ring_copy(False, 4 + q, rows)):
                    cp.wait_send()

        with jax.named_scope("bd"):
            back_caps(t, drained)
        for_each(t, lambda tt, rows: _wait(w_copies(tt, rows)))

        @pl.when(t > 2)
        def _():
            em_copy(t - 2).wait()

    _loop(step_count - 2, backward)
    weights(1)

    def rest(i):
        r = eight(kept // 8 + i)
        rc = rcs[1, r, :]
        live = lcol_ref[r, :] > 1
        for k in range(tiles):
            h, col = inner(k)
            val = emv[1, r, lane(k)].astype(F32) * rc
            strips[h, r, col] = jnp.where(live, val, 0.0).astype(BF16)

    _loop((seqs - kept) // 8, rest)
    _start(w_copies(1, caps[0]))
    _wait(w_copies(1, caps[0]))


def _run_recursion(nd, caps, ident, trans_loc, em, init_loc, lcol, lrow):
    step_count, seqs, bs = em.shape
    hb = bs // 2
    kept = max(caps[1:])
    depth = min(8 if kept < seqs else 4, bs // LANES)
    dma = pltpu.SemaphoreType.DMA
    two, credit = dma((2,)), pltpu.SemaphoreType.REGULAR((2,))
    vm, hbm = pl.BlockSpec(memory_space=pltpu.VMEM), pl.BlockSpec(memory_space=pl.ANY)
    scratch = [
        pltpu.VMEM((12, hb, bs), BF16),
        pltpu.VMEM((8, 2, seqs, hb), BF16),
        pltpu.VMEM((6, seqs, hb), F32),
        pltpu.VMEM((2, seqs, bs), BF16),
        pltpu.VMEM((step_count, seqs, LANES), F32),
        pltpu.VMEM((seqs, LANES), F32),
        pltpu.VMEM((8, seqs), F32),
        pltpu.VMEM((nd, 8, seqs), F32),
        pltpu.VMEM((depth, LANES, hb), BF16),
        pltpu.VMEM((2, kept, hb), F32),
        pltpu.VMEM((2, kept, hb), F32),
        pltpu.VMEM((2, kept, hb), F32),
        pltpu.VMEM((2, 2, kept, hb), F32),
        dma((12,)), two, dma((nd, 2)), dma((3, 2)), dma((nd, 2)), two, dma((nd,)), dma((nd,)), two,
        two, dma((depth,)), two, two, dma((6,)), two, dma((2, 2)), credit, credit, credit,
    ]
    return pl.pallas_call(
        functools.partial(_recursion, caps),
        name=f"recursion{ident}",
        out_shape=[
            jax.ShapeDtypeStruct((sum(caps), bs), BF16),
            jax.ShapeDtypeStruct((sum(caps), bs), BF16),
            jax.ShapeDtypeStruct((seqs, bs), F32),
            jax.ShapeDtypeStruct((8, seqs), F32),
            jax.ShapeDtypeStruct(trans_loc.shape, BF16),
        ],
        in_specs=[hbm, hbm, vm, vm, vm],
        out_specs=[hbm, hbm, hbm, vm, hbm],
        scratch_shapes=scratch,
        compiler_params=pltpu.CompilerParams(collective_id=ident, has_side_effects=True, vmem_limit_bytes=67_043_328),
    )(trans_loc, em, init_loc[None, :], lcol, lrow)


def _prepare(choices, tok_ref, len_ref, emt_hbm, em_hbm, lcol_ref, lrow_ref, rank_ref, level_ref,
             table, stable, picked, blocks, stage, table_sem, block_sem, stage_sem):
    step_count, seqs, bs = em_hbm.shape
    deep = blocks.shape[0]
    part = 32
    slab = min(512, bs)
    sub = lax.broadcasted_iota(jnp.int32, (seqs, LANES), 0)
    lan = lax.broadcasted_iota(jnp.int32, (seqs, LANES), 1)
    across = jnp.broadcast_to(len_ref[...].astype(F32), (seqs, seqs))
    down = jnp.transpose(across)
    ahead = (down > across) | ((down == across) & (sub < lan))
    rank = jnp.sum(jnp.where(ahead, 1.0, 0.0), axis=0, keepdims=True)
    rank_ref[...] = jnp.broadcast_to(rank, rank_ref.shape)
    pick = rank == sub.astype(F32)
    lcol = jnp.broadcast_to(jnp.sum(jnp.where(pick, across, 0.0), axis=1, keepdims=True), (seqs, LANES))
    lcol_ref[...] = lcol.astype(jnp.int32)
    lrow_ref[...] = jnp.transpose(lcol)[0:8].astype(jnp.int32)
    mat = jnp.zeros((seqs, LANES), F32)
    for t in range(step_count):
        tok = jnp.sum(jnp.where(pick, tok_ref[t : t + 1, :].astype(F32), 0.0), axis=1, keepdims=True)
        tok = jnp.broadcast_to(tok, (seqs, LANES))
        mat = jnp.where(lan == t, tok, mat)
        picked[t] = tok.astype(jnp.int32) & 7
    table[0:8] = jnp.transpose(mat)[0:8].astype(jnp.int32)
    alive = jnp.sum(jnp.where(across[0:8] > sub[0:8].astype(F32), 1.0, 0.0), axis=1, keepdims=True)
    table[8:16] = jnp.broadcast_to(alive, (8, LANES)).astype(jnp.int32)
    copy = pltpu.make_async_copy(table, stable, table_sem)
    copy.start()
    copy.wait()
    level = jnp.int32(0)
    for k, caps in enumerate(choices):
        for t in range(1, step_count):
            level = jnp.where(stable[8 + t, 0] > caps[t - 1], k + 1, level)
    level_ref[0] = level

    def parts(t):
        return (stable[8 + t, 0] + (part - 1)) // part

    def fetch(t):
        def body(p, carry):
            for k in range(part):
                s = p * part + k
                pltpu.make_async_copy(emt_hbm.at[stable[t, s] >> 3], blocks.at[t % deep, s], block_sem.at[t % deep]).start()
            return carry

        lax.fori_loop(0, parts(t), body, 0)

    def landed(t):
        def body(p, carry):
            pltpu.make_async_copy(emt_hbm.at[pl.ds(0, part)], blocks.at[t % deep, pl.ds(0, part)], block_sem.at[t % deep]).wait()
            return carry

        lax.fori_loop(0, parts(t), body, 0)

    def select(t):
        def body(p, carry):
            r = pl.ds(pl.multiple_of(p * part, part), part)
            at = picked[t, r, :] + 8 * sub[0:part]
            one = jnp.concatenate([jnp.where(lan[0:part] + off == at, 1.0, 0.0) for off in (0, LANES)], axis=1).astype(BF16)
            for n in range(bs // slab):
                cols = pl.ds(n * slab, slab)
                rows = blocks[t % deep, r, :, cols].reshape(part * 8, slab)
                stage[t % 2, r, cols] = _dot(one, rows).astype(BF16)
            return carry

        lax.fori_loop(0, parts(t), body, 0)

    def out_copy(t):
        return pltpu.make_async_copy(stage.at[t % 2], em_hbm.at[t], stage_sem.at[t % 2])

    def position(t):
        pl.when(t >= 2)(lambda: out_copy(t - 2).wait())
        landed(t)
        select(t)
        out_copy(t).start()
        pl.when(t + deep < step_count)(lambda: fetch(t + deep))

    _loop(deep, fetch)
    _loop(step_count, position)
    _loop(2, lambda e: out_copy(step_count - 1 - e).wait())


def _run_prepare(choices, tokens, lengths, emit_loc):
    bs, symbols = emit_loc.shape
    seqs, step_count = tokens.shape
    dma = pltpu.SemaphoreType.DMA
    vm, hbm = pl.BlockSpec(memory_space=pltpu.VMEM), pl.BlockSpec(memory_space=pl.ANY)
    return pl.pallas_call(
        functools.partial(_prepare, choices),
        name="prepare",
        out_shape=[
            jax.ShapeDtypeStruct((step_count, seqs, bs), BF16),
            jax.ShapeDtypeStruct((seqs, LANES), jnp.int32),
            jax.ShapeDtypeStruct((8, seqs), jnp.int32),
            jax.ShapeDtypeStruct((8, seqs), F32),
            jax.ShapeDtypeStruct((1,), jnp.int32),
        ],
        in_specs=[vm, vm, hbm],
        out_specs=[hbm, vm, vm, vm, pl.BlockSpec(memory_space=pltpu.SMEM)],
        scratch_shapes=[
            pltpu.VMEM((16, LANES), jnp.int32),
            pltpu.SMEM((16, LANES), jnp.int32),
            pltpu.VMEM((step_count, seqs, LANES), jnp.int32),
            pltpu.VMEM((4, seqs, 8, bs), BF16),
            pltpu.VMEM((2, seqs, bs), BF16),
            dma, dma((4,)), dma((2,)),
        ],
        compiler_params=pltpu.CompilerParams(vmem_limit_bytes=60_000_000),
    )(tokens.T, lengths[None, :], emit_loc.T.reshape(symbols // 8, 8, bs))


def _counts(trans_hbm, alpha_hbm, w_hbm, post_hbm, ll_ref, rank_ref, counts_hbm, posterior_hbm, loglik_ref,
            alpha, w, diag, out, post, back, in_sem, alpha_sem, diag_sem, out_sem, back_sem):
    rows, bs = w.shape
    seqs = post.shape[0]
    steps, tile, _ = diag.shape
    slab = min(512, bs)
    first = lax.axis_index(AXIS) * bs
    loads = [pltpu.make_async_copy(post_hbm, post, in_sem.at[0]), pltpu.make_async_copy(w_hbm, w, in_sem.at[1])]
    _start(loads)

    def alpha_copy(i):
        at = pl.multiple_of(i * tile, tile)
        return pltpu.make_async_copy(alpha_hbm.at[:, pl.ds(at, tile)], alpha.at[i], alpha_sem.at[i])

    def diag_copy(i):
        at = pl.multiple_of(first + i * tile, tile)
        return pltpu.make_async_copy(trans_hbm.at[pl.ds(at, tile)], diag.at[i], diag_sem.at[i])

    def out_copy(i):
        at = pl.multiple_of(i * tile, tile)
        return pltpu.make_async_copy(out.at[i], counts_hbm.at[pl.ds(at, tile)], out_sem.at[i])

    def bring(i):
        alpha_copy(i).start()
        diag_copy(i).start()

    _loop(steps, bring)

    rank = jnp.broadcast_to(rank_ref[0:1, :], (seqs, seqs))
    sub = lax.broadcasted_iota(jnp.int32, (seqs, seqs), 0).astype(F32)
    lan = lax.broadcasted_iota(jnp.int32, (seqs, seqs), 1).astype(F32)
    lls = jnp.transpose(jnp.broadcast_to(ll_ref[0:1, :], (seqs, seqs)))
    loglik_ref[...] = jnp.sum(jnp.where(rank == sub, lls, 0.0), axis=0, keepdims=True)
    order = jnp.where(jnp.transpose(rank) == lan, 1.0, 0.0).astype(BF16)
    loads[0].wait()
    for n in range(bs // slab):
        cols = pl.ds(n * slab, slab)
        rest = post[:, cols]
        total = jnp.zeros(rest.shape, F32)
        for _ in range(3):
            head = rest.astype(BF16)
            rest = rest - head.astype(F32)
            total = total + _dot(order, head)
        back[:, cols] = total
    back_copy = pltpu.make_async_copy(back, posterior_hbm, back_sem)
    back_copy.start()
    loads[1].wait()

    def step(i):
        alpha_copy(i).wait()
        lhs = alpha[i]
        diag_copy(i).wait()
        for n in range(bs // slab):
            cols = pl.ds(n * slab, slab)
            out[i, :, cols] = diag[i, :, cols].astype(F32) * _dot(lhs, w[:, cols], 0)
        out_copy(i).start()

    _loop(steps, step)
    _loop(steps, lambda i: out_copy(i).wait())
    back_copy.wait()


def _run_counts(alphas, ws, trans_loc, post, ll, rank):
    rows, bs = alphas.shape
    seqs = post.shape[0]
    tile = min(256, bs)
    steps = bs // tile
    dma = pltpu.SemaphoreType.DMA
    vm, hbm = pl.BlockSpec(memory_space=pltpu.VMEM), pl.BlockSpec(memory_space=pl.ANY)
    return pl.pallas_call(
        _counts,
        name="counts",
        out_shape=[
            jax.ShapeDtypeStruct((bs, bs), F32),
            jax.ShapeDtypeStruct((seqs, bs), F32),
            jax.ShapeDtypeStruct((1, seqs), F32),
        ],
        in_specs=[hbm, hbm, hbm, hbm, vm, vm],
        out_specs=[hbm, hbm, vm],
        scratch_shapes=[
            pltpu.VMEM((steps, rows, tile), BF16),
            pltpu.VMEM((rows, bs), BF16),
            pltpu.VMEM((steps, tile, bs), BF16),
            pltpu.VMEM((steps, tile, bs), F32),
            pltpu.VMEM((seqs, bs), F32),
            pltpu.VMEM((seqs, bs), F32),
            dma((2,)), dma((steps,)), dma((steps,)), dma((steps,)), dma,
        ],
        compiler_params=pltpu.CompilerParams(vmem_limit_bytes=60_000_000),
    )(trans_loc, alphas, ws, post, ll, rank)


def _capacities(seqs, step_count, spread):
    caps = []
    for t in range(1, step_count):
        live = (step_count - t) / step_count
        room = spread * math.sqrt((seqs - 1) * live * (1 - live))
        caps.append(min(seqs, 8 * math.ceil(((seqs - 1) * live + 1 + room) / 8)))
    return tuple(caps)


def solution(mesh):
    nd = mesh.shape[AXIS]

    def local_run(trans_loc, emit_loc, init_loc, tokens_loc, lengths_loc):
        seqs, step_count = tokens_loc.shape
        choices = [_capacities(seqs, step_count, spread) for spread in (2.7, 4.1)]
        em, lcol, lrow, rank, level = _run_prepare(choices, tokens_loc, lengths_loc, emit_loc)

        def run(ident, caps, trans, em, init, lcol, lrow, rank):
            alphas, ws, post, ll, _ = _run_recursion(nd, caps, ident, trans, em, init, lcol, lrow)
            return _run_counts(alphas, ws, trans, post, ll, rank)

        choices.append((seqs,) * (step_count - 1))
        runs = [functools.partial(run, k, caps) for k, caps in enumerate(choices)]
        counts, posterior, loglik = lax.switch(level[0], runs, trans_loc, em, init_loc, lcol, lrow, rank)
        return loglik[0], posterior, counts

    return jax.shard_map(
        local_run,
        mesh=mesh,
        in_specs=(P(None, AXIS), P(AXIS, None), P(AXIS), P("seqs", None), P("seqs")),
        out_specs=(P("seqs"), P("seqs", AXIS), P(("seqs", AXIS), None)),
        check_vma=False,
    )
```

```python
import functools
import math

import jax
import jax.numpy as jnp
from jax import lax
from jax.experimental import pallas as pl
from jax.experimental.pallas import tpu as pltpu
from jax.sharding import PartitionSpec as P

AXIS = "states"
LANES = 128
BOTH = (0, 1)
F32 = jnp.float32
BF16 = jnp.bfloat16


def _dot(a, b, over_a=1, over_b=0):
    dims = (((over_a,), (over_b,)), ((), ()))
    return lax.dot_general(a, b, dims, preferred_element_type=F32)


def _start(copies):
    for cp in copies:
        cp.start()


def _wait(copies):
    for cp in copies:
        cp.wait()


def _loop(n, body):
    def step(i, carry):
        body(i)
        return carry

    lax.fori_loop(0, n, step, 0)


def _recursion(caps, a_hbm, em_hbm, pi_ref, lcol_ref, lrow_ref, al_hbm, w_hbm, post_hbm, ll_ref, turned_hbm,
               bank, al, work, emv, rcs, sbuf, csend, cbuf, strips, ost, dbuf, trans, fin,
               bank_sem, em_sem, al_recv, own_send, part_send, on_send, c_send, c_recv, save_sem, post_sem,
               strip_sem, d_send, d_recv, s_send, t_recv, f_recv, t_free, f_free, d_free):
    nd = cbuf.shape[0]
    nx = nd // 2
    step_count, seqs, bs = em_hbm.shape
    hb = bs // 2
    firsts = [sum(caps[:t]) for t in range(step_count)]
    slab = min(512, hb)
    tiles = bs // LANES
    kept = max(caps[1:])
    sent = pl.ds(0, kept)
    final = step_count - 1
    g = lax.axis_index(AXIS)
    x, c = g // 2, g % 2

    def dev(dx, flip):
        return ((x + dx) % nx) * 2 + (c + flip) % 2

    partner, right, left = dev(0, 1), dev(1, 0), dev(nx - 1, 0)

    def remote(src, dst, send, recv, to):
        return pltpu.make_async_remote_copy(
            src_ref=src, dst_ref=dst, send_sem=send, recv_sem=recv,
            device_id={AXIS: to}, device_id_type=pl.DeviceIdType.MESH)

    def pick(t, fn, lo, hi):
        if hi - lo == 1:
            fn(lo)
        else:
            mid = (lo + hi) // 2
            lax.cond(t < mid, lambda: pick(t, fn, lo, mid), lambda: pick(t, fn, mid, hi))

    def for_each(t, fn):
        pick(t, lambda tt: fn(tt, caps[tt - 1]), 1, step_count)

    def for_caps(t, fn, first=1):
        if len(set(caps)) == 1:
            fn(caps[0])
        else:
            pick(t, lambda tt: fn(caps[tt - 1]), first, step_count)

    acc, cur = work.at[pl.ds(0, 2)], work.at[pl.ds(4, 2)]

    def tile_row(group, i):
        if group == 0:
            src, half = dev(0, i // 2), i % 2
        elif group == 1:
            src, half = dev(nx - 1, i % 2), i // 2
        elif group == 2:
            src, half = dev(1, i % 2), 1 - i // 2
        else:
            src, half = dev(2, i // 2), i % 2
        return src * bs + half * hb

    def load(slot, row, src):
        pltpu.make_async_copy(src.at[pl.ds(pl.multiple_of(row, hb), hb)], bank.at[slot], bank_sem.at[slot]).start()

    def load_tile(slot, group, i):
        load(slot, tile_row(group, i), a_hbm)

    def load_turned(slot, number):
        load(slot, number * hb, turned_hbm)

    def in_bank(slot):
        pltpu.make_async_copy(a_hbm.at[pl.ds(0, hb)], bank.at[slot], bank_sem.at[slot]).wait()

    depth = strips.shape[0]
    bunch = min(2, depth)

    def strip_copy(number, unit, k):
        rows = pl.ds(pl.multiple_of(number * hb + (unit % (tiles // 2)) * LANES, LANES), LANES)
        cols = pl.ds(pl.multiple_of((unit // (tiles // 2)) * hb, hb), hb)
        return pltpu.make_async_copy(strips.at[k], turned_hbm.at[rows, cols], strip_sem.at[k])

    def turn(slot, number, first):
        def body(i):
            units = [bunch * i + e for e in range(bunch)]

            @pl.when(jnp.logical_not(first) | (bunch * i >= depth))
            def _():
                for u in units:
                    strip_copy(0, 0, u % depth).wait()

            for u in units:
                strips[u % depth] = jnp.transpose(bank[slot, :, pl.ds(pl.multiple_of(u * LANES, LANES), LANES)])
            for u in units:
                strip_copy(number, u, u % depth).start()

        _loop(tiles // bunch, body)

    own_each, other_each = -(-7 // final), -(-5 // (final - 1))

    def turn_own(t):
        each = own_each

        def body(e):
            n = t * each + e
            far = n // 4
            pl.when(far == 0)(lambda: in_bank(8 + n))
            pl.when(n < 7)(lambda: turn(8 + n - far * 7, n + far * 9, n == 0))

        _loop(each, body)
        _loop(4, lambda i: pl.when((t > 0) & ((i < t * each) | (i >= t * each + each)))(lambda: in_bank(8 + i)))

    def turn_others(t):
        each = other_each

        def body(e):
            n = (t - 1) * each + e
            right = (e + LANES - each) // LANES
            slot = (1 - right) * n + right * (8 + e - each)
            number = (1 - right) * (4 + n + 4 * (n // 4)) + right * slot
            pl.when((right == 1) & (t == 1))(lambda: in_bank(slot))
            pl.when(((right == 1) & (t == 1)) | ((right == 0) & (n < 5)))(lambda: turn(slot, number, False))

        pl.when(t < final)(lambda: _loop(each + 2, body))

    def em_copy(t):
        return pltpu.make_async_copy(em_hbm.at[t], emv.at[t % 2], em_sem.at[t % 2])

    _loop(2, lambda t: em_copy(t).start())
    _loop(4, lambda i: load_tile(8 + i, 0, i))
    _loop(4, lambda i: load_tile(i, 1, i))

    barrier = pltpu.get_barrier_semaphore()
    for k in range(1, nd):
        pl.semaphore_signal(barrier, inc=1, device_id={AXIS: (g + k) % nd}, device_id_type=pl.DeviceIdType.MESH)
    tall = 16

    def rows_of(i):
        return pl.ds(pl.multiple_of(i * tall, tall), tall)

    def eight(i):
        return pl.ds(pl.multiple_of(i * 8, 8), 8)

    def lane(k):
        return pl.ds(k * LANES, LANES)

    def inner(k):
        return (k * LANES) // hb, pl.ds((k * LANES) % hb, LANES)

    def weigh(t):
        def body(i):
            r = rows_of(i)
            total = jnp.zeros((tall, LANES), F32)
            for k in range(tiles):
                e = emv[t % 2, r, lane(k)].astype(F32)
                h, col = inner(k)
                mass = acc[h, r, col] * e
                acc[h, r, col] = mass
                total = total + mass
            sbuf[r, :] = total

        _loop(seqs // tall, body)

    def normalise(t):
        row = jnp.sum(jnp.transpose(sbuf[...]), axis=0, keepdims=True)
        wide = jnp.broadcast_to(row, csend.shape)
        csend[...] = wide
        cbuf[g] = wide
        peers = [dev(dx, flip) for dx in (2, 1, nx - 1, 0) for flip in BOTH][: nd - 2] + [partner]
        copies = [remote(csend, cbuf.at[g], c_send.at[k], c_recv.at[g], to) for k, to in enumerate(peers)]
        _start(copies)

        with jax.named_scope("ft"):
            @pl.when(t < final)
            def _():
                turn_own(t)

        with jax.named_scope("fx"):
            for k, frm in enumerate(peers):
                remote(csend, cbuf.at[frm], c_send.at[k], c_recv.at[frm], frm).wait_recv()
        norm = cbuf[0, 0:1, :]
        for d in range(1, nd):
            norm = norm + cbuf[d, 0:1, :]
        rcs[t] = 1.0 / jnp.transpose(jnp.broadcast_to(norm, (LANES, LANES)))
        ll_ref[...] = ll_ref[...] + jnp.where(t < lrow_ref[...], jnp.log(jnp.broadcast_to(norm, ll_ref.shape)), 0.0)

        def body(i):
            r = rows_of(i)
            rc = rcs[t, r, :]
            live = t < lcol_ref[r, :]
            for k in range(tiles):
                h, col = inner(k)
                val = jnp.where(live, acc[h, r, col] * rc, cur[h, r, col])
                cur[h, r, col] = val
                al[0, h, r, col] = val.astype(BF16)

        _loop(seqs // tall, body)
        for cp in copies:
            cp.wait_send()

    ll_ref[...] = jnp.zeros_like(ll_ref)
    for h in BOTH:
        acc[h] = jnp.broadcast_to(pi_ref[:, pl.ds(h * hb, hb)], (seqs, hb))
    em_copy(0).wait()
    weigh(0)
    pl.semaphore_wait(barrier, nd - 1)

    def own_copies(rows):
        m = pl.ds(0, rows)
        out = [remote(al.at[0, h, m], al.at[1, h, m], own_send.at[0, h], al_recv.at[1, h], partner) for h in BOTH]
        for h in BOTH:
            out.append(remote(al.at[0, h, m], al.at[2, h, m], own_send.at[1, h], al_recv.at[2, h], right))
            out.append(remote(al.at[0, 1 - h, m], al.at[3, 1 - h, m], own_send.at[2, 1 - h], al_recv.at[3, 1 - h], left))
        return out

    def to_partner(slot, to_slot, half, rows):
        m = pl.ds(0, rows)
        return remote(al.at[slot, half, m], al.at[to_slot, half, m], part_send.at[slot, half], al_recv.at[to_slot, half], partner)

    def onward(s, rows):
        m = pl.ds(0, rows)
        return remote(al.at[2 + s, s, m], al.at[6, s, m], on_send.at[s], al_recv.at[6, s], dev(1 + (nx - 2) * s, 0))

    def arrived(slot, half, rows):
        m = pl.ds(0, rows)
        remote(al.at[slot, half, m], al.at[slot, half, m], part_send.at[slot, half], al_recv.at[slot, half], partner).wait_recv()

    def save_copies(t, rows):
        to = pl.ds(firsts[t - 1], rows)
        return [pltpu.make_async_copy(al.at[0, h, pl.ds(0, rows)], al_hbm.at[to, pl.ds(h * hb, hb)], save_sem.at[h])
                for h in BOTH]

    def multiply(one, two):
        (slot1, half1, tile1), (slot2, half2, tile2) = one, two
        lhs1, lhs2 = al[slot1, half1], al[slot2, half2]
        for h in BOTH:
            for n in range(hb // slab):
                cols, at = pl.ds(h * hb + n * slab, slab), pl.ds(n * slab, slab)
                acc[h, :, at] = acc[h, :, at] + (
                    _dot(lhs1, tile1[:, cols]) + _dot(lhs2, tile2[:, cols]))

    def forward(t):
        pl.when(t > 0)(lambda: predict(t))
        normalise(t)

    def predict(t):
        for_caps(t, lambda rows: _start(own_copies(rows)))
        for_each(t, lambda tt, rows: _start(save_copies(tt, rows)))

        @pl.when(t + 1 < step_count)
        def _():
            em_copy(t + 1).start()

        acc[...] = jnp.zeros(acc.shape, F32)

        def group0(j):
            def ready(rows):
                for half in BOTH:
                    arrived(1, half, rows)

            pl.when(j > 0)(lambda: for_caps(t, ready))
            _loop(2, lambda e: pl.when((t == 1) & (2 * j + e >= own_each))(lambda: in_bank(8 + 2 * j + e)))
            multiply(*((j, e, bank.at[8 + 2 * j + e]) for e in BOTH))
            for e in BOTH:
                load_tile(8 + 2 * j + e, 2, 2 * j + e)

        def group12(k, j):
            def ready(rows):
                arrived(2 + 2 * j, k, rows)
                arrived(3 + 2 * j, 1 - k, rows)

                @pl.when(j == 0)
                def _():
                    to_partner(2, 4, k, rows).start()
                    to_partner(3, 5, 1 - k, rows).start()

                pl.when(k + j == 0)(lambda: _start([onward(0, rows), onward(1, rows)]))

            for_caps(t, ready)
            at = 2 * k + j
            pl.when((t > 1) | (at > 1))(lambda: in_bank(8 + at))
            pl.when((t == 1) & (at >= other_each))(lambda: in_bank(at))
            multiply((2 + 2 * j, k, bank.at[at]), (3 + 2 * j, 1 - k, bank.at[8 + at]))

        def next_tiles(k):
            def body(e):
                i = 2 * k + e
                pl.when(t < final)(lambda: load_tile(8 + i, 0, i))

                @pl.when(t == final)
                def _():
                    load_turned(8 + i, 12 + i)
                    pl.when(k == 0)(lambda: load_turned(i, 4 + i))

            _loop(2, body)

        def group3(j):
            def ready(rows):
                for half in BOTH:
                    arrived(6 + j, half, rows)

                @pl.when(j == 0)
                def _():
                    for half in BOTH:
                        to_partner(6, 7, half, rows).start()

            for_caps(t, ready)
            multiply(*((6 + j, e, bank.at[4 + 2 * j + e]) for e in BOTH))

        with jax.named_scope("f0"):
            _loop(2, group0)

        @pl.when(t == 1)
        def _():
            _loop(4, lambda i: load_tile(4 + i, 3, i))
            _loop(other_each, in_bank)

        with jax.named_scope("ft"):
            turn_others(t)
        pl.when(t == final)(lambda: _loop(depth, lambda k: strip_copy(0, 0, k).wait()))

        def groups12(k):
            with jax.named_scope("f1"):
                _loop(2, functools.partial(group12, k))
            pl.when((k == 1) & (t > 1) & (t < 4))(lambda: turn(8 + t, 8 + t, False))
            next_tiles(k)

        _loop(2, groups12)
        pl.when(t == 1)(lambda: _loop(4, lambda i: in_bank(4 + i)))
        with jax.named_scope("f3"):
            _loop(2, group3)

        @pl.when(t == final)
        def _():
            _loop(4, lambda i: load_turned(4 + i, 8 + i))
            _loop(2, lambda i: load_turned(2 + i, 6 + i))

        def drained(rows):
            for cp in own_copies(rows):
                cp.wait_send()
            for half in BOTH:
                to_partner(2, 4, half, rows).wait_send()
                to_partner(3, 5, half, rows).wait_send()
                to_partner(6, 7, half, rows).wait_send()
                onward(half, rows).wait_send()

        for_caps(t, drained)
        for_each(t, lambda tt, rows: _wait(save_copies(tt, rows)))
        em_copy(t).wait()
        with jax.named_scope("fw"):
            weigh(t)

    _loop(step_count, forward)

    def post_copy(h):
        return pltpu.make_async_copy(cur.at[h], post_hbm.at[:, pl.ds(pl.multiple_of(h * hb, hb), hb)], post_sem.at[h])

    _loop(2, lambda h: post_copy(h).start())

    back_caps = functools.partial(for_caps, first=2)

    def weights(t):
        def body(i):
            r = eight(i)
            rc = rcs[t, r, :]
            live, later = t < lcol_ref[r, :], t + 1 < lcol_ref[r, :]
            for k in range(tiles):
                h, col = inner(k)
                beta = jnp.where(later, acc[h, r, col] + fin[0, h, r, col] + fin[1, h, r, col], 1.0)
                val = emv[t % 2, r, lane(k)].astype(F32) * beta * rc
                strips[h, r, col] = jnp.where(live, val, 0.0).astype(BF16)

        _loop(kept // 8, body)

    def w_copies(t, rows):
        to = pl.ds(firsts[t - 1], rows)
        return [pltpu.make_async_copy(strips.at[h, pl.ds(0, rows)], w_hbm.at[to, pl.ds(h * hb, hb)], save_sem.at[h])
                for h in BOTH]

    sub = hb // 2

    def part(s, base=0):
        return pl.ds(pl.multiple_of(base + s * sub, sub), sub)

    def partial_sums(out, tile, s):
        out[sent, part(s)] = _dot(strips[0, sent, :], tile[:, part(s)]) + _dot(strips[1, sent, :], tile[:, part(s, hb)])

    def add_into(out, s, *terms):
        def body(i):
            r = eight(i)
            val = out[r, part(s)]
            for term in terms:
                val = val + term[r, part(s)]
            out[r, part(s)] = val

        _loop(kept // 8, body)

    def to_core(q, s, rows):
        at = (q, pl.ds(0, rows), part(s))
        return remote(ost.at[at], dbuf.at[at], d_send.at[q, s], d_recv.at[q, s], partner)

    def staged(n, q):
        return work.at[(1 - n % 2) * (2 + n) + q]

    def ring_copy(n, q, s, rows, dst, recv):
        src = staged(n, q).at[pl.ds(0, rows), part(s)]
        return remote(src, dst, s_send.at[2 * n + q, s], recv, dev(1 + (nx - 2) * q, 0))

    def far_copy(q, s, rows):
        return ring_copy(0, q, s, rows, trans.at[q, pl.ds(0, rows), part(s)], t_recv.at[q, s])

    def near_copy(n, q, s, rows):
        half = (n + q) % 2
        return ring_copy(n, q, s, rows, fin.at[q, half, pl.ds(0, rows), part(s)], f_recv.at[q, half, s])

    def freed(sem, q):
        pl.semaphore_signal(sem, inc=1, device_id={AXIS: dev(nx - 1 - (nx - 2) * q, 0)},
                            device_id_type=pl.DeviceIdType.MESH)

    def backward(idx):
        t = step_count - 1 - idx
        with jax.named_scope("bw"):
            weights(t)
        _loop(2, lambda q: freed(f_free.at[q], q))
        for_each(t, lambda tt, rows: _start(w_copies(tt, rows)))

        @pl.when(t > 2)
        def _():
            em_copy(t - 2).start()

        def slot_of(n, q, flip):
            inner = ((n + 1) % 4) // 2
            return (1 - inner) * (8 + 2 * flip + q) + inner * (4 * (1 - q) + 2 * (n - 1) + flip)

        def products(n, s, flip, outs):
            slots = [slot_of(n, q, flip) for q in BOTH]

            @pl.when((s == 0) & ((n % 3 == 0) | (idx == 0)))
            def _():
                for slot in slots:
                    in_bank(slot)

            for slot, out in zip(slots, outs):
                partial_sums(out, bank.at[slot], s)

            @pl.when((s == 1) & (n == 0))
            def _():
                for slot in slots:
                    load_turned(slot, slot - 8)

            @pl.when((s == 1) & (n == 3) & (t > 2))
            def _():
                for slot in slots:
                    load_turned(slot, slot + 4)

        def for_other(n, s):
            def drain(rows):
                for q in BOTH:
                    to_core(q, s, rows).wait_send()

            pl.when(n > 0)(lambda: back_caps(t, drain))
            products(n, s, 1, [ost.at[q] for q in BOTH])

            @pl.when((n > 0) | (idx > 0))
            def _():
                for q in BOTH:
                    pl.semaphore_wait(d_free.at[q, s], 1)

            back_caps(t, lambda rows: _start([to_core(q, s, rows) for q in BOTH]))

        def for_this(n, s):
            outs = [staged(n, q) for q in BOTH]
            pl.when((n == 2) & (idx == 0) & (s == 0))(lambda: _wait([post_copy(q) for q in BOTH]))

            def drain(rows):
                for q in BOTH:
                    near_copy(1, q, s, rows).wait_send()

            pl.when(n == 3)(lambda: back_caps(t, drain))
            products(n, s, 0, outs)

            def pass_on(q):
                out = staged(n, q)
                back_caps(t, lambda rows: to_core(q, s, rows).wait_recv())

                @pl.when(n == 2)
                def _():
                    back_caps(t, lambda rows: far_copy(q, s, rows).wait_recv())
                    add_into(out, s, dbuf.at[q], trans.at[q])
                    pl.when(t > 2)(lambda: freed(t_free.at[q, s], q))

                pl.when(n != 2)(lambda: add_into(out, s, dbuf.at[q]))

                @pl.when((n < 3) | (t > 2))
                def _():
                    pl.semaphore_signal(d_free.at[q, s], inc=1, device_id={AXIS: partner}, device_id_type=pl.DeviceIdType.MESH)

                @pl.when(n == 0)
                def _():
                    pl.when(idx > 0)(lambda: pl.semaphore_wait(t_free.at[q, s], 1))
                    back_caps(t, lambda rows: far_copy(q, s, rows).start())

                @pl.when((n == 1) | (n == 2))
                def _():
                    pl.when((n == 1) & (s == 0))(lambda: pl.semaphore_wait(f_free.at[q], 1))
                    back_caps(t, lambda rows: near_copy(n, q, s, rows).start())

            _loop(2, pass_on)

        def stage(h):
            n, s = h // 2, h % 2
            with jax.named_scope("bo"):
                for_other(n, s)
            with jax.named_scope("bt"):
                for_this(n, s)

        _loop(8, stage)

        def landed(rows):
            for q in BOTH:
                for s in BOTH:
                    near_copy(1, q, s, rows).wait_recv()
                    near_copy(2, q, s, rows).wait_recv()

        with jax.named_scope("bl"):
            back_caps(t, landed)

        def drained(rows):
            for q in BOTH:
                for s in BOTH:
                    for cp in (to_core(q, s, rows), far_copy(q, s, rows), near_copy(2, q, s, rows)):
                        cp.wait_send()

        with jax.named_scope("bd"):
            back_caps(t, drained)
        for_each(t, lambda tt, rows: _wait(w_copies(tt, rows)))

        @pl.when(t > 2)
        def _():
            em_copy(t - 2).wait()

    _loop(step_count - 2, backward)
    weights(1)

    def rest(i):
        r = eight(kept // 8 + i)
        rc = rcs[1, r, :]
        live = lcol_ref[r, :] > 1
        for k in range(tiles):
            h, col = inner(k)
            val = emv[1, r, lane(k)].astype(F32) * rc
            strips[h, r, col] = jnp.where(live, val, 0.0).astype(BF16)

    _loop((seqs - kept) // 8, rest)
    _start(w_copies(1, caps[0]))
    _wait(w_copies(1, caps[0]))


def _run_recursion(nd, caps, ident, trans_loc, em, init_loc, lcol, lrow):
    step_count, seqs, bs = em.shape
    hb = bs // 2
    kept = max(caps[1:])
    depth = min(8 if kept < seqs else 4, bs // LANES)
    dma = pltpu.SemaphoreType.DMA
    two, four = dma((2,)), dma((2, 2))
    credit, credits = pltpu.SemaphoreType.REGULAR((2,)), pltpu.SemaphoreType.REGULAR((2, 2))
    vm, hbm = pl.BlockSpec(memory_space=pltpu.VMEM), pl.BlockSpec(memory_space=pl.ANY)
    scratch = [
        pltpu.VMEM((12, hb, bs), BF16),
        pltpu.VMEM((8, 2, seqs, hb), BF16),
        pltpu.VMEM((6, seqs, hb), F32),
        pltpu.VMEM((2, seqs, bs), BF16),
        pltpu.VMEM((step_count, seqs, LANES), F32),
        pltpu.VMEM((seqs, LANES), F32),
        pltpu.VMEM((8, seqs), F32),
        pltpu.VMEM((nd, 8, seqs), F32),
        pltpu.VMEM((depth, LANES, hb), BF16),
        pltpu.VMEM((2, kept, hb), F32),
        pltpu.VMEM((2, kept, hb), F32),
        pltpu.VMEM((2, kept, hb), F32),
        pltpu.VMEM((2, 2, kept, hb), F32),
        dma((12,)), two, dma((nd, 2)), dma((3, 2)), dma((nd, 2)), two, dma((nd,)), dma((nd,)), two,
        two, dma((depth,)), four, four, dma((6, 2)), four, dma((2, 2, 2)), credits, credit, credits,
    ]
    return pl.pallas_call(
        functools.partial(_recursion, caps),
        name=f"recursion{ident}",
        out_shape=[
            jax.ShapeDtypeStruct((sum(caps), bs), BF16),
            jax.ShapeDtypeStruct((sum(caps), bs), BF16),
            jax.ShapeDtypeStruct((seqs, bs), F32),
            jax.ShapeDtypeStruct((8, seqs), F32),
            jax.ShapeDtypeStruct(trans_loc.shape, BF16),
        ],
        in_specs=[hbm, hbm, vm, vm, vm],
        out_specs=[hbm, hbm, hbm, vm, hbm],
        scratch_shapes=scratch,
        compiler_params=pltpu.CompilerParams(collective_id=ident, has_side_effects=True, vmem_limit_bytes=67_043_328),
    )(trans_loc, em, init_loc[None, :], lcol, lrow)


def _prepare(choices, tok_ref, len_ref, emt_hbm, em_hbm, lcol_ref, lrow_ref, rank_ref, level_ref,
             table, stable, picked, blocks, stage, table_sem, block_sem, stage_sem):
    step_count, seqs, bs = em_hbm.shape
    deep = blocks.shape[0]
    part = 32
    slab = min(512, bs)
    sub = lax.broadcasted_iota(jnp.int32, (seqs, LANES), 0)
    lan = lax.broadcasted_iota(jnp.int32, (seqs, LANES), 1)
    across = jnp.broadcast_to(len_ref[...].astype(F32), (seqs, seqs))
    down = jnp.transpose(across)
    ahead = (down > across) | ((down == across) & (sub < lan))
    rank = jnp.sum(jnp.where(ahead, 1.0, 0.0), axis=0, keepdims=True)
    rank_ref[...] = jnp.broadcast_to(rank, rank_ref.shape)
    pick = rank == sub.astype(F32)
    lcol = jnp.broadcast_to(jnp.sum(jnp.where(pick, across, 0.0), axis=1, keepdims=True), (seqs, LANES))
    lcol_ref[...] = lcol.astype(jnp.int32)
    lrow_ref[...] = jnp.transpose(lcol)[0:8].astype(jnp.int32)
    mat = jnp.zeros((seqs, LANES), F32)
    for t in range(step_count):
        tok = jnp.sum(jnp.where(pick, tok_ref[t : t + 1, :].astype(F32), 0.0), axis=1, keepdims=True)
        tok = jnp.broadcast_to(tok, (seqs, LANES))
        mat = jnp.where(lan == t, tok, mat)
        picked[t] = tok.astype(jnp.int32) & 7
    table[0:8] = jnp.transpose(mat)[0:8].astype(jnp.int32)
    alive = jnp.sum(jnp.where(across[0:8] > sub[0:8].astype(F32), 1.0, 0.0), axis=1, keepdims=True)
    table[8:16] = jnp.broadcast_to(alive, (8, LANES)).astype(jnp.int32)
    copy = pltpu.make_async_copy(table, stable, table_sem)
    copy.start()
    copy.wait()
    level = jnp.int32(0)
    for k, caps in enumerate(choices):
        for t in range(1, step_count):
            level = jnp.where(stable[8 + t, 0] > caps[t - 1], k + 1, level)
    level_ref[0] = level

    def parts(t):
        return (stable[8 + t, 0] + (part - 1)) // part

    def fetch(t):
        def body(p, carry):
            for k in range(part):
                s = p * part + k
                pltpu.make_async_copy(emt_hbm.at[stable[t, s] >> 3], blocks.at[t % deep, s], block_sem.at[t % deep]).start()
            return carry

        lax.fori_loop(0, parts(t), body, 0)

    def landed(t):
        def body(p, carry):
            pltpu.make_async_copy(emt_hbm.at[pl.ds(0, part)], blocks.at[t % deep, pl.ds(0, part)], block_sem.at[t % deep]).wait()
            return carry

        lax.fori_loop(0, parts(t), body, 0)

    def select(t):
        def body(p, carry):
            r = pl.ds(pl.multiple_of(p * part, part), part)
            at = picked[t, r, :] + 8 * sub[0:part]
            one = jnp.concatenate([jnp.where(lan[0:part] + off == at, 1.0, 0.0) for off in (0, LANES)], axis=1).astype(BF16)
            for n in range(bs // slab):
                cols = pl.ds(n * slab, slab)
                rows = blocks[t % deep, r, :, cols].reshape(part * 8, slab)
                stage[t % 2, r, cols] = _dot(one, rows).astype(BF16)
            return carry

        lax.fori_loop(0, parts(t), body, 0)

    def out_copy(t):
        return pltpu.make_async_copy(stage.at[t % 2], em_hbm.at[t], stage_sem.at[t % 2])

    def position(t):
        pl.when(t >= 2)(lambda: out_copy(t - 2).wait())
        landed(t)
        select(t)
        out_copy(t).start()
        pl.when(t + deep < step_count)(lambda: fetch(t + deep))

    _loop(deep, fetch)
    _loop(step_count, position)
    _loop(2, lambda e: out_copy(step_count - 1 - e).wait())


def _run_prepare(choices, tokens, lengths, emit_loc):
    bs, symbols = emit_loc.shape
    seqs, step_count = tokens.shape
    dma = pltpu.SemaphoreType.DMA
    vm, hbm = pl.BlockSpec(memory_space=pltpu.VMEM), pl.BlockSpec(memory_space=pl.ANY)
    return pl.pallas_call(
        functools.partial(_prepare, choices),
        name="prepare",
        out_shape=[
            jax.ShapeDtypeStruct((step_count, seqs, bs), BF16),
            jax.ShapeDtypeStruct((seqs, LANES), jnp.int32),
            jax.ShapeDtypeStruct((8, seqs), jnp.int32),
            jax.ShapeDtypeStruct((8, seqs), F32),
            jax.ShapeDtypeStruct((1,), jnp.int32),
        ],
        in_specs=[vm, vm, hbm],
        out_specs=[hbm, vm, vm, vm, pl.BlockSpec(memory_space=pltpu.SMEM)],
        scratch_shapes=[
            pltpu.VMEM((16, LANES), jnp.int32),
            pltpu.SMEM((16, LANES), jnp.int32),
            pltpu.VMEM((step_count, seqs, LANES), jnp.int32),
            pltpu.VMEM((4, seqs, 8, bs), BF16),
            pltpu.VMEM((2, seqs, bs), BF16),
            dma, dma((4,)), dma((2,)),
        ],
        compiler_params=pltpu.CompilerParams(vmem_limit_bytes=60_000_000),
    )(tokens.T, lengths[None, :], emit_loc.T.reshape(symbols // 8, 8, bs))


def _counts(trans_hbm, alpha_hbm, w_hbm, post_hbm, ll_ref, rank_ref, counts_hbm, posterior_hbm, loglik_ref,
            alpha, w, diag, out, post, back, in_sem, alpha_sem, diag_sem, out_sem, back_sem):
    rows, bs = w.shape
    seqs = post.shape[0]
    steps, tile, _ = diag.shape
    slab = min(512, bs)
    first = lax.axis_index(AXIS) * bs
    post_load, w_load = (pltpu.make_async_copy(a, b, in_sem.at[k]) for k, (a, b) in enumerate(((post_hbm, post), (w_hbm, w))))
    _start((post_load, w_load))

    def alpha_copy(i):
        at = pl.multiple_of(i * tile, tile)
        return pltpu.make_async_copy(alpha_hbm.at[:, pl.ds(at, tile)], alpha.at[i], alpha_sem.at[i])

    def diag_copy(i):
        at = pl.multiple_of(first + i * tile, tile)
        return pltpu.make_async_copy(trans_hbm.at[pl.ds(at, tile)], diag.at[i], diag_sem.at[i])

    def out_copy(i):
        at = pl.multiple_of(i * tile, tile)
        return pltpu.make_async_copy(out.at[i], counts_hbm.at[pl.ds(at, tile)], out_sem.at[i])

    def bring(i):
        alpha_copy(i).start()
        diag_copy(i).start()

    _loop(steps, bring)

    rank = jnp.broadcast_to(rank_ref[0:1, :], (seqs, seqs))
    sub = lax.broadcasted_iota(jnp.int32, (seqs, seqs), 0).astype(F32)
    lan = lax.broadcasted_iota(jnp.int32, (seqs, seqs), 1).astype(F32)
    lls = jnp.transpose(jnp.broadcast_to(ll_ref[0:1, :], (seqs, seqs)))
    loglik_ref[...] = jnp.sum(jnp.where(rank == sub, lls, 0.0), axis=0, keepdims=True)
    order = jnp.where(jnp.transpose(rank) == lan, 1.0, 0.0).astype(BF16)
    post_load.wait()
    for n in range(bs // slab):
        cols = pl.ds(n * slab, slab)
        rest = post[:, cols]
        total = jnp.zeros(rest.shape, F32)
        for _ in range(3):
            head = rest.astype(BF16)
            rest = rest - head.astype(F32)
            total = total + _dot(order, head)
        back[:, cols] = total
    back_copy = pltpu.make_async_copy(back, posterior_hbm, back_sem)
    back_copy.start()
    w_load.wait()

    def step(i):
        alpha_copy(i).wait()
        lhs = alpha[i]
        diag_copy(i).wait()
        for n in range(bs // slab):
            cols = pl.ds(n * slab, slab)
            out[i, :, cols] = diag[i, :, cols].astype(F32) * _dot(lhs, w[:, cols], 0)
        out_copy(i).start()

    _loop(steps, step)
    _loop(steps, lambda i: out_copy(i).wait())
    back_copy.wait()


def _run_counts(alphas, ws, trans_loc, post, ll, rank):
    rows, bs = alphas.shape
    seqs = post.shape[0]
    tile = min(256, bs)
    steps = bs // tile
    dma = pltpu.SemaphoreType.DMA
    vm, hbm = pl.BlockSpec(memory_space=pltpu.VMEM), pl.BlockSpec(memory_space=pl.ANY)
    return pl.pallas_call(
        _counts,
        name="counts",
        out_shape=[
            jax.ShapeDtypeStruct((bs, bs), F32),
            jax.ShapeDtypeStruct((seqs, bs), F32),
            jax.ShapeDtypeStruct((1, seqs), F32),
        ],
        in_specs=[hbm, hbm, hbm, hbm, vm, vm],
        out_specs=[hbm, hbm, vm],
        scratch_shapes=[
            pltpu.VMEM((steps, rows, tile), BF16),
            pltpu.VMEM((rows, bs), BF16),
            pltpu.VMEM((steps, tile, bs), BF16),
            pltpu.VMEM((steps, tile, bs), F32),
            pltpu.VMEM((seqs, bs), F32),
            pltpu.VMEM((seqs, bs), F32),
            dma((2,)), dma((steps,)), dma((steps,)), dma((steps,)), dma,
        ],
        compiler_params=pltpu.CompilerParams(vmem_limit_bytes=60_000_000),
    )(trans_loc, alphas, ws, post, ll, rank)


def _capacities(seqs, step_count, spread):
    caps = []
    for t in range(1, step_count):
        live = (step_count - t) / step_count
        room = spread * math.sqrt((seqs - 1) * live * (1 - live))
        caps.append(min(seqs, 8 * math.ceil(((seqs - 1) * live + 1 + room) / 8)))
    return tuple(caps)


def solution(mesh):
    nd = mesh.shape[AXIS]

    def local_run(trans_loc, emit_loc, init_loc, tokens_loc, lengths_loc):
        seqs, step_count = tokens_loc.shape
        choices = [_capacities(seqs, step_count, spread) for spread in (2.7, 4.1)]
        em, lcol, lrow, rank, level = _run_prepare(choices, tokens_loc, lengths_loc, emit_loc)

        def run(ident, caps, trans, em, init, lcol, lrow, rank):
            alphas, ws, post, ll, _ = _run_recursion(nd, caps, ident, trans, em, init, lcol, lrow)
            return _run_counts(alphas, ws, trans, post, ll, rank)

        choices.append((seqs,) * (step_count - 1))
        runs = [functools.partial(run, k, caps) for k, caps in enumerate(choices)]
        counts, posterior, loglik = lax.switch(level[0], runs, trans_loc, em, init_loc, lcol, lrow, rank)
        return loglik[0], posterior, counts

    return jax.shard_map(
        local_run,
        mesh=mesh,
        in_specs=(P(None, AXIS), P(AXIS, None), P(AXIS), P("seqs", None), P("seqs")),
        out_specs=(P("seqs"), P("seqs", AXIS), P(("seqs", AXIS), None)),
        check_vma=False,
    )
```

```python
import functools
import math

import jax
import jax.numpy as jnp
from jax import lax
from jax.experimental import pallas as pl
from jax.experimental.pallas import tpu as pltpu
from jax.sharding import PartitionSpec as P

AXIS = "states"
LANES = 128
BOTH = (0, 1)
F32 = jnp.float32
BF16 = jnp.bfloat16


def _dot(a, b, over_a=1, over_b=0):
    dims = (((over_a,), (over_b,)), ((), ()))
    return lax.dot_general(a, b, dims, preferred_element_type=F32)


def _start(copies):
    for cp in copies:
        cp.start()


def _wait(copies):
    for cp in copies:
        cp.wait()


def _loop(n, body):
    def step(i, carry):
        body(i)
        return carry

    lax.fori_loop(0, n, step, 0)


def _recursion(caps, a_hbm, em_hbm, pi_ref, lcol_ref, lrow_ref, al_hbm, w_hbm, post_hbm, ll_ref, turned_hbm,
               bank, al, work, emv, rcs, sbuf, csend, cbuf, strips, ost, dbuf, trans, fin,
               bank_sem, em_sem, al_recv, own_send, part_send, on_send, c_send, c_recv, save_sem, post_sem,
               strip_sem, d_send, d_recv, s_send, t_recv, f_recv, t_free, f_free, d_free):
    nd = cbuf.shape[0]
    nx = nd // 2
    step_count, seqs, bs = em_hbm.shape
    hb = bs // 2
    firsts = [sum(caps[:t]) for t in range(step_count)]
    slab = min(512, hb)
    tiles = bs // LANES
    kept = max(caps[1:])
    sent = pl.ds(0, kept)
    final = step_count - 1
    g = lax.axis_index(AXIS)
    x, c = g // 2, g % 2

    def dev(dx, flip):
        return ((x + dx) % nx) * 2 + (c + flip) % 2

    partner, right, left = dev(0, 1), dev(1, 0), dev(nx - 1, 0)

    def remote(src, dst, send, recv, to):
        return pltpu.make_async_remote_copy(
            src_ref=src, dst_ref=dst, send_sem=send, recv_sem=recv,
            device_id={AXIS: to}, device_id_type=pl.DeviceIdType.MESH)

    def pick(t, fn, lo, hi):
        if hi - lo == 1:
            fn(lo)
        else:
            mid = (lo + hi) // 2
            lax.cond(t < mid, lambda: pick(t, fn, lo, mid), lambda: pick(t, fn, mid, hi))

    def for_each(t, fn):
        pick(t, lambda tt: fn(tt, caps[tt - 1]), 1, step_count)

    def for_caps(t, fn, first=1):
        if len(set(caps)) == 1:
            fn(caps[0])
        else:
            pick(t, lambda tt: fn(caps[tt - 1]), first, step_count)

    acc, cur = work.at[pl.ds(0, 2)], work.at[pl.ds(4, 2)]

    def tile_row(group, i):
        if group == 0:
            src, half = dev(0, i // 2), i % 2
        elif group == 1:
            src, half = dev(nx - 1, i % 2), i // 2
        elif group == 2:
            src, half = dev(1, i % 2), 1 - i // 2
        else:
            src, half = dev(2, i // 2), i % 2
        return src * bs + half * hb

    def load(slot, row, src):
        pltpu.make_async_copy(src.at[pl.ds(pl.multiple_of(row, hb), hb)], bank.at[slot], bank_sem.at[slot]).start()

    def load_tile(slot, group, i):
        load(slot, tile_row(group, i), a_hbm)

    def load_turned(slot, number):
        load(slot, number * hb, turned_hbm)

    def in_bank(slot):
        pltpu.make_async_copy(a_hbm.at[pl.ds(0, hb)], bank.at[slot], bank_sem.at[slot]).wait()

    depth = strips.shape[0]
    bunch = min(2, depth)

    def strip_copy(number, unit, k):
        rows = pl.ds(pl.multiple_of(number * hb + (unit % (tiles // 2)) * LANES, LANES), LANES)
        cols = pl.ds(pl.multiple_of((unit // (tiles // 2)) * hb, hb), hb)
        return pltpu.make_async_copy(strips.at[k], turned_hbm.at[rows, cols], strip_sem.at[k])

    def turn(slot, number, first):
        def body(i):
            units = [bunch * i + e for e in range(bunch)]

            @pl.when(jnp.logical_not(first) | (bunch * i >= depth))
            def _():
                for u in units:
                    strip_copy(0, 0, u % depth).wait()

            for u in units:
                strips[u % depth] = jnp.transpose(bank[slot, :, pl.ds(pl.multiple_of(u * LANES, LANES), LANES)])
            for u in units:
                strip_copy(number, u, u % depth).start()

        _loop(tiles // bunch, body)

    own_each, other_each = -(-7 // final), -(-5 // (final - 1))

    def turn_own(t):
        each = own_each

        def body(e):
            n = t * each + e
            far = n // 4
            pl.when(far == 0)(lambda: in_bank(8 + n))
            pl.when(n < 7)(lambda: turn(8 + n - far * 7, n + far * 9, n == 0))

        _loop(each, body)
        _loop(4, lambda i: pl.when((t > 0) & ((i < t * each) | (i >= t * each + each)))(lambda: in_bank(8 + i)))

    def turn_others(t):
        each = other_each

        def body(e):
            n = (t - 1) * each + e
            right = (e + LANES - each) // LANES
            slot = (1 - right) * n + right * (8 + e - each)
            number = (1 - right) * (4 + n + 4 * (n // 4)) + right * slot
            pl.when((right == 1) & (t == 1))(lambda: in_bank(slot))
            pl.when(((right == 1) & (t == 1)) | ((right == 0) & (n < 5)))(lambda: turn(slot, number, False))

        pl.when(t < final)(lambda: _loop(each + 2, body))

    def em_copy(t):
        return pltpu.make_async_copy(em_hbm.at[t], emv.at[t % 2], em_sem.at[t % 2])

    _loop(2, lambda t: em_copy(t).start())
    _loop(4, lambda i: load_tile(8 + i, 0, i))
    _loop(4, lambda i: load_tile(i, 1, i))

    barrier = pltpu.get_barrier_semaphore()
    for k in range(1, nd):
        pl.semaphore_signal(barrier, inc=1, device_id={AXIS: (g + k) % nd}, device_id_type=pl.DeviceIdType.MESH)
    tall = 16

    def rows_of(i):
        return pl.ds(pl.multiple_of(i * tall, tall), tall)

    def eight(i):
        return pl.ds(pl.multiple_of(i * 8, 8), 8)

    def lane(k):
        return pl.ds(k * LANES, LANES)

    def inner(k):
        return (k * LANES) // hb, pl.ds((k * LANES) % hb, LANES)

    def weigh(t):
        def body(i):
            r = rows_of(i)
            total = jnp.zeros((tall, LANES), F32)
            for k in range(tiles):
                e = emv[t % 2, r, lane(k)].astype(F32)
                h, col = inner(k)
                mass = acc[h, r, col] * e
                acc[h, r, col] = mass
                total = total + mass
            sbuf[r, :] = total

        _loop(seqs // tall, body)

    def normalise(t):
        row = jnp.sum(jnp.transpose(sbuf[...]), axis=0, keepdims=True)
        wide = jnp.broadcast_to(row, csend.shape)
        csend[...] = wide
        cbuf[g] = wide
        peers = [dev(dx, flip) for dx in (2, 1, nx - 1, 0) for flip in BOTH][: nd - 2] + [partner]
        copies = [remote(csend, cbuf.at[g], c_send.at[k], c_recv.at[g], to) for k, to in enumerate(peers)]
        _start(copies)

        with jax.named_scope("ft"):
            @pl.when(t < final)
            def _():
                turn_own(t)

        with jax.named_scope("fx"):
            for k, frm in enumerate(peers):
                remote(csend, cbuf.at[frm], c_send.at[k], c_recv.at[frm], frm).wait_recv()
        norm = cbuf[0, 0:1, :]
        for d in range(1, nd):
            norm = norm + cbuf[d, 0:1, :]
        rcs[t] = 1.0 / jnp.transpose(jnp.broadcast_to(norm, (LANES, LANES)))
        ll_ref[...] = ll_ref[...] + jnp.where(t < lrow_ref[...], jnp.log(jnp.broadcast_to(norm, ll_ref.shape)), 0.0)

        def body(i):
            r = rows_of(i)
            rc = rcs[t, r, :]
            live = t < lcol_ref[r, :]
            for k in range(tiles):
                h, col = inner(k)
                val = jnp.where(live, acc[h, r, col] * rc, cur[h, r, col])
                cur[h, r, col] = val
                al[0, h, r, col] = val.astype(BF16)

        _loop(seqs // tall, body)
        for cp in copies:
            cp.wait_send()

    ll_ref[...] = jnp.zeros_like(ll_ref)
    for h in BOTH:
        acc[h] = jnp.broadcast_to(pi_ref[:, pl.ds(h * hb, hb)], (seqs, hb))
    em_copy(0).wait()
    weigh(0)
    pl.semaphore_wait(barrier, nd - 1)

    def own_copies(rows):
        m = pl.ds(0, rows)
        out = [remote(al.at[0, h, m], al.at[1, h, m], own_send.at[0, h], al_recv.at[1, h], partner) for h in BOTH]
        for h in BOTH:
            out.append(remote(al.at[0, h, m], al.at[2, h, m], own_send.at[1, h], al_recv.at[2, h], right))
            out.append(remote(al.at[0, 1 - h, m], al.at[3, 1 - h, m], own_send.at[2, 1 - h], al_recv.at[3, 1 - h], left))
        return out

    def to_partner(slot, to_slot, half, rows):
        m = pl.ds(0, rows)
        return remote(al.at[slot, half, m], al.at[to_slot, half, m], part_send.at[slot, half], al_recv.at[to_slot, half], partner)

    def onward(s, rows):
        m = pl.ds(0, rows)
        return remote(al.at[2 + s, s, m], al.at[6, s, m], on_send.at[s], al_recv.at[6, s], dev(1 + (nx - 2) * s, 0))

    def arrived(slot, half, rows):
        m = pl.ds(0, rows)
        remote(al.at[slot, half, m], al.at[slot, half, m], part_send.at[slot, half], al_recv.at[slot, half], partner).wait_recv()

    def save_copies(t, rows):
        to = pl.ds(firsts[t - 1], rows)
        return [pltpu.make_async_copy(al.at[0, h, pl.ds(0, rows)], al_hbm.at[to, pl.ds(h * hb, hb)], save_sem.at[h])
                for h in BOTH]

    def multiply(one, two):
        (slot1, half1, tile1), (slot2, half2, tile2) = one, two
        lhs1, lhs2 = al[slot1, half1], al[slot2, half2]
        for h in BOTH:
            for n in range(hb // slab):
                cols, at = pl.ds(h * hb + n * slab, slab), pl.ds(n * slab, slab)
                acc[h, :, at] = acc[h, :, at] + (
                    _dot(lhs1, tile1[:, cols]) + _dot(lhs2, tile2[:, cols]))

    def forward(t):
        pl.when(t > 0)(lambda: predict(t))
        normalise(t)

    def predict(t):
        for_caps(t, lambda rows: _start(own_copies(rows)))
        for_each(t, lambda tt, rows: _start(save_copies(tt, rows)))

        @pl.when(t + 1 < step_count)
        def _():
            em_copy(t + 1).start()

        acc[...] = jnp.zeros(acc.shape, F32)

        def group0(j):
            def ready(rows):
                for half in BOTH:
                    arrived(1, half, rows)

            pl.when(j > 0)(lambda: for_caps(t, ready))
            _loop(2, lambda e: pl.when((t == 1) & (2 * j + e >= own_each))(lambda: in_bank(8 + 2 * j + e)))
            multiply(*((j, e, bank.at[8 + 2 * j + e]) for e in BOTH))
            for e in BOTH:
                load_tile(8 + 2 * j + e, 2, 2 * j + e)

        def group12(k, j):
            def ready(rows):
                arrived(2 + 2 * j, k, rows)
                arrived(3 + 2 * j, 1 - k, rows)

                @pl.when(j == 0)
                def _():
                    to_partner(2, 4, k, rows).start()
                    to_partner(3, 5, 1 - k, rows).start()

                pl.when(k + j == 0)(lambda: _start([onward(0, rows), onward(1, rows)]))

            for_caps(t, ready)
            at = 2 * k + j
            pl.when((t > 1) | (at > 1))(lambda: in_bank(8 + at))
            pl.when((t == 1) & (at >= other_each))(lambda: in_bank(at))
            multiply((2 + 2 * j, k, bank.at[at]), (3 + 2 * j, 1 - k, bank.at[8 + at]))

        def next_tiles(k):
            def body(e):
                i = 2 * k + e
                pl.when(t < final)(lambda: load_tile(8 + i, 0, i))

                @pl.when(t == final)
                def _():
                    load_turned(8 + i, 12 + i)
                    pl.when(k == 0)(lambda: load_turned(i, 4 + i))

            _loop(2, body)

        def group3(j):
            def ready(rows):
                for half in BOTH:
                    arrived(6 + j, half, rows)

                @pl.when(j == 0)
                def _():
                    for half in BOTH:
                        to_partner(6, 7, half, rows).start()

            for_caps(t, ready)
            multiply(*((6 + j, e, bank.at[4 + 2 * j + e]) for e in BOTH))

        with jax.named_scope("f0"):
            _loop(2, group0)

        @pl.when(t == 1)
        def _():
            _loop(4, lambda i: load_tile(4 + i, 3, i))
            _loop(other_each, in_bank)

        with jax.named_scope("ft"):
            turn_others(t)
        pl.when(t == final)(lambda: _loop(depth, lambda k: strip_copy(0, 0, k).wait()))

        def groups12(k):
            with jax.named_scope("f1"):
                _loop(2, functools.partial(group12, k))
            pl.when((k == 1) & (t > 1) & (t < 4))(lambda: turn(8 + t, 8 + t, False))
            next_tiles(k)

        _loop(2, groups12)
        pl.when(t == 1)(lambda: _loop(4, lambda i: in_bank(4 + i)))
        with jax.named_scope("f3"):
            _loop(2, group3)

        @pl.when(t == final)
        def _():
            _loop(4, lambda i: load_turned(4 + i, 8 + i))
            _loop(2, lambda i: load_turned(2 + i, 6 + i))

        def drained(rows):
            for cp in own_copies(rows):
                cp.wait_send()
            for half in BOTH:
                to_partner(2, 4, half, rows).wait_send()
                to_partner(3, 5, half, rows).wait_send()
                to_partner(6, 7, half, rows).wait_send()
                onward(half, rows).wait_send()

        for_caps(t, drained)
        for_each(t, lambda tt, rows: _wait(save_copies(tt, rows)))
        em_copy(t).wait()
        with jax.named_scope("fw"):
            weigh(t)

    _loop(step_count, forward)

    def post_copy(h):
        return pltpu.make_async_copy(cur.at[h], post_hbm.at[:, pl.ds(pl.multiple_of(h * hb, hb), hb)], post_sem.at[h])

    _loop(2, lambda h: post_copy(h).start())

    back_caps = functools.partial(for_caps, first=2)

    def weights(t):
        def body(i):
            r = eight(i)
            rc = rcs[t, r, :]
            live, later = t < lcol_ref[r, :], t + 1 < lcol_ref[r, :]
            for k in range(tiles):
                h, col = inner(k)
                beta = jnp.where(later, acc[h, r, col] + fin[0, h, r, col] + fin[1, h, r, col], 1.0)
                val = emv[t % 2, r, lane(k)].astype(F32) * beta * rc
                strips[h, r, col] = jnp.where(live, val, 0.0).astype(BF16)

        _loop(kept // 8, body)

    def w_copies(t, rows):
        to = pl.ds(firsts[t - 1], rows)
        return [pltpu.make_async_copy(strips.at[h, pl.ds(0, rows)], w_hbm.at[to, pl.ds(h * hb, hb)], save_sem.at[h])
                for h in BOTH]

    def partial_sums(out, tile):
        for n in range(hb // slab):
            cols = pl.ds(n * slab, slab)
            more = pl.ds(hb + n * slab, slab)
            out[sent, cols] = _dot(strips[0, sent, :], tile[:, cols]) + _dot(strips[1, sent, :], tile[:, more])

    def add_into(out, *terms):
        def body(i):
            r = eight(i)
            val = out[r, :]
            for term in terms:
                val = val + term[r, :]
            out[r, :] = val

        _loop(kept // 8, body)

    def to_core(q, rows):
        m = pl.ds(0, rows)
        return remote(ost.at[q, m], dbuf.at[q, m], d_send.at[q], d_recv.at[q], partner)

    def staged(p):
        n, q = p // 2, p % 2
        return (1 - n % 2) * (2 + n) + q

    def ring_copy(far, p, rows):
        m, q = pl.ds(0, rows), p % 2
        to = dev(1 + (nx - 2) * q, 0)
        src, send = work.at[staged(p), m], s_send.at[p]
        if far:
            return remote(src, trans.at[q, m], send, t_recv.at[q], to)
        half = (p // 2 + q) % 2
        return remote(src, fin.at[q, half, m], send, f_recv.at[q, half], to)

    def freed(sem, q):
        pl.semaphore_signal(sem.at[q], inc=1, device_id={AXIS: dev(nx - 1 - (nx - 2) * q, 0)},
                            device_id_type=pl.DeviceIdType.MESH)

    def backward(idx):
        t = step_count - 1 - idx
        with jax.named_scope("bw"):
            weights(t)
        _loop(2, functools.partial(freed, f_free))
        for_each(t, lambda tt, rows: _start(w_copies(tt, rows)))

        @pl.when(t > 2)
        def _():
            em_copy(t - 2).start()

        def slot_of(p, flip):
            n, q = p // 2, p % 2
            inner = ((n + 1) % 4) // 2
            return inner == 0, (1 - inner) * (8 + 2 * flip + q) + inner * (4 * (1 - q) + 2 * (n - 1) + flip)

        def products(n, flip, outs):
            outer, _ = slot_of(2 * n, flip)
            slots = [slot_of(2 * n + q, flip)[1] for q in BOTH]

            @pl.when(outer | (idx == 0))
            def _():
                for slot in slots:
                    in_bank(slot)

            for slot, out in zip(slots, outs):
                partial_sums(out, bank.at[slot])

            @pl.when(n == 0)
            def _():
                for slot in slots:
                    load_turned(slot, slot - 8)

            @pl.when((n == 3) & (t > 2))
            def _():
                for slot in slots:
                    load_turned(slot, slot + 4)

        def for_other(n):
            def drain(rows):
                for q in BOTH:
                    to_core(q, rows).wait_send()

            pl.when(n > 0)(lambda: back_caps(t, drain))
            products(n, 1, [ost.at[q] for q in BOTH])

            @pl.when((n > 0) | (idx > 0))
            def _():
                for q in BOTH:
                    pl.semaphore_wait(d_free.at[q], 1)

            back_caps(t, lambda rows: _start([to_core(q, rows) for q in BOTH]))

        def for_this(n):
            outs = [work.at[staged(2 * n + q)] for q in BOTH]
            pl.when((n == 2) & (idx == 0))(lambda: _wait([post_copy(q) for q in BOTH]))

            def drain(rows):
                for q in BOTH:
                    ring_copy(False, 2 + q, rows).wait_send()

            pl.when(n == 3)(lambda: back_caps(t, drain))
            products(n, 0, outs)
            for q, out in enumerate(outs):
                p = 2 * n + q
                back_caps(t, lambda rows: to_core(q, rows).wait_recv())

                @pl.when(n == 2)
                def _():
                    back_caps(t, lambda rows: ring_copy(True, q, rows).wait_recv())
                    add_into(out, dbuf.at[q], trans.at[q])
                    pl.when(t > 2)(lambda: freed(t_free, q))

                pl.when(n != 2)(lambda: add_into(out, dbuf.at[q]))

                @pl.when((n < 3) | (t > 2))
                def _():
                    pl.semaphore_signal(d_free.at[q], inc=1, device_id={AXIS: partner}, device_id_type=pl.DeviceIdType.MESH)

                @pl.when(n == 0)
                def _():
                    pl.when(idx > 0)(lambda: pl.semaphore_wait(t_free.at[q], 1))
                    back_caps(t, lambda rows: ring_copy(True, q, rows).start())

                @pl.when((n == 1) | (n == 2))
                def _():
                    pl.when(n == 1)(lambda: pl.semaphore_wait(f_free.at[q], 1))
                    back_caps(t, lambda rows: ring_copy(False, p, rows).start())

        def stage(n):
            with jax.named_scope("bo"):
                for_other(n)
            with jax.named_scope("bt"):
                for_this(n)

        _loop(4, stage)

        def landed(rows):
            for p in range(2, 6):
                ring_copy(False, p, rows).wait_recv()

        with jax.named_scope("bl"):
            back_caps(t, landed)

        def drained(rows):
            for q in BOTH:
                for cp in (to_core(q, rows), ring_copy(True, q, rows), ring_copy(False, 4 + q, rows)):
                    cp.wait_send()

        with jax.named_scope("bd"):
            back_caps(t, drained)
        for_each(t, lambda tt, rows: _wait(w_copies(tt, rows)))

        @pl.when(t > 2)
        def _():
            em_copy(t - 2).wait()

    _loop(step_count - 2, backward)
    weights(1)

    def rest(i):
        r = eight(kept // 8 + i)
        rc = rcs[1, r, :]
        live = lcol_ref[r, :] > 1
        for k in range(tiles):
            h, col = inner(k)
            val = emv[1, r, lane(k)].astype(F32) * rc
            strips[h, r, col] = jnp.where(live, val, 0.0).astype(BF16)

    _loop((seqs - kept) // 8, rest)
    _start(w_copies(1, caps[0]))
    _wait(w_copies(1, caps[0]))


def _run_recursion(nd, caps, ident, trans_loc, em, init_loc, lcol, lrow):
    step_count, seqs, bs = em.shape
    hb = bs // 2
    kept = max(caps[1:])
    depth = min(8 if kept < seqs else 4, bs // LANES)
    dma = pltpu.SemaphoreType.DMA
    two, credit = dma((2,)), pltpu.SemaphoreType.REGULAR((2,))
    vm, hbm = pl.BlockSpec(memory_space=pltpu.VMEM), pl.BlockSpec(memory_space=pl.ANY)
    scratch = [
        pltpu.VMEM((12, hb, bs), BF16),
        pltpu.VMEM((8, 2, seqs, hb), BF16),
        pltpu.VMEM((6, seqs, hb), F32),
        pltpu.VMEM((2, seqs, bs), BF16),
        pltpu.VMEM((step_count, seqs, LANES), F32),
        pltpu.VMEM((seqs, LANES), F32),
        pltpu.VMEM((8, seqs), F32),
        pltpu.VMEM((nd, 8, seqs), F32),
        pltpu.VMEM((depth, LANES, hb), BF16),
        pltpu.VMEM((2, kept, hb), F32),
        pltpu.VMEM((2, kept, hb), F32),
        pltpu.VMEM((2, kept, hb), F32),
        pltpu.VMEM((2, 2, kept, hb), F32),
        dma((12,)), two, dma((nd, 2)), dma((3, 2)), dma((nd, 2)), two, dma((nd,)), dma((nd,)), two,
        two, dma((depth,)), two, two, dma((6,)), two, dma((2, 2)), credit, credit, credit,
    ]
    return pl.pallas_call(
        functools.partial(_recursion, caps),
        name=f"recursion{ident}",
        out_shape=[
            jax.ShapeDtypeStruct((sum(caps), bs), BF16),
            jax.ShapeDtypeStruct((sum(caps), bs), BF16),
            jax.ShapeDtypeStruct((seqs, bs), F32),
            jax.ShapeDtypeStruct((8, seqs), F32),
            jax.ShapeDtypeStruct(trans_loc.shape, BF16),
        ],
        in_specs=[hbm, hbm, vm, vm, vm],
        out_specs=[hbm, hbm, hbm, vm, hbm],
        scratch_shapes=scratch,
        compiler_params=pltpu.CompilerParams(collective_id=ident, has_side_effects=True, vmem_limit_bytes=67_043_328),
    )(trans_loc, em, init_loc[None, :], lcol, lrow)


def _prepare(choices, tok_ref, len_ref, emt_hbm, em_hbm, lcol_ref, lrow_ref, rank_ref, level_ref,
             table, stable, picked, blocks, stage, table_sem, block_sem, stage_sem):
    step_count, seqs, bs = em_hbm.shape
    deep = blocks.shape[0]
    part = 32
    slab = min(512, bs)
    sub = lax.broadcasted_iota(jnp.int32, (seqs, LANES), 0)
    lan = lax.broadcasted_iota(jnp.int32, (seqs, LANES), 1)
    across = jnp.broadcast_to(len_ref[...].astype(F32), (seqs, seqs))
    down = jnp.transpose(across)
    ahead = (down > across) | ((down == across) & (sub < lan))
    rank = jnp.sum(jnp.where(ahead, 1.0, 0.0), axis=0, keepdims=True)
    rank_ref[...] = jnp.broadcast_to(rank, rank_ref.shape)
    pick = rank == sub.astype(F32)
    lcol = jnp.broadcast_to(jnp.sum(jnp.where(pick, across, 0.0), axis=1, keepdims=True), (seqs, LANES))
    lcol_ref[...] = lcol.astype(jnp.int32)
    lrow_ref[...] = jnp.transpose(lcol)[0:8].astype(jnp.int32)
    mat = jnp.zeros((seqs, LANES), F32)
    for t in range(step_count):
        tok = jnp.sum(jnp.where(pick, tok_ref[t : t + 1, :].astype(F32), 0.0), axis=1, keepdims=True)
        tok = jnp.broadcast_to(tok, (seqs, LANES))
        mat = jnp.where(lan == t, tok, mat)
        picked[t] = tok.astype(jnp.int32) & 7
    table[0:8] = jnp.transpose(mat)[0:8].astype(jnp.int32)
    alive = jnp.sum(jnp.where(across[0:8] > sub[0:8].astype(F32), 1.0, 0.0), axis=1, keepdims=True)
    table[8:16] = jnp.broadcast_to(alive, (8, LANES)).astype(jnp.int32)
    copy = pltpu.make_async_copy(table, stable, table_sem)
    copy.start()
    copy.wait()
    level = jnp.int32(0)
    for k, caps in enumerate(choices):
        for t in range(1, step_count):
            level = jnp.where(stable[8 + t, 0] > caps[t - 1], k + 1, level)
    level_ref[0] = level

    def parts(t):
        return (stable[8 + t, 0] + (part - 1)) // part

    def fetch(t):
        def body(p, carry):
            for k in range(part):
                s = p * part + k
                pltpu.make_async_copy(emt_hbm.at[stable[t, s] >> 3], blocks.at[t % deep, s], block_sem.at[t % deep]).start()
            return carry

        lax.fori_loop(0, parts(t), body, 0)

    def landed(t):
        def body(p, carry):
            pltpu.make_async_copy(emt_hbm.at[pl.ds(0, part)], blocks.at[t % deep, pl.ds(0, part)], block_sem.at[t % deep]).wait()
            return carry

        lax.fori_loop(0, parts(t), body, 0)

    def select(t):
        def body(p, carry):
            r = pl.ds(pl.multiple_of(p * part, part), part)
            at = picked[t, r, :] + 8 * sub[0:part]
            one = jnp.concatenate([jnp.where(lan[0:part] + off == at, 1.0, 0.0) for off in (0, LANES)], axis=1).astype(BF16)
            for n in range(bs // slab):
                cols = pl.ds(n * slab, slab)
                rows = blocks[t % deep, r, :, cols].reshape(part * 8, slab)
                stage[t % 2, r, cols] = _dot(one, rows).astype(BF16)
            return carry

        lax.fori_loop(0, parts(t), body, 0)

    def out_copy(t):
        return pltpu.make_async_copy(stage.at[t % 2], em_hbm.at[t], stage_sem.at[t % 2])

    def position(t):
        pl.when(t >= 2)(lambda: out_copy(t - 2).wait())
        landed(t)
        select(t)
        out_copy(t).start()
        pl.when(t + deep < step_count)(lambda: fetch(t + deep))

    _loop(deep, fetch)
    _loop(step_count, position)
    _loop(2, lambda e: out_copy(step_count - 1 - e).wait())


def _run_prepare(choices, tokens, lengths, emit_loc):
    bs, symbols = emit_loc.shape
    seqs, step_count = tokens.shape
    dma = pltpu.SemaphoreType.DMA
    vm, hbm = pl.BlockSpec(memory_space=pltpu.VMEM), pl.BlockSpec(memory_space=pl.ANY)
    return pl.pallas_call(
        functools.partial(_prepare, choices),
        name="prepare",
        out_shape=[
            jax.ShapeDtypeStruct((step_count, seqs, bs), BF16),
            jax.ShapeDtypeStruct((seqs, LANES), jnp.int32),
            jax.ShapeDtypeStruct((8, seqs), jnp.int32),
            jax.ShapeDtypeStruct((8, seqs), F32),
            jax.ShapeDtypeStruct((1,), jnp.int32),
        ],
        in_specs=[vm, vm, hbm],
        out_specs=[hbm, vm, vm, vm, pl.BlockSpec(memory_space=pltpu.SMEM)],
        scratch_shapes=[
            pltpu.VMEM((16, LANES), jnp.int32),
            pltpu.SMEM((16, LANES), jnp.int32),
            pltpu.VMEM((step_count, seqs, LANES), jnp.int32),
            pltpu.VMEM((4, seqs, 8, bs), BF16),
            pltpu.VMEM((2, seqs, bs), BF16),
            dma, dma((4,)), dma((2,)),
        ],
        compiler_params=pltpu.CompilerParams(vmem_limit_bytes=60_000_000),
    )(tokens.T, lengths[None, :], emit_loc.T.reshape(symbols // 8, 8, bs))


def _counts(trans_hbm, alpha_hbm, w_hbm, post_hbm, ll_ref, rank_ref, counts_hbm, posterior_hbm, loglik_ref,
            alpha, w, diag, out, post, back, in_sem, alpha_sem, diag_sem, out_sem, back_sem):
    rows, bs = w.shape
    seqs = post.shape[0]
    steps, tile, _ = diag.shape
    slab = min(512, bs)
    first = lax.axis_index(AXIS) * bs
    loads = [pltpu.make_async_copy(post_hbm, post, in_sem.at[0]), pltpu.make_async_copy(w_hbm, w, in_sem.at[1])]
    _start(loads)

    def alpha_copy(i):
        at = pl.multiple_of(i * tile, tile)
        return pltpu.make_async_copy(alpha_hbm.at[:, pl.ds(at, tile)], alpha.at[i], alpha_sem.at[i])

    def diag_copy(i):
        at = pl.multiple_of(first + i * tile, tile)
        return pltpu.make_async_copy(trans_hbm.at[pl.ds(at, tile)], diag.at[i], diag_sem.at[i])

    def out_copy(i):
        at = pl.multiple_of(i * tile, tile)
        return pltpu.make_async_copy(out.at[i], counts_hbm.at[pl.ds(at, tile)], out_sem.at[i])

    def bring(i):
        alpha_copy(i).start()
        diag_copy(i).start()

    _loop(steps, bring)

    rank = jnp.broadcast_to(rank_ref[0:1, :], (seqs, seqs))
    sub = lax.broadcasted_iota(jnp.int32, (seqs, seqs), 0).astype(F32)
    lan = lax.broadcasted_iota(jnp.int32, (seqs, seqs), 1).astype(F32)
    lls = jnp.transpose(jnp.broadcast_to(ll_ref[0:1, :], (seqs, seqs)))
    loglik_ref[...] = jnp.sum(jnp.where(rank == sub, lls, 0.0), axis=0, keepdims=True)
    order = jnp.where(jnp.transpose(rank) == lan, 1.0, 0.0).astype(BF16)
    loads[0].wait()
    for n in range(bs // slab):
        cols = pl.ds(n * slab, slab)
        rest = post[:, cols]
        total = jnp.zeros(rest.shape, F32)
        for _ in range(3):
            head = rest.astype(BF16)
            rest = rest - head.astype(F32)
            total = total + _dot(order, head)
        back[:, cols] = total
    back_copy = pltpu.make_async_copy(back, posterior_hbm, back_sem)
    back_copy.start()
    loads[1].wait()

    def step(i):
        alpha_copy(i).wait()
        lhs = alpha[i]
        diag_copy(i).wait()
        for n in range(bs // slab):
            cols = pl.ds(n * slab, slab)
            out[i, :, cols] = diag[i, :, cols].astype(F32) * _dot(lhs, w[:, cols], 0)
        out_copy(i).start()

    _loop(steps, step)
    _loop(steps, lambda i: out_copy(i).wait())
    back_copy.wait()


def _run_counts(alphas, ws, trans_loc, post, ll, rank):
    rows, bs = alphas.shape
    seqs = post.shape[0]
    tile = min(256, bs)
    steps = bs // tile
    dma = pltpu.SemaphoreType.DMA
    vm, hbm = pl.BlockSpec(memory_space=pltpu.VMEM), pl.BlockSpec(memory_space=pl.ANY)
    return pl.pallas_call(
        _counts,
        name="counts",
        out_shape=[
            jax.ShapeDtypeStruct((bs, bs), F32),
            jax.ShapeDtypeStruct((seqs, bs), F32),
            jax.ShapeDtypeStruct((1, seqs), F32),
        ],
        in_specs=[hbm, hbm, hbm, hbm, vm, vm],
        out_specs=[hbm, hbm, vm],
        scratch_shapes=[
            pltpu.VMEM((steps, rows, tile), BF16),
            pltpu.VMEM((rows, bs), BF16),
            pltpu.VMEM((steps, tile, bs), BF16),
            pltpu.VMEM((steps, tile, bs), F32),
            pltpu.VMEM((seqs, bs), F32),
            pltpu.VMEM((seqs, bs), F32),
            dma((2,)), dma((steps,)), dma((steps,)), dma((steps,)), dma,
        ],
        compiler_params=pltpu.CompilerParams(vmem_limit_bytes=60_000_000),
    )(trans_loc, alphas, ws, post, ll, rank)


def _capacities(seqs, step_count, spread):
    caps = []
    for t in range(1, step_count):
        live = (step_count - t) / step_count
        room = spread * math.sqrt((seqs - 1) * live * (1 - live))
        caps.append(min(seqs, 8 * math.ceil(((seqs - 1) * live + 1 + room) / 8)))
    return tuple(caps)


def solution(mesh):
    nd = mesh.shape[AXIS]

    def local_run(trans_loc, emit_loc, init_loc, tokens_loc, lengths_loc):
        seqs, step_count = tokens_loc.shape
        choices = [_capacities(seqs, step_count, spread) for spread in (2.7, 4.1)]
        em, lcol, lrow, rank, level = _run_prepare(choices, tokens_loc, lengths_loc, emit_loc)

        def run(ident, caps, trans, em, init, lcol, lrow, rank):
            alphas, ws, post, ll, _ = _run_recursion(nd, caps, ident, trans, em, init, lcol, lrow)
            return _run_counts(alphas, ws, trans, post, ll, rank)

        choices.append((seqs,) * (step_count - 1))
        runs = [functools.partial(run, k, caps) for k, caps in enumerate(choices)]
        counts, posterior, loglik = lax.switch(level[0], runs, trans_loc, em, init_loc, lcol, lrow, rank)
        return loglik[0], posterior, counts

    return jax.shard_map(
        local_run,
        mesh=mesh,
        in_specs=(P(None, AXIS), P(AXIS, None), P(AXIS), P("seqs", None), P("seqs")),
        out_specs=(P("seqs"), P("seqs", AXIS), P(("seqs", AXIS), None)),
        check_vma=False,
    )
```
